256 devices in a mesh: cand: 2 (over y), gx: 64 (over x, z), gy: 2 (over core).
Axes of the slice: x: 4, y: 2, z: 16, core: 2. Of those that a mesh axis runs over, the one named last changes fastest.
The devices are a block of a 4x16x16 slice.
Arguments:
- electric: float32 [2, 3, 512, 64, 128], P(None, None, ('cand', 'gx'), 'gy'), parts along dimension 2, may hold values from -6 to 6
- magnetic: float32 [2, 3, 512, 64, 128], P(None, None, ('cand', 'gx'), 'gy'), parts along dimension 2, may hold values from -6 to 6
- density: float32 [512, 64, 128], P(('cand', 'gx'), 'gy'), parts along dimension 0, may hold values from 0 to 0.1
- design_mask: int32 [512, 64, 128], P(('cand', 'gx'), 'gy'), parts along dimension 0, may hold values 0 or 1
- planes: int32 [4], P('cand'), parts along dimension 0, may hold values from 8 to 119
- profiles: float32 [2, 512, 64], P(None, ('cand', 'gx'), 'gy'), parts along dimension 1, may hold values from -6 to 6
- waveforms: float32 [2, 16], P(None, 'cand'), parts along dimension 1, may hold values from -4 to 4
Outputs:
- electric_out: float32 [2, 3, 512, 64, 128], P(None, None, ('cand', 'gx'), 'gy'), parts along dimension 2
- magnetic_out: float32 [2, 3, 512, 64, 128], P(None, None, ('cand', 'gx'), 'gy'), parts along dimension 2
- gradient: float32 [512, 64, 128], P(('cand', 'gx'), 'gy'), parts along dimension 0
The draws below stay inside these ranges and needn't reach their ends.
There are 2 independent parts, one for each index of `cand`. The reference program is written for one: setup_inputs(seed, part) draws one part's arguments, and reference() takes and returns one part's arrays. A program takes and returns all parts, laid end to end along the dimension named above; each array names one. Nothing has to cross between parts.
All inputs are finite; a program needn't handle non-finite values. No bound on the sum of `design_mask` on one device may be relied on, other than what follows from the above.
Results may differ from the reference program's by a relative error of at most 0.00016.
Values sent between devices are 32-bit elements; how exact they have to be, the bound alone decides.
A program may use at most 64 MiB of HBM per device.

```python
import jax
import jax.numpy as jnp
from jax import lax

NZ = 128
STEPS = 8
PMLW = 8
NX = 256
NY = 64


def plant(values, own_key, least, high):
    index_at = [jax.random.randint(jax.random.fold_in(own_key, axis), (), 0, length) for axis, length in enumerate(values.shape)]
    main_axis = values.shape.index(max(values.shape))
    beside = index_at[:main_axis] + [(index_at[main_axis] + 1) % values.shape[main_axis]] + index_at[main_axis + 1:]
    return values.at[tuple(index_at)].set(least).at[tuple(beside)].set(high)


def shard_levels(key, shape, split, smallest, top_value):
    level, own = 1.0, jax.random.fold_in(key, 6)
    for position, blocks in split:
        steps = jnp.exp(jax.random.uniform(jax.random.fold_in(own, position), (blocks,), jnp.float32, smallest / len(split), top_value / len(split)))
        level = level * jnp.repeat(steps, shape[position] // blocks).reshape([-1 if axis == position else 1 for axis in range(len(shape))])
    return level


def normal_values(rng, shape, spread, reach, cuts=(), held_as=jnp.bfloat16):
    entries = spread * jax.random.normal(rng, shape, jnp.float32)
    if cuts:
        entries = entries * shard_levels(rng, shape, cuts, -0.22, 0.18)
    return jnp.clip(entries, -reach, reach).astype(held_as)


def setup_inputs(seed: int = 0, part: int = 0) -> dict:
    splits = jax.random.split(jax.random.key(seed), 8)
    part_splits = jax.random.split(jax.random.fold_in(splits[7], part), 8)
    electric = normal_values(part_splits[0], (2, 3, NX, NY, NZ), 1.0, 6.0, ((2, 64), (3, 2)), jnp.float32)
    magnetic = normal_values(part_splits[1], (2, 3, NX, NY, NZ), 1.0, 6.0, ((2, 64), (3, 2)), jnp.float32)
    density = jnp.clip(0.1 * jax.random.uniform(part_splits[2], (NX, NY, NZ), jnp.float32) ** shard_levels(part_splits[2], (NX, NY, NZ), ((0, 64), (1, 2)), -0.2, 0.2), 0.0, 0.1)
    design_mask = plant((jax.random.randint(part_splits[3], (NX, NY, NZ), 0, 2) < 1).astype(jnp.int32), jax.random.fold_in(part_splits[3], 1), 0, 1)
    planes = jax.random.randint(part_splits[4], (2,), PMLW, NZ - PMLW).astype(jnp.int32)
    profiles = normal_values(part_splits[5], (2, NX, NY), 1.0, 6.0, ((1, 64), (2, 2)), jnp.float32)
    waveforms = normal_values(part_splits[6], (2, STEPS), 1.0, 4.0, (), jnp.float32)
    return dict(electric=electric, magnetic=magnetic, density=density, design_mask=design_mask, planes=planes, profiles=profiles, waveforms=waveforms)


step_dt = 0.7
contrast = 5.0
sigma_max = 2.0
small_eps = 1e-6
inv_spacing = 0.5


def coefficients(depth_cells, layer):
    zpos = jnp.arange(depth_cells).astype(jnp.float32)
    lower = (layer - zpos - 0.5) / layer
    upper = (zpos + 0.5 - (depth_cells - layer)) / layer
    depth = jnp.maximum(jnp.maximum(lower, upper), 0.0)
    sigma = sigma_max * depth * depth * depth
    half = sigma * step_dt / 2.0
    return (1.0 - half) / (1.0 + half), step_dt / (1.0 + half)


def fwd_diff(field, upper, axis):
    rest = lax.slice_in_dim(field, 1, field.shape[axis], axis=axis)
    return jnp.concatenate([rest, upper], axis) - field


def bwd_diff(field, lower, axis):
    rest = lax.slice_in_dim(field, 0, field.shape[axis] - 1, axis=axis)
    return field - jnp.concatenate([lower, rest], axis)


def fwd_z(field):
    return (jnp.concatenate([field[..., 1:], jnp.zeros_like(field[..., :1])], -1) - field) * inv_spacing


def bwd_z(field):
    return (field - jnp.concatenate([jnp.zeros_like(field[..., :1]), field[..., :-1]], -1)) * inv_spacing


def magnetic_update(elec, magn, x_upper, y_upper, decay, gain):
    ex, ey, ez = elec[:, 0], elec[:, 1], elec[:, 2]
    curl_x = fwd_diff(ez, y_upper[:, 1], 2) * inv_spacing - fwd_z(ey)
    curl_y = fwd_z(ex) - fwd_diff(ez, x_upper[:, 1], 1)
    curl_z = fwd_diff(ey, x_upper[:, 0], 1) - fwd_diff(ex, y_upper[:, 0], 2) * inv_spacing
    curl = jnp.stack([curl_x, curl_y, curl_z], 1)
    return decay * magn - gain * curl


def electric_update(elec, magn, x_lower, y_lower, decay, gain, inv_eps, drive):
    hx, hy, hz = magn[:, 0], magn[:, 1], magn[:, 2]
    curl_x = bwd_diff(hz, y_lower[:, 1], 2) * inv_spacing - bwd_z(hy)
    curl_y = bwd_z(hx) - bwd_diff(hz, x_lower[:, 1], 1)
    curl_z = bwd_diff(hy, x_lower[:, 0], 1) - bwd_diff(hx, y_lower[:, 0], 2) * inv_spacing
    new_x = decay * elec[:, 0] + gain * (inv_eps * curl_x - drive)
    new_y = decay * elec[:, 1] + gain * (inv_eps * curl_y)
    new_z = decay * elec[:, 2] + gain * (inv_eps * curl_z)
    return jnp.stack([new_x, new_y, new_z], 1)


def correlate(elec):
    return jnp.sum(elec[0] * elec[1], axis=0)


def reference(electric, magnetic, density, design_mask, planes, profiles, waveforms):
    decay, gain = coefficients(NZ, PMLW)
    flags = design_mask.astype(jnp.float32)
    inv_eps = 1.0 / (1.0 + contrast * density * flags)
    zidx = jnp.arange(NZ).astype(jnp.int32)
    source = profiles[0][:, :, None] * (zidx == planes[0]).astype(jnp.float32)
    adjoint = profiles[1][:, :, None] * (zidx == planes[1]).astype(jnp.float32)
    probe = (zidx == planes[1]).astype(jnp.float32)
    x_zero = jnp.zeros((2, 2, 1, NY, NZ), jnp.float32)
    y_zero = jnp.zeros((2, 2, NX, 1, NZ), jnp.float32)
    elec, magn = electric, magnetic
    corr = jnp.zeros((NX, NY, NZ), jnp.float32)
    for step in range(STEPS):
        magn = magnetic_update(elec, magn, x_zero, y_zero, decay, gain)
        drive = jnp.stack([source * waveforms[0, step], adjoint * waveforms[1, step]])
        elec = electric_update(elec, magn, x_zero, y_zero, decay, gain, inv_eps, drive)
        corr = corr + correlate(elec)
    power = jnp.sum(elec[0] * elec[0] * probe) / (NX * NY)
    gradient = flags * contrast * inv_eps * inv_eps * step_dt * corr / (power + small_eps)
    return elec, magn, gradient
```

```python
import jax
import jax.numpy as jnp
from jax import lax
from jax.experimental import pallas as pl
from jax.experimental.pallas import tpu as pltpu
from jax.sharding import PartitionSpec as P

STEPS = 8
PMLW = 8
CAND_GX = ("cand", "gx")
CHIPS_X = 4
MESH = pl.DeviceIdType.MESH

step_dt = 0.7
contrast = 5.0
sigma_max = 2.0
small_eps = 1e-06
inv_spacing = 0.5

WIN = 4
WINDOWS = STEPS // WIN
LEFT = 3
FRAME = 9
HALO = 8


def kernel(
    planes, waves, prof, e_in, h_in, den_in, mask_in,
    e_out, h_out, g_out,
    we, wh, fe, fh, send_h, send_e, recv_h, recv_e, ce, src, den, mask, grad, hist, part1, part2,
    load_sem, halo_send, halo_recv, mat_send, mat_recv,
    right_send, right_recv, left_send, left_recv,
    sum1_send, sum1_recv, sum2_send, sum2_recv,
):
    width, own_rows = den.shape[0], den.shape[1]
    rows, depth = own_rows + HALO, den.shape[2]
    count_x = lax.axis_size("gx")
    count_z = count_x // CHIPS_X
    gx, gy = lax.axis_index("gx"), lax.axis_index("gy")
    chip_x, chip_z = gx // count_z, lax.rem(gx, count_z)
    other = 1 - gy
    right = {"gx": lax.rem(gx + 1, count_x), "gy": gy}
    left = {"gx": lax.rem(gx + count_x - 1, count_x), "gy": gy}
    across = {"gx": gx, "gy": other}
    plane_peers = []
    for dx in range(CHIPS_X):
        for dc in range(2):
            if dx or dc:
                peer = lax.rem(chip_x + dx, CHIPS_X) * count_z + chip_z
                plane_peers.append({"gx": peer, "gy": other if dc else gy})
    line_peers = [
        {"gx": chip_x * count_z + lax.rem(chip_z + dz, count_z), "gy": gy}
        for dz in range(1, count_z)
    ]
    own = pl.multiple_of(gy * HALO, HALO)
    top = pl.multiple_of((1 - gy) * (own_rows - HALO), HALO)
    there = pl.multiple_of(gy * own_rows, HALO)
    X0 = LEFT
    block = pl.ds(X0, width)

    loads = [
        pltpu.make_async_copy(den_in, den, load_sem.at[0]),
        pltpu.make_async_copy(mask_in, mask, load_sem.at[1]),
        pltpu.make_async_copy(e_in, we.at[:, :, block, pl.ds(own, own_rows), :], load_sem.at[2]),
        pltpu.make_async_copy(
            h_in, wh.at[:, :, block, pl.ds(own + HALO, own_rows), :], load_sem.at[3]
        ),
    ]
    for load in loads:
        load.start()

    barrier = pltpu.get_barrier_semaphore()
    peers = [left, right] + plane_peers + line_peers
    for peer in peers:
        pl.semaphore_signal(barrier, inc=1, device_id=peer, device_id_type=MESH)

    lanes = lax.broadcasted_iota(jnp.int32, (1, depth), 1)
    zpos = lanes.astype(jnp.float32)
    lower = (PMLW - zpos - 0.5) / PMLW
    upper = (zpos + 0.5 - (depth - PMLW)) / PMLW
    deep = jnp.maximum(jnp.maximum(lower, upper), 0.0)
    half = sigma_max * deep * deep * deep * step_dt / 2.0
    decay1 = (1.0 - half) / (1.0 + half)
    gain1 = step_dt / (1.0 + half)
    decay = jnp.broadcast_to(decay1, (rows, depth))
    gain = jnp.broadcast_to(gain1, (rows, depth))
    gain_half = gain * inv_spacing
    first_lane = jnp.broadcast_to(lanes == 0, (rows, depth))
    last_lane = jnp.broadcast_to(lanes == depth - 1, (rows, depth))
    on_left = (gx > 0).astype(jnp.float32)
    on_right = (gx < count_x - 1).astype(jnp.float32)

    eye = lax.broadcasted_iota(jnp.int32, (own_rows, own_rows), 0) == lax.broadcasted_iota(
        jnp.int32, (own_rows, own_rows), 1
    )
    for s in range(2):
        spot = jnp.where(lanes == planes[s], gain1, 0.0)
        for x in range(width):
            row = jnp.broadcast_to(prof[s, x : x + 1, :], (own_rows, own_rows))
            column = jnp.sum(jnp.where(eye, row, 0.0), axis=1, keepdims=True)
            src[s, x, pl.ds(own, own_rows), :] = column * spot

    pad = jnp.zeros((HALO, depth), jnp.float32)
    plane0 = jnp.zeros((rows, depth), jnp.float32)
    for s in range(2):
        for c in range(3):
            for p in range(FRAME):
                if c != 1:
                    we[s, c, p, rows : rows + HALO, :] = pad
                    wh[s, c, p, 0:HALO, :] = pad
            wh[s, c, 0, HALO:, :] = plane0
    for c in (0, 2):
        for p in range(width + 1):
            fe[c, p, rows : rows + HALO, :] = pad
            fh[c, p, 0:HALO, :] = pad
    for c in range(3):
        fe[c, width, 0:rows, :] = plane0
        fh[c, 0, HALO:, :] = plane0

    pl.semaphore_wait(barrier, len(peers))

    halos = [
        pltpu.make_async_remote_copy(
            e_in.at[:, :, :, pl.ds(top, HALO), :],
            we.at[:, :, block, pl.ds(there, HALO), :],
            halo_send.at[0], halo_recv.at[0], device_id=across, device_id_type=MESH,
        ),
        pltpu.make_async_remote_copy(
            h_in.at[:, :, :, pl.ds(top, HALO), :],
            wh.at[:, :, block, pl.ds(there + HALO, HALO), :],
            halo_send.at[1], halo_recv.at[1], device_id=across, device_id_type=MESH,
        ),
        pltpu.make_async_remote_copy(
            src.at[:, :, pl.ds(pl.multiple_of(own + top, HALO), HALO), :],
            src.at[:, :, pl.ds(there, HALO), :],
            halo_send.at[2], halo_recv.at[2], device_id=across, device_id_type=MESH,
        ),
        pltpu.make_async_remote_copy(
            ce.at[block, pl.ds(pl.multiple_of(own + top, HALO), HALO), :],
            ce.at[block, pl.ds(there, HALO), :],
            halo_send.at[3], halo_recv.at[3], device_id=across, device_id_type=MESH,
        ),
    ]
    halos[0].start()
    halos[1].start()
    halos[2].start()
    loads[0].wait()
    loads[1].wait()
    for x in range(width):
        flags = mask[x].astype(jnp.float32)
        inv_eps = 1.0 / (1.0 + contrast * den[x] * flags)
        ce[X0 + x, pl.ds(own, own_rows), :] = inv_eps * gain1
        grad[x] = flags * contrast * inv_eps * inv_eps * step_dt
    halos[3].start()
    loads[2].wait()
    loads[3].wait()
    for halo in halos:
        halo.wait()

    materials = [
        pltpu.make_async_remote_copy(
            ce.at[pl.ds(X0 + width - 2, 2)], ce.at[pl.ds(X0 - 2, 2)],
            mat_send.at[0], mat_recv.at[0], device_id=right, device_id_type=MESH,
        ),
        pltpu.make_async_remote_copy(
            ce.at[pl.ds(X0, 2)], ce.at[pl.ds(X0 + width, 2)],
            mat_send.at[1], mat_recv.at[1], device_id=left, device_id_type=MESH,
        ),
    ]

    def to_right(s, w, k):
        return pltpu.make_async_remote_copy(
            send_h.at[s, w, k], recv_h.at[s, w, k],
            right_send.at[s, w, k], right_recv.at[s, w, k], device_id=right, device_id_type=MESH,
        )

    def to_left(s, w, k):
        return pltpu.make_async_remote_copy(
            send_e.at[s, w, k], recv_e.at[s, w, k],
            left_send.at[s, w, k], left_recv.at[s, w, k], device_id=left, device_id_type=MESH,
        )

    def up_z(f):
        return jnp.where(last_lane, 0.0, pltpu.roll(f, depth - 1, 1))

    def down_z(f):
        return jnp.where(first_lane, 0.0, pltpu.roll(f, 1, 1))

    def h_update(h_old, e, e_y, e_x, comps=(0, 1, 2)):
        new = {}
        if 0 in comps:
            new[0] = decay * h_old(0) - gain_half * ((e_y(2) - e[2]) - (up_z(e[1]) - e[1]))
        new[1] = decay * h_old(1) - (gain_half * (up_z(e[0]) - e[0]) - gain * (e_x[2] - e[2]))
        new[2] = decay * h_old(2) - (gain * (e_x[1] - e[1]) - gain_half * (e_y(0) - e[0]))
        return new

    def e_update(e_old, h, h_y, h_x, c, drive):
        cx = c * inv_spacing
        x = decay * e_old(0) + cx * ((h[2] - h_y(2)) - (h[1] - down_z(h[1])))
        if drive is not None:
            x = x - drive
        y = decay * e_old(1) + (cx * (h[0] - down_z(h[0])) - c * (h[2] - h_x[2]))
        z = decay * e_old(2) + (c * (h[1] - h_x[1]) - cx * (h[0] - h_y(0)))
        return {0: x, 1: y, 2: z}

    R0, R1 = slice(0, rows), slice(1, rows + 1)
    H0, HM = slice(HALO, HALO + rows), slice(HALO - 1, HALO + rows - 1)

    def free(s, w):
        for c in (1, 2):
            send_e[s, w, 0, c - 1] = we[s, c, X0, R0, :]
        to_left(s, w, 0).start()
        for k in range(WIN):
            last = k == WIN - 1
            h_planes = [x for x in range(width) if x >= k or x < width - 1 - k]
            if last:
                h_planes = [width - 1]
            for x in h_planes:
                if k == 0:
                    old_h = lambda c, x=x: wh[s, c, X0 + x, H0, :]
                    get_e = lambda c, x, r: we[s, c, X0 + x, r, :]
                else:
                    old_h = lambda c, x=x: fh[c, x + 1, H0, :]
                    get_e = lambda c, x, r: fe[c, x, r, :]
                e = {c: get_e(c, x, R0) for c in range(3)}
                e_x = {
                    c: (get_e(c, x + 1, R0) if x < width - 1 else jnp.zeros_like(e[c]))
                    for c in (1, 2)
                }
                new = h_update(
                    old_h, e, lambda c, x=x: get_e(c, x, R1), e_x, (1, 2) if last else (0, 1, 2)
                )
                if not last:
                    for c in range(3):
                        fh[c, x + 1, H0, :] = new[c]
                if x == width - 1:
                    send_h[s, w, k, 0] = new[1]
                    send_h[s, w, k, 1] = new[2]
            to_right(s, w, k).start()
            if last:
                break
            wave = waves[s, w * WIN + k]
            e_planes = [x for x in range(width) if x >= k + 1 or x < width - 1 - k]
            for x in e_planes:
                if k == 0:
                    old_e = lambda c, x=x: we[s, c, X0 + x, R0, :]
                else:
                    old_e = lambda c, x=x: fe[c, x, R0, :]
                h = {c: fh[c, x + 1, H0, :] for c in range(3)}
                h_x = {c: fh[c, x, H0, :] for c in (1, 2)}
                new = e_update(
                    old_e, h, lambda c, x=x: fh[c, x + 1, HM, :], h_x,
                    ce[X0 + x], src[s, x] * wave,
                )
                for c in range(3):
                    fe[c, x, R0, :] = new[c]
                if x == 0:
                    send_e[s, w, k + 1, 0] = new[1]
                    send_e[s, w, k + 1, 1] = new[2]
            to_left(s, w, k + 1).start()

    def true(s, w):
        for c in range(3):
            for p in (X0 - 2, X0 - 1, X0 + width, X0 + width + 1):
                we[s, c, p, R0, :] = plane0
                wh[s, c, p, H0, :] = plane0
        for k in range(WIN):
            reach = min(k + 1, WIN - k)
            h_lo, h_hi = -reach, width + min(k, WIN - 1 - k)
            e_out_reach = min(k + 1, WIN - 1 - k)
            to_left(s, w, k).wait_recv()
            e_next = None
            for x in range(h_hi - 1, h_lo - 1, -1):
                p = X0 + x
                e = {c: we[s, c, p, R0, :] for c in range(3)}
                if e_next is None:
                    e_x = {c: we[s, c, p + 1, R0, :] for c in (1, 2)}
                else:
                    e_x = e_next
                e_next = e
                if x == width - 1:
                    e_x = {c: (e_x[c] + recv_e[s, w, k, c - 1]) * on_right for c in (1, 2)}
                new = h_update(
                    lambda c: wh[s, c, p, H0, :], e, lambda c: we[s, c, p, R1, :], e_x
                )
                for c in range(3):
                    wh[s, c, p, H0, :] = new[c]
            to_right(s, w, k).wait_recv()
            wave = waves[s, w * WIN + k]
            h_last = None
            for x in range(-e_out_reach, width + e_out_reach):
                p = X0 + x
                h = {c: wh[s, c, p, H0, :] for c in range(3)}
                if h_last is None:
                    h_x = {c: wh[s, c, p - 1, H0, :] for c in (1, 2)}
                else:
                    h_x = h_last
                h_last = h
                if x == 0:
                    h_x = {c: (h_x[c] + recv_h[s, w, k, c - 1]) * on_left for c in (1, 2)}
                inside = 0 <= x < width
                new = e_update(
                    lambda c: we[s, c, p, R0, :], h, lambda c: wh[s, c, p, HM, :], h_x,
                    ce[p], src[s, x] * wave if inside else None,
                )
                for c in range(3):
                    we[s, c, p, R0, :] = new[c]
                    if inside:
                        hist[s, w * WIN + k, c, x] = new[c]

    def start_free(s, carry):
        free(s, 0)
        return carry

    lax.fori_loop(0, 2, start_free, 0)
    for material in materials:
        material.start()
    for material in materials:
        material.wait_recv()

    sum1 = [
        pltpu.make_async_remote_copy(
            part1.at[0], part1.at[1 + n], sum1_send.at[n], sum1_recv.at[n],
            device_id=peer, device_id_type=MESH,
        )
        for n, peer in enumerate(plane_peers)
    ]
    sum2 = [
        pltpu.make_async_remote_copy(
            part2.at[0], part2.at[1 + n], sum2_send.at[n], sum2_recv.at[n],
            device_id=peer, device_id_type=MESH,
        )
        for n, peer in enumerate(line_peers)
    ]
    outs = [
        pltpu.make_async_copy(we.at[:, :, block, pl.ds(own, own_rows), :], e_out, load_sem.at[2]),
        pltpu.make_async_copy(
            wh.at[:, :, block, pl.ds(own + HALO, own_rows), :], h_out, load_sem.at[3]
        ),
        pltpu.make_async_copy(grad, g_out, load_sem.at[0]),
    ]

    def turn(j, carry):
        w, s = j // 2, lax.rem(j, 2)
        true(s, w)

        @pl.when(w == 0)
        def _():
            free(s, 1)

        @pl.when(j == 2)
        def _():
            total = jnp.zeros((own_rows, depth), jnp.float32)
            for c in range(3):
                for x in range(width):
                    e = we[0, c, X0 + x, pl.ds(own, own_rows), :]
                    total = total + e * e
            line = jnp.sum(total, axis=0, keepdims=True)
            part1[0] = jnp.where(lanes == planes[1], line, 0.0)
            for copy in sum1:
                copy.start()

        return carry

    lax.fori_loop(0, 2 * WINDOWS, turn, 0)

    for copy in sum1:
        copy.wait_recv()
    total = part1[0]
    for n in range(len(sum1)):
        total = total + part1[1 + n]
    part2[0] = total
    for copy in sum2:
        copy.start()
    outs[0].start()
    outs[1].start()

    for x in range(width):
        corr = jnp.zeros((own_rows, depth), jnp.float32)
        for k in range(STEPS):
            for c in range(3):
                corr = corr + (
                    hist[0, k, c, x, pl.ds(own, own_rows), :]
                    * hist[1, k, c, x, pl.ds(own, own_rows), :]
                )
        grad[x] = grad[x] * corr

    for copy in sum2:
        copy.wait_recv()
    total = part2[0]
    for n in range(len(sum2)):
        total = total + part2[1 + n]
    cells = count_x * width * lax.axis_size("gy") * own_rows
    power = jnp.sum(total, axis=1, keepdims=True) / cells
    scale = jnp.broadcast_to(1.0 / (power + small_eps), (own_rows, depth))
    for x in range(width):
        grad[x] = grad[x] * scale
    outs[2].start()
    for out in outs:
        out.wait()
    for material in materials:
        material.wait_send()
    for copy in sum1 + sum2:
        copy.wait_send()

    def drain(j, carry):
        w, s = j // 2, lax.rem(j, 2)
        for k in range(WIN):
            to_right(s, w, k).wait_send()
            to_left(s, w, k).wait_send()
        return carry

    lax.fori_loop(0, 2 * WINDOWS, drain, 0)


def shards(electric, magnetic, density, design_mask, planes, profiles, waveforms):
    sets, comps, width, own_rows, depth = electric.shape
    rows = own_rows + HALO
    count_z = lax.axis_size("gx") // CHIPS_X
    f32 = jnp.float32
    vmem, dma = pltpu.VMEM, pltpu.SemaphoreType.DMA
    series = vmem((sets, WINDOWS, WIN, 2, rows, depth), f32)
    any_space = pl.BlockSpec(memory_space=pl.ANY)
    smem_space = pl.BlockSpec(memory_space=pltpu.SMEM)
    return pl.pallas_call(
        kernel,
        out_shape=(
            jax.ShapeDtypeStruct(electric.shape, f32),
            jax.ShapeDtypeStruct(magnetic.shape, f32),
            jax.ShapeDtypeStruct(density.shape, f32),
        ),
        in_specs=[smem_space, smem_space, pl.BlockSpec(memory_space=pltpu.VMEM)] + [any_space] * 4,
        out_specs=(any_space,) * 3,
        scratch_shapes=[
            vmem((sets, comps, FRAME, rows + HALO, depth), f32),
            vmem((sets, comps, FRAME, rows + HALO, depth), f32),
            vmem((comps, width + 1, rows + HALO, depth), f32),
            vmem((comps, width + 1, rows + HALO, depth), f32),
            series, series, series, series,
            vmem((FRAME, rows, depth), f32),
            vmem((sets, width, rows, depth), f32),
            vmem((width, own_rows, depth), f32),
            vmem((width, own_rows, depth), jnp.int32),
            vmem((width, own_rows, depth), f32),
            vmem((sets, STEPS, comps, width, rows, depth), f32),
            vmem((2 * CHIPS_X, 1, depth), f32),
            vmem((count_z, 1, depth), f32),
            dma((4,)), dma((4,)), dma((4,)), dma((2,)), dma((2,)),
            dma((sets, WINDOWS, WIN)), dma((sets, WINDOWS, WIN)),
            dma((sets, WINDOWS, WIN)), dma((sets, WINDOWS, WIN)),
            dma((2 * CHIPS_X - 1,)), dma((2 * CHIPS_X - 1,)),
            dma((count_z - 1,)), dma((count_z - 1,)),
        ],
        compiler_params=pltpu.CompilerParams(collective_id=0, has_side_effects=True),
    )(planes, waveforms, profiles, electric, magnetic, density, design_mask)


def solution(mesh):
    return jax.shard_map(
        shards,
        mesh=mesh,
        in_specs=(
            P(None, None, CAND_GX, "gy", None),
            P(None, None, CAND_GX, "gy", None),
            P(CAND_GX, "gy", None),
            P(CAND_GX, "gy", None),
            P("cand"),
            P(None, CAND_GX, "gy"),
            P(None, "cand"),
        ),
        out_specs=(
            P(None, None, CAND_GX, "gy", None),
            P(None, None, CAND_GX, "gy", None),
            P(CAND_GX, "gy", None),
        ),
        check_vma=False,
    )
```

```python
import jax
import jax.numpy as jnp
from jax import lax
from jax.experimental import pallas as pl
from jax.experimental.pallas import tpu as pltpu
from jax.sharding import PartitionSpec as P

STEPS = 8
PMLW = 8
CAND_GX = ("cand", "gx")
CHIPS_X = 4
MESH = pl.DeviceIdType.MESH

step_dt = 0.7
contrast = 5.0
sigma_max = 2.0
small_eps = 1e-06
inv_spacing = 0.5

WIN = 4
WINDOWS = STEPS // WIN
LEFT = 3
FRAME = 9
HALO = 8


def kernel(
    planes_in, waves_in, prof_in, e_in, h_in, den_in, mask_in,
    we, wh, grad,
    fe, fh, send_h, send_e, recv_h, recv_e, ce, src, den, mask, hist, part1, part2,
    planes, waves, prof, load_sem, near, mid, far, halo_send, halo_recv, mat_send, mat_recv,
    right_send, right_recv, left_send, left_recv,
    sum1_send, sum1_recv, sum2_send, sum2_recv,
):
    width, own_rows = den.shape[0], den.shape[1]
    rows, depth = own_rows + HALO, den.shape[2]
    count_x = lax.axis_size("gx")
    count_z = count_x // CHIPS_X
    gx, gy = lax.axis_index("gx"), lax.axis_index("gy")
    chip_x, chip_z = gx // count_z, lax.rem(gx, count_z)
    other = 1 - gy
    right = {"gx": lax.rem(gx + 1, count_x), "gy": gy}
    left = {"gx": lax.rem(gx + count_x - 1, count_x), "gy": gy}
    across = {"gx": gx, "gy": other}
    plane_peers = []
    for dx in range(CHIPS_X):
        for dc in range(2):
            if dx or dc:
                peer = lax.rem(chip_x + dx, CHIPS_X) * count_z + chip_z
                plane_peers.append({"gx": peer, "gy": other if dc else gy})

    def along_z(dz):
        return {"gx": chip_x * count_z + lax.rem(chip_z + dz, count_z), "gy": gy}

    def both_ways(d):
        return [along_z(dz) for dz in sorted({d % count_z, -d % count_z} - {0})]

    line_peers = [along_z(dz) for dz in range(1, count_z)]
    next_chips = [
        {"gx": lax.rem(chip_x + dx, CHIPS_X) * count_z + chip_z, "gy": gy} for dx in (1, CHIPS_X - 1)
    ]
    own = pl.multiple_of(gy * HALO, HALO)
    top = pl.multiple_of((1 - gy) * (own_rows - HALO), HALO)
    there = pl.multiple_of(gy * own_rows, HALO)
    X0 = LEFT
    block = pl.ds(X0, width)

    loads = [
        pltpu.make_async_copy(den_in, den, load_sem.at[0]),
        pltpu.make_async_copy(mask_in, mask, load_sem.at[1]),
        pltpu.make_async_copy(e_in, we.at[:, :, block, pl.ds(own, own_rows), :], load_sem.at[2]),
        pltpu.make_async_copy(
            h_in, wh.at[:, :, block, pl.ds(own + HALO, own_rows), :], load_sem.at[3]
        ),
        pltpu.make_async_copy(planes_in, planes, load_sem.at[4]),
        pltpu.make_async_copy(waves_in, waves, load_sem.at[5]),
        pltpu.make_async_copy(prof_in, prof, load_sem.at[6]),
    ]
    for load in loads:
        load.start()

    def signal(semaphore, peers):
        for peer in peers:
            pl.semaphore_signal(semaphore, inc=1, device_id=peer, device_id_type=MESH)

    barrier = pltpu.get_barrier_semaphore()
    peers = [across, left, right] + next_chips + both_ways(1)
    near_peers = next_chips + both_ways(1)
    mid_peers = next_chips + both_ways(2)
    far_peers = both_ways(4)
    signal(barrier, peers)

    lanes = lax.broadcasted_iota(jnp.int32, (1, depth), 1)
    zpos = lanes.astype(jnp.float32)
    lower = (PMLW - zpos - 0.5) / PMLW
    upper = (zpos + 0.5 - (depth - PMLW)) / PMLW
    deep = jnp.maximum(jnp.maximum(lower, upper), 0.0)
    half = sigma_max * deep * deep * deep * step_dt / 2.0
    decay1 = (1.0 - half) / (1.0 + half)
    gain1 = step_dt / (1.0 + half)
    decay = jnp.broadcast_to(decay1, (rows, depth))
    gain = jnp.broadcast_to(gain1, (rows, depth))
    gain_half = gain * inv_spacing
    first_lane = jnp.broadcast_to(lanes == 0, (rows, depth))
    last_lane = jnp.broadcast_to(lanes == depth - 1, (rows, depth))
    on_left = (gx > 0).astype(jnp.float32)
    on_right = (gx < count_x - 1).astype(jnp.float32)

    eye = lax.broadcasted_iota(jnp.int32, (own_rows, own_rows), 0) == lax.broadcasted_iota(
        jnp.int32, (own_rows, own_rows), 1
    )
    loads[4].wait()
    loads[6].wait()
    for s in range(2):
        spot = jnp.where(lanes == planes[s], gain1, 0.0)
        for x in range(width):
            row = jnp.broadcast_to(prof[s, x : x + 1, :], (own_rows, own_rows))
            column = jnp.sum(jnp.where(eye, row, 0.0), axis=1, keepdims=True)
            src[s, x, pl.ds(own, own_rows), :] = column * spot

    pad = jnp.zeros((HALO, depth), jnp.float32)
    plane0 = jnp.zeros((rows, depth), jnp.float32)
    for s in range(2):
        for c in range(3):
            for p in range(FRAME):
                if c != 1:
                    we[s, c, p, rows : rows + HALO, :] = pad
                    wh[s, c, p, 0:HALO, :] = pad
            wh[s, c, 0, HALO:, :] = plane0
    for c in (0, 2):
        for p in range(width + 1):
            fe[c, p, rows : rows + HALO, :] = pad
            fh[c, p, 0:HALO, :] = pad
    for c in range(3):
        fe[c, width, 0:rows, :] = plane0
        fh[c, 0, HALO:, :] = plane0

    pl.semaphore_wait(barrier, len(peers))
    signal(near, near_peers)

    halos = [
        pltpu.make_async_remote_copy(
            e_in.at[:, :, :, pl.ds(top, HALO), :],
            we.at[:, :, block, pl.ds(there, HALO), :],
            halo_send.at[0], halo_recv.at[0], device_id=across, device_id_type=MESH,
        ),
        pltpu.make_async_remote_copy(
            h_in.at[:, :, :, pl.ds(top, HALO), :],
            wh.at[:, :, block, pl.ds(there + HALO, HALO), :],
            halo_send.at[1], halo_recv.at[1], device_id=across, device_id_type=MESH,
        ),
        pltpu.make_async_remote_copy(
            src.at[:, :, pl.ds(pl.multiple_of(own + top, HALO), HALO), :],
            src.at[:, :, pl.ds(there, HALO), :],
            halo_send.at[2], halo_recv.at[2], device_id=across, device_id_type=MESH,
        ),
        pltpu.make_async_remote_copy(
            ce.at[block, pl.ds(pl.multiple_of(own + top, HALO), HALO), :],
            ce.at[block, pl.ds(there, HALO), :],
            halo_send.at[3], halo_recv.at[3], device_id=across, device_id_type=MESH,
        ),
    ]
    halos[0].start()
    halos[1].start()
    halos[2].start()
    loads[0].wait()
    loads[1].wait()
    for x in range(width):
        flags = mask[x].astype(jnp.float32)
        inv_eps = 1.0 / (1.0 + contrast * den[x] * flags)
        ce[X0 + x, pl.ds(own, own_rows), :] = inv_eps * gain1
        grad[x] = flags * contrast * inv_eps * inv_eps * step_dt
    halos[3].start()
    loads[2].wait()
    loads[3].wait()
    loads[5].wait()
    for halo in halos:
        halo.wait()

    materials = [
        pltpu.make_async_remote_copy(
            ce.at[pl.ds(X0 + width - 2, 2)], ce.at[pl.ds(X0 - 2, 2)],
            mat_send.at[0], mat_recv.at[0], device_id=right, device_id_type=MESH,
        ),
        pltpu.make_async_remote_copy(
            ce.at[pl.ds(X0, 2)], ce.at[pl.ds(X0 + width, 2)],
            mat_send.at[1], mat_recv.at[1], device_id=left, device_id_type=MESH,
        ),
    ]

    def to_right(s, w, k):
        return pltpu.make_async_remote_copy(
            send_h.at[s, w, k], recv_h.at[s, w, k],
            right_send.at[s, w, k], right_recv.at[s, w, k], device_id=right, device_id_type=MESH,
        )

    def to_left(s, w, k):
        return pltpu.make_async_remote_copy(
            send_e.at[s, w, k], recv_e.at[s, w, k],
            left_send.at[s, w, k], left_recv.at[s, w, k], device_id=left, device_id_type=MESH,
        )

    def up_z(f):
        return jnp.where(last_lane, 0.0, pltpu.roll(f, depth - 1, 1))

    def down_z(f):
        return jnp.where(first_lane, 0.0, pltpu.roll(f, 1, 1))

    def h_update(h_old, e, e_y, e_x, comps=(0, 1, 2)):
        new = {}
        if 0 in comps:
            new[0] = decay * h_old(0) - gain_half * ((e_y(2) - e[2]) - (up_z(e[1]) - e[1]))
        new[1] = decay * h_old(1) - (gain_half * (up_z(e[0]) - e[0]) - gain * (e_x[2] - e[2]))
        new[2] = decay * h_old(2) - (gain * (e_x[1] - e[1]) - gain_half * (e_y(0) - e[0]))
        return new

    def e_update(e_old, h, h_y, h_x, c, drive):
        cx = c * inv_spacing
        x = decay * e_old(0) + cx * ((h[2] - h_y(2)) - (h[1] - down_z(h[1])))
        if drive is not None:
            x = x - drive
        y = decay * e_old(1) + (cx * (h[0] - down_z(h[0])) - c * (h[2] - h_x[2]))
        z = decay * e_old(2) + (c * (h[1] - h_x[1]) - cx * (h[0] - h_y(0)))
        return {0: x, 1: y, 2: z}

    R0, R1 = slice(0, rows), slice(1, rows + 1)
    H0, HM = slice(HALO, HALO + rows), slice(HALO - 1, HALO + rows - 1)

    def free(s, w):
        for c in (1, 2):
            send_e[s, w, 0, c - 1] = we[s, c, X0, R0, :]
        to_left(s, w, 0).start()
        for k in range(WIN):
            last = k == WIN - 1
            h_planes = [x for x in range(width) if x >= k or x < width - 1 - k]
            if last:
                h_planes = [width - 1]
            for x in h_planes:
                if k == 0:
                    old_h = lambda c, x=x: wh[s, c, X0 + x, H0, :]
                    get_e = lambda c, x, r: we[s, c, X0 + x, r, :]
                else:
                    old_h = lambda c, x=x: fh[c, x + 1, H0, :]
                    get_e = lambda c, x, r: fe[c, x, r, :]
                e = {c: get_e(c, x, R0) for c in range(3)}
                e_x = {
                    c: (get_e(c, x + 1, R0) if x < width - 1 else jnp.zeros_like(e[c]))
                    for c in (1, 2)
                }
                new = h_update(
                    old_h, e, lambda c, x=x: get_e(c, x, R1), e_x, (1, 2) if last else (0, 1, 2)
                )
                if not last:
                    for c in range(3):
                        fh[c, x + 1, H0, :] = new[c]
                if x == width - 1:
                    send_h[s, w, k, 0] = new[1]
                    send_h[s, w, k, 1] = new[2]
            to_right(s, w, k).start()
            if last:
                break
            wave = waves[s, w * WIN + k]
            e_planes = [x for x in range(width) if x >= k + 1 or x < width - 1 - k]
            for x in e_planes:
                if k == 0:
                    old_e = lambda c, x=x: we[s, c, X0 + x, R0, :]
                else:
                    old_e = lambda c, x=x: fe[c, x, R0, :]
                h = {c: fh[c, x + 1, H0, :] for c in range(3)}
                h_x = {c: fh[c, x, H0, :] for c in (1, 2)}
                new = e_update(
                    old_e, h, lambda c, x=x: fh[c, x + 1, HM, :], h_x,
                    ce[X0 + x], src[s, x] * wave,
                )
                for c in range(3):
                    fe[c, x, R0, :] = new[c]
                if x == 0:
                    send_e[s, w, k + 1, 0] = new[1]
                    send_e[s, w, k + 1, 1] = new[2]
            to_left(s, w, k + 1).start()

    def true(s, w, before_last):
        for c in range(3):
            for p in (X0 - 2, X0 - 1, X0 + width, X0 + width + 1):
                we[s, c, p, R0, :] = plane0
                wh[s, c, p, H0, :] = plane0
        for k in range(WIN):
            reach = min(k + 1, WIN - k)
            h_lo, h_hi = -reach, width + min(k, WIN - 1 - k)
            e_out_reach = min(k + 1, WIN - 1 - k)
            if k == WIN - 1:
                before_last()
            to_left(s, w, k).wait_recv()
            e_next = None
            for x in range(h_hi - 1, h_lo - 1, -1):
                p = X0 + x
                e = {c: we[s, c, p, R0, :] for c in range(3)}
                if e_next is None:
                    e_x = {c: we[s, c, p + 1, R0, :] for c in (1, 2)}
                else:
                    e_x = e_next
                e_next = e
                if x == width - 1:
                    e_x = {c: (e_x[c] + recv_e[s, w, k, c - 1]) * on_right for c in (1, 2)}
                new = h_update(
                    lambda c: wh[s, c, p, H0, :], e, lambda c: we[s, c, p, R1, :], e_x
                )
                for c in range(3):
                    wh[s, c, p, H0, :] = new[c]
            to_right(s, w, k).wait_recv()
            wave = waves[s, w * WIN + k]
            h_last = None
            for x in range(-e_out_reach, width + e_out_reach):
                p = X0 + x
                h = {c: wh[s, c, p, H0, :] for c in range(3)}
                if h_last is None:
                    h_x = {c: wh[s, c, p - 1, H0, :] for c in (1, 2)}
                else:
                    h_x = h_last
                h_last = h
                if x == 0:
                    h_x = {c: (h_x[c] + recv_h[s, w, k, c - 1]) * on_left for c in (1, 2)}
                inside = 0 <= x < width
                new = e_update(
                    lambda c: we[s, c, p, R0, :], h, lambda c: wh[s, c, p, HM, :], h_x,
                    ce[p], src[s, x] * wave if inside else None,
                )
                for c in range(3):
                    we[s, c, p, R0, :] = new[c]
                    if inside:
                        hist[s, w * WIN + k, c, x] = new[c]

    def start_free(s, carry):
        free(s, 0)
        return carry

    lax.fori_loop(0, 2, start_free, 0)
    pl.semaphore_wait(near, len(near_peers))
    signal(mid, mid_peers)
    for material in materials:
        material.start()
    for material in materials:
        material.wait_recv()

    sum1 = [
        pltpu.make_async_remote_copy(
            part1.at[0], part1.at[1 + n], sum1_send.at[n], sum1_recv.at[n],
            device_id=peer, device_id_type=MESH,
        )
        for n, peer in enumerate(plane_peers)
    ]
    sum2 = [
        pltpu.make_async_remote_copy(
            part2.at[0], part2.at[1 + n], sum2_send.at[n], sum2_recv.at[n],
            device_id=peer, device_id_type=MESH,
        )
        for n, peer in enumerate(line_peers)
    ]
    def turn(j, carry):
        w, s = j // 2, lax.rem(j, 2)

        def add_plane():
            @pl.when(j == 3)
            def _():
                for copy in sum1:
                    copy.wait_recv()
                total = part1[0]
                for n in range(len(sum1)):
                    total = total + part1[1 + n]
                part2[0] = total
                for copy in sum2:
                    copy.start()

        true(s, w, add_plane)

        @pl.when(w == 0)
        def _():
            free(s, 1)

        @pl.when(j == 1)
        def _():
            pl.semaphore_wait(mid, len(mid_peers))
            signal(far, far_peers)

        @pl.when(j == 2)
        def _():
            pl.semaphore_wait(far, len(far_peers))
            total = jnp.zeros((own_rows, depth), jnp.float32)
            for c in range(3):
                for x in range(width):
                    e = we[0, c, X0 + x, pl.ds(own, own_rows), :]
                    total = total + e * e
            line = jnp.sum(total, axis=0, keepdims=True)
            part1[0] = jnp.where(lanes == planes[1], line, 0.0)
            for copy in sum1:
                copy.start()

        return carry

    lax.fori_loop(0, 2 * WINDOWS, turn, 0)

    for x in range(width):
        corr = jnp.zeros((own_rows, depth), jnp.float32)
        for k in range(STEPS):
            for c in range(3):
                corr = corr + (
                    hist[0, k, c, x, pl.ds(own, own_rows), :]
                    * hist[1, k, c, x, pl.ds(own, own_rows), :]
                )
        grad[x] = grad[x] * corr

    for copy in sum2:
        copy.wait_recv()
    total = part2[0]
    for n in range(len(sum2)):
        total = total + part2[1 + n]
    cells = count_x * width * lax.axis_size("gy") * own_rows
    power = jnp.sum(total, axis=1, keepdims=True) / cells
    scale = jnp.broadcast_to(1.0 / (power + small_eps), (own_rows, depth))
    for x in range(width):
        grad[x] = grad[x] * scale
    for material in materials:
        material.wait_send()
    for copy in sum1 + sum2:
        copy.wait_send()

    def drain(j, carry):
        w, s = j // 2, lax.rem(j, 2)
        for k in range(WIN):
            to_right(s, w, k).wait_send()
            to_left(s, w, k).wait_send()
        return carry

    lax.fori_loop(0, 2 * WINDOWS, drain, 0)


def store(we, wh, grad, e_out, h_out, g_out, sem):
    width, own_rows = grad.shape[0], grad.shape[1]
    own = pl.multiple_of(lax.axis_index("gy") * HALO, HALO)
    block = pl.ds(LEFT, width)
    outs = [
        pltpu.make_async_copy(we.at[:, :, block, pl.ds(own, own_rows), :], e_out, sem.at[0]),
        pltpu.make_async_copy(wh.at[:, :, block, pl.ds(own + HALO, own_rows), :], h_out, sem.at[1]),
        pltpu.make_async_copy(grad, g_out, sem.at[2]),
    ]
    for out in outs:
        out.start()
    for out in outs:
        out.wait()


def vmem_array(shape):
    return pltpu.VMEM(shape, jnp.float32)


def in_vmem(x):
    return pltpu.with_memory_space_constraint(x, pltpu.VMEM)


def shards(electric, magnetic, density, design_mask, planes, profiles, waveforms):
    sets, comps, width, own_rows, depth = electric.shape
    rows = own_rows + HALO
    count_z = lax.axis_size("gx") // CHIPS_X
    f32 = jnp.float32
    vmem, dma = pltpu.VMEM, pltpu.SemaphoreType.DMA
    series = vmem((sets, WINDOWS, WIN, 2, rows, depth), f32)
    any_space = pl.BlockSpec(memory_space=pl.ANY)
    held = pl.BlockSpec(memory_space=pltpu.VMEM)
    smem, wait = pltpu.SMEM, pltpu.SemaphoreType.REGULAR
    frame = (sets, comps, FRAME, rows + HALO, depth)
    e_frame, h_frame, grad = pl.pallas_call(
        kernel,
        out_shape=(vmem_array(frame), vmem_array(frame), vmem_array(density.shape)),
        in_specs=[any_space] * 7,
        out_specs=(held,) * 3,
        scratch_shapes=[
            vmem((comps, width + 1, rows + HALO, depth), f32),
            vmem((comps, width + 1, rows + HALO, depth), f32),
            series, series, series, series,
            vmem((FRAME, rows, depth), f32),
            vmem((sets, width, rows, depth), f32),
            vmem((width, own_rows, depth), f32),
            vmem((width, own_rows, depth), jnp.int32),
            vmem((sets, STEPS, comps, width, rows, depth), f32),
            vmem((2 * CHIPS_X, 1, depth), f32),
            vmem((count_z, 1, depth), f32),
            smem(planes.shape, jnp.int32),
            smem(waveforms.shape, f32),
            vmem(profiles.shape, f32),
            dma((7,)), wait, wait, wait, dma((4,)), dma((4,)), dma((2,)), dma((2,)),
            dma((sets, WINDOWS, WIN)), dma((sets, WINDOWS, WIN)),
            dma((sets, WINDOWS, WIN)), dma((sets, WINDOWS, WIN)),
            dma((2 * CHIPS_X - 1,)), dma((2 * CHIPS_X - 1,)),
            dma((max(count_z - 1, 1),)), dma((max(count_z - 1, 1),)),
        ],
        compiler_params=pltpu.CompilerParams(
            collective_id=0, has_side_effects=True, vmem_limit_bytes=64_200_000
        ),
    )(planes, waveforms, profiles, electric, magnetic, density, design_mask)
    return pl.pallas_call(
        store,
        out_shape=(
            jax.ShapeDtypeStruct(electric.shape, f32),
            jax.ShapeDtypeStruct(magnetic.shape, f32),
            jax.ShapeDtypeStruct(density.shape, f32),
        ),
        in_specs=[held] * 3,
        out_specs=(any_space,) * 3,
        scratch_shapes=[dma((3,))],
        compiler_params=pltpu.CompilerParams(vmem_limit_bytes=4 << 20),
    )(in_vmem(e_frame), in_vmem(h_frame), in_vmem(grad))


def solution(mesh):
    return jax.shard_map(
        shards,
        mesh=mesh,
        in_specs=(
            P(None, None, CAND_GX, "gy", None),
            P(None, None, CAND_GX, "gy", None),
            P(CAND_GX, "gy", None),
            P(CAND_GX, "gy", None),
            P("cand"),
            P(None, CAND_GX, "gy"),
            P(None, "cand"),
        ),
        out_specs=(
            P(None, None, CAND_GX, "gy", None),
            P(None, None, CAND_GX, "gy", None),
            P(CAND_GX, "gy", None),
        ),
        check_vma=False,
    )
```

```python
import jax
import jax.numpy as jnp
from jax import lax
from jax.experimental import pallas as pl
from jax.experimental.pallas import tpu as pltpu
from jax.sharding import PartitionSpec as P

STEPS = 8
PMLW = 8
CAND_GX = ("cand", "gx")
CHIPS_X = 4
MESH = pl.DeviceIdType.MESH

step_dt = 0.7
contrast = 5.0
sigma_max = 2.0
small_eps = 1e-06
inv_spacing = 0.5

WIN = 4
WINDOWS = STEPS // WIN
LEFT = 3
FRAME = 9
HALO = 8


def kernel(
    planes_in, waves_in, prof_in, e_in, h_in, den_in, mask_in,
    we, wh, grad,
    fe, fh, send_h, send_e, recv_h, recv_e, ce, src, den, mask, hist, part1, part2,
    planes, waves, prof, load_sem, near, mid, far, halo_send, halo_recv, mat_send, mat_recv,
    right_send, right_recv, left_send, left_recv,
    sum1_send, sum1_recv, sum2_send, sum2_recv,
):
    width, own_rows = den.shape[0], den.shape[1]
    rows, depth = own_rows + HALO, den.shape[2]
    count_x = lax.axis_size("gx")
    count_z = count_x // CHIPS_X
    gx, gy = lax.axis_index("gx"), lax.axis_index("gy")
    chip_x, chip_z = gx // count_z, lax.rem(gx, count_z)
    other = 1 - gy
    right = {"gx": lax.rem(gx + 1, count_x), "gy": gy}
    left = {"gx": lax.rem(gx + count_x - 1, count_x), "gy": gy}
    across = {"gx": gx, "gy": other}
    right_across, left_across = dict(right, gy=other), dict(left, gy=other)
    has_right, has_left = gx < count_x - 1, gx > 0
    plane_peers = []
    for dx in range(CHIPS_X):
        for dc in range(2):
            if dx or dc:
                peer = lax.rem(chip_x + dx, CHIPS_X) * count_z + chip_z
                plane_peers.append({"gx": peer, "gy": other if dc else gy})

    def along_z(dz):
        return {"gx": chip_x * count_z + lax.rem(chip_z + dz, count_z), "gy": gy}

    def both_ways(d):
        return [along_z(dz) for dz in sorted({d % count_z, -d % count_z} - {0})]

    line_peers = [along_z(dz) for dz in range(1, count_z)]
    next_chips = [
        {"gx": lax.rem(chip_x + dx, CHIPS_X) * count_z + chip_z, "gy": gy} for dx in (1, CHIPS_X - 1)
    ]
    own = pl.multiple_of(gy * HALO, HALO)
    top = pl.multiple_of((1 - gy) * (own_rows - HALO), HALO)
    there = pl.multiple_of(gy * own_rows, HALO)
    X0 = LEFT
    block = pl.ds(X0, width)

    loads = [
        pltpu.make_async_copy(den_in, den, load_sem.at[0]),
        pltpu.make_async_copy(mask_in, mask, load_sem.at[1]),
        pltpu.make_async_copy(e_in, we.at[:, :, block, pl.ds(own, own_rows), :], load_sem.at[2]),
        pltpu.make_async_copy(
            h_in, wh.at[:, :, block, pl.ds(own + HALO, own_rows), :], load_sem.at[3]
        ),
        pltpu.make_async_copy(planes_in, planes, load_sem.at[4]),
        pltpu.make_async_copy(waves_in, waves, load_sem.at[5]),
        pltpu.make_async_copy(prof_in, prof, load_sem.at[6]),
    ]
    for load in loads:
        load.start()

    def signal(semaphore, peers):
        for peer in peers:
            pl.semaphore_signal(semaphore, inc=1, device_id=peer, device_id_type=MESH)

    barrier = pltpu.get_barrier_semaphore()
    peers = [across, left, right, left_across, right_across] + next_chips + both_ways(1)
    near_peers = next_chips + both_ways(1)
    mid_peers = next_chips + both_ways(2)
    far_peers = both_ways(4)
    signal(barrier, peers)

    lanes = lax.broadcasted_iota(jnp.int32, (1, depth), 1)
    zpos = lanes.astype(jnp.float32)
    lower = (PMLW - zpos - 0.5) / PMLW
    upper = (zpos + 0.5 - (depth - PMLW)) / PMLW
    deep = jnp.maximum(jnp.maximum(lower, upper), 0.0)
    half = sigma_max * deep * deep * deep * step_dt / 2.0
    decay1 = (1.0 - half) / (1.0 + half)
    gain1 = step_dt / (1.0 + half)
    decay = jnp.broadcast_to(decay1, (rows, depth))
    gain = jnp.broadcast_to(gain1, (rows, depth))
    gain_half = gain * inv_spacing
    first_lane = jnp.broadcast_to(lanes == 0, (rows, depth))
    last_lane = jnp.broadcast_to(lanes == depth - 1, (rows, depth))
    on_left = has_left.astype(jnp.float32)
    on_right = has_right.astype(jnp.float32)

    pad = jnp.zeros((HALO, depth), jnp.float32)
    plane0 = jnp.zeros((rows, depth), jnp.float32)
    for s in range(2):
        for c in range(3):
            for p in range(FRAME):
                if c != 1:
                    we[s, c, p, rows : rows + HALO, :] = pad
                    wh[s, c, p, 0:HALO, :] = pad
            wh[s, c, 0, HALO:, :] = plane0
    for c in (0, 2):
        for p in range(width + 1):
            fe[c, p, rows : rows + HALO, :] = pad
            fh[c, p, 0:HALO, :] = pad
    for c in range(3):
        fe[c, width, 0:rows, :] = plane0
        fh[c, 0, HALO:, :] = plane0

    @pl.when(jnp.logical_not(has_right))
    def _():
        recv_e[...] = jnp.zeros_like(recv_e)
        for p in (X0 + width, X0 + width + 1):
            ce[p] = plane0

    @pl.when(jnp.logical_not(has_left))
    def _():
        recv_h[...] = jnp.zeros_like(recv_h)
        for p in (X0 - 2, X0 - 1):
            ce[p] = plane0

    pl.semaphore_wait(barrier, len(peers))

    halos = [
        pltpu.make_async_remote_copy(
            e_in.at[:, :, :, pl.ds(top, HALO), :],
            we.at[:, :, block, pl.ds(there, HALO), :],
            halo_send.at[0], halo_recv.at[0], device_id=across, device_id_type=MESH,
        ),
        pltpu.make_async_remote_copy(
            h_in.at[:, :, :, pl.ds(top, HALO), :],
            wh.at[:, :, block, pl.ds(there + HALO, HALO), :],
            halo_send.at[1], halo_recv.at[1], device_id=across, device_id_type=MESH,
        ),
        pltpu.make_async_remote_copy(
            src.at[:, :, pl.ds(pl.multiple_of(own + top, HALO), HALO), :],
            src.at[:, :, pl.ds(there, HALO), :],
            halo_send.at[2], halo_recv.at[2], device_id=across, device_id_type=MESH,
        ),
        pltpu.make_async_remote_copy(
            ce.at[block, pl.ds(pl.multiple_of(own + top, HALO), HALO), :],
            ce.at[block, pl.ds(there, HALO), :],
            halo_send.at[3], halo_recv.at[3], device_id=across, device_id_type=MESH,
        ),
    ]
    halos[0].start()
    halos[1].start()

    own_slice = pl.ds(own, own_rows)
    halo_slice = pl.ds(pl.multiple_of(own + top, HALO), HALO)
    there_slice = pl.ds(there, HALO)
    high, low = pl.ds(X0 + width - 2, 2), pl.ds(X0, 2)
    high_ghost, low_ghost = pl.ds(X0 + width, 2), pl.ds(X0 - 2, 2)

    def material(n, planes_from, planes_to, rows_from, rows_to, device):
        return pltpu.make_async_remote_copy(
            ce.at[planes_from, rows_from], ce.at[planes_to, rows_to],
            mat_send.at[n], mat_recv.at[n], device_id=device, device_id_type=MESH,
        )

    go_right = [
        material(0, high, low_ghost, own_slice, own_slice, right),
        material(1, high, low_ghost, halo_slice, there_slice, right_across),
    ]
    go_left = [
        material(2, low, high_ghost, own_slice, own_slice, left),
        material(3, low, high_ghost, halo_slice, there_slice, left_across),
    ]

    def each(condition, action):
        @pl.when(condition)
        def _():
            action()

    def start_all(copies):
        for copy in copies:
            copy.start()

    loads[0].wait()
    loads[1].wait()
    for x in range(width):
        flags = mask[x].astype(jnp.float32)
        inv_eps = 1.0 / (1.0 + contrast * den[x] * flags)
        ce[X0 + x, own_slice, :] = inv_eps * gain1
        grad[x] = flags * contrast * inv_eps * inv_eps * step_dt
    halos[3].start()
    each(has_right, lambda: start_all(go_right))
    each(has_left, lambda: start_all(go_left))
    eye = lax.broadcasted_iota(jnp.int32, (own_rows, own_rows), 0) == lax.broadcasted_iota(
        jnp.int32, (own_rows, own_rows), 1
    )
    loads[4].wait()
    loads[6].wait()
    for s in range(2):
        spot = jnp.where(lanes == planes[s], gain1, 0.0)
        for x in range(width):
            row = jnp.broadcast_to(prof[s, x : x + 1, :], (own_rows, own_rows))
            column = jnp.sum(jnp.where(eye, row, 0.0), axis=1, keepdims=True)
            src[s, x, pl.ds(own, own_rows), :] = column * spot

    halos[2].start()
    signal(near, near_peers)
    loads[2].wait()
    loads[3].wait()
    loads[5].wait()
    for halo in halos:
        halo.wait()

    def to_right(s, w, k):
        return pltpu.make_async_remote_copy(
            send_h.at[s, w, k], recv_h.at[s, w, k],
            right_send.at[s, w, k], right_recv.at[s, w, k], device_id=right, device_id_type=MESH,
        )

    def to_left(s, w, k):
        return pltpu.make_async_remote_copy(
            send_e.at[s, w, k], recv_e.at[s, w, k],
            left_send.at[s, w, k], left_recv.at[s, w, k], device_id=left, device_id_type=MESH,
        )

    def up_z(f):
        return jnp.where(last_lane, 0.0, pltpu.roll(f, depth - 1, 1))

    def down_z(f):
        return jnp.where(first_lane, 0.0, pltpu.roll(f, 1, 1))

    def h_update(h_old, e, e_y, e_x, comps=(0, 1, 2)):
        new = {}
        if 0 in comps:
            new[0] = decay * h_old(0) - gain_half * ((e_y(2) - e[2]) - (up_z(e[1]) - e[1]))
        new[1] = decay * h_old(1) - (gain_half * (up_z(e[0]) - e[0]) - gain * (e_x[2] - e[2]))
        new[2] = decay * h_old(2) - (gain * (e_x[1] - e[1]) - gain_half * (e_y(0) - e[0]))
        return new

    def e_update(e_old, h, h_y, h_x, c, drive):
        cx = c * inv_spacing
        x = decay * e_old(0) + cx * ((h[2] - h_y(2)) - (h[1] - down_z(h[1])))
        if drive is not None:
            x = x - drive
        y = decay * e_old(1) + (cx * (h[0] - down_z(h[0])) - c * (h[2] - h_x[2]))
        z = decay * e_old(2) + (c * (h[1] - h_x[1]) - cx * (h[0] - h_y(0)))
        return {0: x, 1: y, 2: z}

    R0, R1 = slice(0, rows), slice(1, rows + 1)
    H0, HM = slice(HALO, HALO + rows), slice(HALO - 1, HALO + rows - 1)

    def free(s, w):
        for c in (1, 2):
            send_e[s, w, 0, c - 1] = we[s, c, X0, R0, :]
        each(has_left, lambda: to_left(s, w, 0).start())
        for k in range(WIN):
            last = k == WIN - 1
            h_planes = [x for x in range(width) if x >= k or x < width - 1 - k]
            if last:
                h_planes = [width - 1]
            for x in h_planes:
                if k == 0:
                    old_h = lambda c, x=x: wh[s, c, X0 + x, H0, :]
                    get_e = lambda c, x, r: we[s, c, X0 + x, r, :]
                else:
                    old_h = lambda c, x=x: fh[c, x + 1, H0, :]
                    get_e = lambda c, x, r: fe[c, x, r, :]
                e = {c: get_e(c, x, R0) for c in range(3)}
                e_x = {
                    c: (get_e(c, x + 1, R0) if x < width - 1 else jnp.zeros_like(e[c]))
                    for c in (1, 2)
                }
                new = h_update(
                    old_h, e, lambda c, x=x: get_e(c, x, R1), e_x, (1, 2) if last else (0, 1, 2)
                )
                if not last:
                    for c in range(3):
                        fh[c, x + 1, H0, :] = new[c]
                if x == width - 1:
                    send_h[s, w, k, 0] = new[1]
                    send_h[s, w, k, 1] = new[2]
            each(has_right, lambda: to_right(s, w, k).start())
            if last:
                break
            wave = waves[s, w * WIN + k]
            e_planes = [x for x in range(width) if x >= k + 1 or x < width - 1 - k]
            for x in e_planes:
                if k == 0:
                    old_e = lambda c, x=x: we[s, c, X0 + x, R0, :]
                else:
                    old_e = lambda c, x=x: fe[c, x, R0, :]
                h = {c: fh[c, x + 1, H0, :] for c in range(3)}
                h_x = {c: fh[c, x, H0, :] for c in (1, 2)}
                new = e_update(
                    old_e, h, lambda c, x=x: fh[c, x + 1, HM, :], h_x,
                    ce[X0 + x], src[s, x] * wave,
                )
                for c in range(3):
                    fe[c, x, R0, :] = new[c]
                if x == 0:
                    send_e[s, w, k + 1, 0] = new[1]
                    send_e[s, w, k + 1, 1] = new[2]
            each(has_left, lambda: to_left(s, w, k + 1).start())

    def true(s, w, relay):
        for c in range(3):
            for p in (X0 - 2, X0 - 1, X0 + width, X0 + width + 1):
                we[s, c, p, R0, :] = plane0
                wh[s, c, p, H0, :] = plane0
        for k in range(WIN):
            reach = min(k + 1, WIN - k)
            h_lo, h_hi = -reach, width + min(k, WIN - 1 - k)
            e_out_reach = min(k + 1, WIN - 1 - k)
            if k == WIN - 2:
                relay()
            each(has_right, lambda: to_left(s, w, k).wait_recv())
            e_next = None
            for x in range(h_hi - 1, h_lo - 1, -1):
                p = X0 + x
                e = {c: we[s, c, p, R0, :] for c in range(3)}
                if e_next is None:
                    e_x = {c: we[s, c, p + 1, R0, :] for c in (1, 2)}
                else:
                    e_x = e_next
                e_next = e
                if x == width - 1:
                    e_x = {c: (e_x[c] + recv_e[s, w, k, c - 1]) * on_right for c in (1, 2)}
                new = h_update(
                    lambda c: wh[s, c, p, H0, :], e, lambda c: we[s, c, p, R1, :], e_x
                )
                for c in range(3):
                    wh[s, c, p, H0, :] = new[c]
            each(has_left, lambda: to_right(s, w, k).wait_recv())
            wave = waves[s, w * WIN + k]
            h_last = None
            for x in range(-e_out_reach, width + e_out_reach):
                p = X0 + x
                h = {c: wh[s, c, p, H0, :] for c in range(3)}
                if h_last is None:
                    h_x = {c: wh[s, c, p - 1, H0, :] for c in (1, 2)}
                else:
                    h_x = h_last
                h_last = h
                if x == 0:
                    h_x = {c: (h_x[c] + recv_h[s, w, k, c - 1]) * on_left for c in (1, 2)}
                inside = 0 <= x < width
                new = e_update(
                    lambda c: we[s, c, p, R0, :], h, lambda c: wh[s, c, p, HM, :], h_x,
                    ce[p], src[s, x] * wave if inside else None,
                )
                for c in range(3):
                    we[s, c, p, R0, :] = new[c]
                    if inside:
                        hist[s, w * WIN + k, c, x] = new[c]

    def start_free(s, carry):
        free(s, 0)
        return carry

    lax.fori_loop(0, 2, start_free, 0)
    pl.semaphore_wait(near, len(near_peers))
    signal(mid, mid_peers)

    def wait_recvs(copies):
        for copy in copies:
            copy.wait_recv()

    def wait_sends(copies):
        for copy in copies:
            copy.wait_send()

    each(has_left, lambda: wait_recvs(go_right))
    each(has_right, lambda: wait_recvs(go_left))

    sum1 = [
        pltpu.make_async_remote_copy(
            part1.at[0], part1.at[1 + n], sum1_send.at[n], sum1_recv.at[n],
            device_id=peer, device_id_type=MESH,
        )
        for n, peer in enumerate(plane_peers)
    ]
    sum2 = [
        pltpu.make_async_remote_copy(
            part2.at[0], part2.at[1 + n], sum2_send.at[n], sum2_recv.at[n],
            device_id=peer, device_id_type=MESH,
        )
        for n, peer in enumerate(line_peers)
    ]
    def turn(j, carry):
        w, s = j // 2, lax.rem(j, 2)

        def add_plane():
            @pl.when(j == 3)
            def _():
                for copy in sum1:
                    copy.wait_recv()
                total = part1[0]
                for n in range(len(sum1)):
                    total = total + part1[1 + n]
                part2[0] = total
                for copy in sum2:
                    copy.start()

        true(s, w, add_plane)

        @pl.when(w == 0)
        def _():
            free(s, 1)

        @pl.when(j == 1)
        def _():
            pl.semaphore_wait(mid, len(mid_peers))
            signal(far, far_peers)

        @pl.when(j == 2)
        def _():
            pl.semaphore_wait(far, len(far_peers))
            total = jnp.zeros((own_rows, depth), jnp.float32)
            for c in range(3):
                for x in range(width):
                    e = we[0, c, X0 + x, pl.ds(own, own_rows), :]
                    total = total + e * e
            line = jnp.sum(total, axis=0, keepdims=True)
            part1[0] = jnp.where(lanes == planes[1], line, 0.0)
            for copy in sum1:
                copy.start()

        return carry

    lax.fori_loop(0, 2 * WINDOWS, turn, 0)

    for x in range(width):
        corr = jnp.zeros((own_rows, depth), jnp.float32)
        for k in range(STEPS):
            for c in range(3):
                corr = corr + (
                    hist[0, k, c, x, pl.ds(own, own_rows), :]
                    * hist[1, k, c, x, pl.ds(own, own_rows), :]
                )
        grad[x] = grad[x] * corr

    for copy in sum2:
        copy.wait_recv()
    total = part2[0]
    for n in range(len(sum2)):
        total = total + part2[1 + n]
    cells = count_x * width * lax.axis_size("gy") * own_rows
    power = jnp.sum(total, axis=1, keepdims=True) / cells
    scale = jnp.broadcast_to(1.0 / (power + small_eps), (own_rows, depth))
    for x in range(width):
        grad[x] = grad[x] * scale
    each(has_right, lambda: wait_sends(go_right))
    each(has_left, lambda: wait_sends(go_left))
    for copy in sum1 + sum2:
        copy.wait_send()

    def drain(j, carry):
        w, s = j // 2, lax.rem(j, 2)
        for k in range(WIN):
            each(has_right, lambda: to_right(s, w, k).wait_send())
            each(has_left, lambda: to_left(s, w, k).wait_send())
        return carry

    lax.fori_loop(0, 2 * WINDOWS, drain, 0)


def store(we, wh, grad, e_out, h_out, g_out, sem):
    width, own_rows = grad.shape[0], grad.shape[1]
    own = pl.multiple_of(lax.axis_index("gy") * HALO, HALO)
    block = pl.ds(LEFT, width)
    outs = [
        pltpu.make_async_copy(we.at[:, :, block, pl.ds(own, own_rows), :], e_out, sem.at[0]),
        pltpu.make_async_copy(wh.at[:, :, block, pl.ds(own + HALO, own_rows), :], h_out, sem.at[1]),
        pltpu.make_async_copy(grad, g_out, sem.at[2]),
    ]
    for out in outs:
        out.start()
    for out in outs:
        out.wait()


def vmem_array(shape):
    return pltpu.VMEM(shape, jnp.float32)


def in_vmem(x):
    return pltpu.with_memory_space_constraint(x, pltpu.VMEM)


def shards(electric, magnetic, density, design_mask, planes, profiles, waveforms):
    sets, comps, width, own_rows, depth = electric.shape
    rows = own_rows + HALO
    count_z = lax.axis_size("gx") // CHIPS_X
    f32 = jnp.float32
    vmem, dma = pltpu.VMEM, pltpu.SemaphoreType.DMA
    series = vmem((sets, WINDOWS, WIN, 2, rows, depth), f32)
    any_space = pl.BlockSpec(memory_space=pl.ANY)
    held = pl.BlockSpec(memory_space=pltpu.VMEM)
    smem, wait = pltpu.SMEM, pltpu.SemaphoreType.REGULAR
    frame = (sets, comps, FRAME, rows + HALO, depth)
    e_frame, h_frame, grad = pl.pallas_call(
        kernel,
        out_shape=(vmem_array(frame), vmem_array(frame), vmem_array(density.shape)),
        in_specs=[any_space] * 7,
        out_specs=(held,) * 3,
        scratch_shapes=[
            vmem((comps, width + 1, rows + HALO, depth), f32),
            vmem((comps, width + 1, rows + HALO, depth), f32),
            series, series, series, series,
            vmem((FRAME, rows, depth), f32),
            vmem((sets, width, rows, depth), f32),
            vmem((width, own_rows, depth), f32),
            vmem((width, own_rows, depth), jnp.int32),
            vmem((sets, STEPS, comps, width, rows, depth), f32),
            vmem((2 * CHIPS_X, 1, depth), f32),
            vmem((count_z, 1, depth), f32),
            smem(planes.shape, jnp.int32),
            smem(waveforms.shape, f32),
            vmem(profiles.shape, f32),
            dma((7,)), wait, wait, wait, dma((4,)), dma((4,)), dma((4,)), dma((4,)),
            dma((sets, WINDOWS, WIN)), dma((sets, WINDOWS, WIN)),
            dma((sets, WINDOWS, WIN)), dma((sets, WINDOWS, WIN)),
            dma((2 * CHIPS_X - 1,)), dma((2 * CHIPS_X - 1,)),
            dma((max(count_z - 1, 1),)), dma((max(count_z - 1, 1),)),
        ],
        compiler_params=pltpu.CompilerParams(
            collective_id=0, has_side_effects=True, vmem_limit_bytes=64_200_000
        ),
    )(planes, waveforms, profiles, electric, magnetic, density, design_mask)
    return pl.pallas_call(
        store,
        out_shape=(
            jax.ShapeDtypeStruct(electric.shape, f32),
            jax.ShapeDtypeStruct(magnetic.shape, f32),
            jax.ShapeDtypeStruct(density.shape, f32),
        ),
        in_specs=[held] * 3,
        out_specs=(any_space,) * 3,
        scratch_shapes=[dma((3,))],
        compiler_params=pltpu.CompilerParams(vmem_limit_bytes=4 << 20),
    )(in_vmem(e_frame), in_vmem(h_frame), in_vmem(grad))


def solution(mesh):
    return jax.shard_map(
        shards,
        mesh=mesh,
        in_specs=(
            P(None, None, CAND_GX, "gy", None),
            P(None, None, CAND_GX, "gy", None),
            P(CAND_GX, "gy", None),
            P(CAND_GX, "gy", None),
            P("cand"),
            P(None, CAND_GX, "gy"),
            P(None, "cand"),
        ),
        out_specs=(
            P(None, None, CAND_GX, "gy", None),
            P(None, None, CAND_GX, "gy", None),
            P(CAND_GX, "gy", None),
        ),
        check_vma=False,
    )
```

```python
import jax
import jax.numpy as jnp
from jax import lax
from jax.experimental import pallas as pl
from jax.experimental.pallas import tpu as pltpu
from jax.sharding import PartitionSpec as P

STEPS = 8
PMLW = 8
CAND_GX = ("cand", "gx")
CHIPS_X = 4
MESH = pl.DeviceIdType.MESH

step_dt = 0.7
contrast = 5.0
sigma_max = 2.0
small_eps = 1e-06
inv_spacing = 0.5

WIN = 4
WINDOWS = STEPS // WIN
LEFT = 3
FRAME = 9
HALO = 8


def kernel(
    planes_in, waves_in, prof_in, e_in, h_in, den_in, mask_in,
    we, wh, grad,
    fe, fh, pe, ph, send_h, send_e, recv_h, recv_e, ce, src, den, mask, hist, part1, part2,
    planes, waves, prof, load_sem, near, mid, far, halo_send, halo_recv, mat_send, mat_recv,
    right_send, right_recv, left_send, left_recv,
    sum1_send, sum1_recv, sum2_send, sum2_recv,
):
    width, own_rows = den.shape[0], den.shape[1]
    rows, depth = own_rows + HALO, den.shape[2]
    count_x = lax.axis_size("gx")
    count_z = count_x // CHIPS_X
    gx, gy = lax.axis_index("gx"), lax.axis_index("gy")
    chip_x, chip_z = gx // count_z, lax.rem(gx, count_z)
    other = 1 - gy
    right = {"gx": lax.rem(gx + 1, count_x), "gy": gy}
    left = {"gx": lax.rem(gx + count_x - 1, count_x), "gy": gy}
    across = {"gx": gx, "gy": other}
    right_across, left_across = dict(right, gy=other), dict(left, gy=other)
    has_right, has_left = gx < count_x - 1, gx > 0
    plane_peers = []
    for dx in range(CHIPS_X):
        for dc in range(2):
            if dx or dc:
                peer = lax.rem(chip_x + dx, CHIPS_X) * count_z + chip_z
                plane_peers.append({"gx": peer, "gy": other if dc else gy})

    def along_z(dz):
        return {"gx": chip_x * count_z + lax.rem(chip_z + dz, count_z), "gy": gy}

    def both_ways(d):
        return [along_z(dz) for dz in sorted({d % count_z, -d % count_z} - {0})]

    line_peers = [
        along_z(dz) for dz in sorted(range(1, count_z), key=lambda d: -min(d, count_z - d))
    ]
    next_chips = [
        {"gx": lax.rem(chip_x + dx, CHIPS_X) * count_z + chip_z, "gy": gy} for dx in (1, CHIPS_X - 1)
    ]
    own = pl.multiple_of(gy * HALO, HALO)
    top = pl.multiple_of((1 - gy) * (own_rows - HALO), HALO)
    there = pl.multiple_of(gy * own_rows, HALO)
    X0 = LEFT
    block = pl.ds(X0, width)

    early_rows = pl.ds(HALO, own_rows)
    loads = [
        pltpu.make_async_copy(den_in, den, load_sem.at[0]),
        pltpu.make_async_copy(mask_in, mask, load_sem.at[1]),
        pltpu.make_async_copy(e_in, we.at[:, :, block, pl.ds(own, own_rows), :], load_sem.at[2]),
        pltpu.make_async_copy(
            h_in, wh.at[:, :, block, pl.ds(own + HALO, own_rows), :], load_sem.at[3]
        ),
        pltpu.make_async_copy(planes_in, planes, load_sem.at[4]),
        pltpu.make_async_copy(waves_in, waves, load_sem.at[5]),
        pltpu.make_async_copy(prof_in, prof, load_sem.at[6]),
        pltpu.make_async_copy(e_in.at[0], pe.at[:, pl.ds(0, width), early_rows], load_sem.at[7]),
        pltpu.make_async_copy(h_in.at[0], ph.at[:, pl.ds(1, width), early_rows], load_sem.at[8]),
    ]
    for load in loads:
        load.start()

    def signal(semaphore, peers):
        for peer in peers:
            pl.semaphore_signal(semaphore, inc=1, device_id=peer, device_id_type=MESH)

    barrier = pltpu.get_barrier_semaphore()
    peers = [across, left, right, left_across, right_across] + next_chips + both_ways(1)
    near_peers = next_chips + both_ways(1)
    mid_peers = next_chips + both_ways(2)
    far_peers = both_ways(4)
    signal(barrier, peers)

    lanes = lax.broadcasted_iota(jnp.int32, (1, depth), 1)
    zpos = lanes.astype(jnp.float32)
    lower = (PMLW - zpos - 0.5) / PMLW
    upper = (zpos + 0.5 - (depth - PMLW)) / PMLW
    deep = jnp.maximum(jnp.maximum(lower, upper), 0.0)
    half = sigma_max * deep * deep * deep * step_dt / 2.0
    decay1 = (1.0 - half) / (1.0 + half)
    gain1 = step_dt / (1.0 + half)
    gain_half1 = gain1 * inv_spacing
    on_left = has_left.astype(jnp.float32)
    on_right = has_right.astype(jnp.float32)

    pad = jnp.zeros((HALO, depth), jnp.float32)
    plane0 = jnp.zeros((rows, depth), jnp.float32)
    for s in range(2):
        for c in range(3):
            for p in range(FRAME):
                if c != 1:
                    we[s, c, p, rows : rows + HALO, :] = pad
                    wh[s, c, p, 0:HALO, :] = pad
            wh[s, c, 0, HALO:, :] = plane0
    for c in (0, 2):
        for p in range(width + 1):
            fe[c, p, rows : rows + HALO, :] = pad
            fh[c, p, 0:HALO, :] = pad
            pe[c, p, rows : rows + HALO, :] = pad
            ph[c, p, 0:HALO, :] = pad
    for c in range(3):
        fe[c, width, 0:rows, :] = plane0
        fh[c, 0, HALO:, :] = plane0
        ph[c, 0, HALO:, :] = plane0

    @pl.when(jnp.logical_not(has_right))
    def _():
        recv_e[...] = jnp.zeros_like(recv_e)
        for p in (X0 + width, X0 + width + 1):
            ce[p] = plane0

    @pl.when(jnp.logical_not(has_left))
    def _():
        recv_h[...] = jnp.zeros_like(recv_h)
        for p in (X0 - 2, X0 - 1):
            ce[p] = plane0

    pl.semaphore_wait(barrier, len(peers))
    signal(near, near_peers)

    def halo(n, source, target):
        return pltpu.make_async_remote_copy(
            source, target, halo_send.at[n], halo_recv.at[n],
            device_id=across, device_id_type=MESH,
        )

    own_slice = pl.ds(own, own_rows)
    halo_slice = pl.ds(pl.multiple_of(own + top, HALO), HALO)
    there_slice = pl.ds(there, HALO)
    e_halos = [
        halo(s, e_in.at[s, :, :, pl.ds(top, HALO), :], we.at[s, :, block, there_slice, :])
        for s in range(2)
    ]
    h_halos = [
        halo(
            2 + s, h_in.at[s, :, :, pl.ds(top, HALO), :],
            wh.at[s, :, block, pl.ds(there + HALO, HALO), :],
        )
        for s in range(2)
    ]
    src_halo = halo(4, src.at[:, :, halo_slice, :], src.at[:, :, there_slice, :])
    ce_halo = halo(5, ce.at[block, halo_slice, :], ce.at[block, there_slice, :])
    for s in range(2):
        e_halos[s].start()
        h_halos[s].start()

    high, low = pl.ds(X0 + width - 2, 2), pl.ds(X0, 2)
    high_ghost, low_ghost = pl.ds(X0 + width, 2), pl.ds(X0 - 2, 2)

    def material(n, planes_from, planes_to, rows_from, rows_to, device):
        return pltpu.make_async_remote_copy(
            ce.at[planes_from, rows_from], ce.at[planes_to, rows_to],
            mat_send.at[n], mat_recv.at[n], device_id=device, device_id_type=MESH,
        )

    go_right = [
        material(0, high, low_ghost, own_slice, own_slice, right),
        material(1, high, low_ghost, halo_slice, there_slice, right_across),
    ]
    go_left = [
        material(2, low, high_ghost, own_slice, own_slice, left),
        material(3, low, high_ghost, halo_slice, there_slice, left_across),
    ]

    def each(condition, action):
        @pl.when(condition)
        def _():
            action()

    def start_all(copies):
        for copy in copies:
            copy.start()

    loads[0].wait()
    loads[1].wait()
    for x in range(width):
        flags = mask[x].astype(jnp.float32)
        inv_eps = 1.0 / (1.0 + contrast * den[x] * flags)
        ce[X0 + x, own_slice, :] = inv_eps * gain1
        grad[x] = flags * contrast * inv_eps * inv_eps * step_dt
    ce_halo.start()
    each(has_right, lambda: start_all(go_right))
    each(has_left, lambda: start_all(go_left))
    eye = lax.broadcasted_iota(jnp.int32, (own_rows, own_rows), 0) == lax.broadcasted_iota(
        jnp.int32, (own_rows, own_rows), 1
    )
    loads[4].wait()
    loads[6].wait()
    for s in range(2):
        spot = jnp.where(lanes == planes[s], gain1, 0.0)
        for x in range(width):
            row = jnp.broadcast_to(prof[s, x : x + 1, :], (own_rows, own_rows))
            column = jnp.sum(jnp.where(eye, row, 0.0), axis=1, keepdims=True)
            src[s, x, pl.ds(own, own_rows), :] = column * spot

    src_halo.start()
    loads[5].wait()
    loads[7].wait()
    loads[8].wait()
    def spread(row, n):
        return jnp.broadcast_to(row, (n, depth))

    def up_z(f):
        return jnp.where(spread(lanes == depth - 1, f.shape[0]), 0.0, pltpu.roll(f, depth - 1, 1))

    def down_z(f):
        return jnp.where(spread(lanes == 0, f.shape[0]), 0.0, pltpu.roll(f, 1, 1))

    def h_update(h_old, e, e_y, e_x, comps=(0, 1, 2)):
        decay, gain, gain_half = (spread(r, e[0].shape[0]) for r in (decay1, gain1, gain_half1))
        new = {}
        if 0 in comps:
            new[0] = decay * h_old(0) - gain_half * ((e_y(2) - e[2]) - (up_z(e[1]) - e[1]))
        new[1] = decay * h_old(1) - (gain_half * (up_z(e[0]) - e[0]) - gain * (e_x[2] - e[2]))
        new[2] = decay * h_old(2) - (gain * (e_x[1] - e[1]) - gain_half * (e_y(0) - e[0]))
        return new

    def e_update(e_old, h, h_y, h_x, c, drive):
        decay = spread(decay1, h[0].shape[0])
        cx = c * inv_spacing
        x = decay * e_old(0) + cx * ((h[2] - h_y(2)) - (h[1] - down_z(h[1])))
        if drive is not None:
            x = x - drive
        y = decay * e_old(1) + (cx * (h[0] - down_z(h[0])) - c * (h[2] - h_x[2]))
        z = decay * e_old(2) + (c * (h[1] - h_x[1]) - cx * (h[0] - h_y(0)))
        return {0: x, 1: y, 2: z}

    def run_free(first, rest, put_left, put_right, material_of, drive_of):
        put_left(0, first.e(1, 0, 0), first.e(2, 0, 0))
        for k in range(WIN):
            last = k == WIN - 1
            now = first if k == 0 else rest
            h_planes = [x for x in range(width) if x >= k or x < width - 1 - k]
            if last:
                h_planes = [width - 1]
            for x in h_planes:
                e = {c: now.e(c, x, 0) for c in range(3)}
                e_x = {
                    c: (now.e(c, x + 1, 0) if x < width - 1 else jnp.zeros_like(e[c]))
                    for c in (1, 2)
                }
                new = h_update(
                    lambda c: now.h(c, x, 0), e, lambda c: now.e(c, x, 1), e_x,
                    (1, 2) if last else (0, 1, 2),
                )
                if not last:
                    for c in range(3):
                        rest.set_h(c, x, new[c])
                if x == width - 1:
                    edge = new
            put_right(k, edge[1], edge[2])
            if last:
                break
            for x in [x for x in range(width) if x >= k + 1 or x < width - 1 - k]:
                h = {c: rest.h(c, x, 0) for c in range(3)}
                h_x = {c: rest.h(c, x - 1, 0) for c in (1, 2)}
                new = e_update(
                    lambda c: now.e(c, x, 0), h, lambda c: rest.h(c, x, -1), h_x,
                    material_of(x), drive_of(x, k),
                )
                for c in range(3):
                    rest.set_e(c, x, new[c])
                if x == 0:
                    edge = new
            put_left(k + 1, edge[1], edge[2])

    class Fields:
        def __init__(self, e_ref, h_ref, e_x, h_x, e_row, h_row, n):
            self.e_ref, self.h_ref, self.e_x, self.h_x = e_ref, h_ref, e_x, h_x
            self.e_row, self.h_row, self.n = e_row, h_row, n

        def e(self, c, x, dy):
            return self.e_ref[c, self.e_x + x, self.e_row + dy : self.e_row + dy + self.n, :]

        def h(self, c, x, dy):
            return self.h_ref[c, self.h_x + x, self.h_row + dy : self.h_row + dy + self.n, :]

        def set_e(self, c, x, value):
            self.e_ref[c, self.e_x + x, self.e_row : self.e_row + self.n, :] = value

        def set_h(self, c, x, value):
            self.h_ref[c, self.h_x + x, self.h_row : self.h_row + self.n, :] = value

    def to_side(go_right, s, w, k, spare=None, part=None):
        source, target = (send_h, recv_h) if go_right else (send_e, recv_e)
        source, target = source.at[s, w if spare is None else spare, k], target.at[s, w, k]
        if part is not None:
            source, target = source.at[:, part], target.at[:, part]
        send, recv = (right_send, right_recv) if go_right else (left_send, left_recv)
        return pltpu.make_async_remote_copy(
            source, target, send.at[s, w, k], recv.at[s, w, k],
            device_id=right if go_right else left, device_id_type=MESH,
        )

    far_rows = pl.ds(pl.multiple_of(gy * 2 * HALO, HALO), own_rows - HALO)
    near_rows = pl.ds(pl.multiple_of((1 - gy) * (own_rows - HALO), HALO), 2 * HALO)

    def early():
        fields = Fields(pe, ph, 0, 1, HALO, HALO, own_rows)

        def put(go_right, k, y, z):
            buffer = send_h if go_right else send_e
            buffer[0, WINDOWS, k, 0, own_slice, :] = y
            buffer[0, WINDOWS, k, 1, own_slice, :] = z
            each(
                has_right if go_right else has_left,
                lambda: to_side(go_right, 0, 0, k, WINDOWS, far_rows).start(),
            )

        run_free(
            fields, fields,
            lambda k, y, z: put(False, k, y, z), lambda k, y, z: put(True, k, y, z),
            lambda x: ce[X0 + x, own_slice, :],
            lambda x, k: src[0, x, own_slice, :] * waves[0, k],
        )

    def free(s, w):
        def put(go_right, k, y, z):
            buffer = send_h if go_right else send_e
            buffer[s, w, k, 0] = y
            buffer[s, w, k, 1] = z
            there_is = has_right if go_right else has_left
            if w == 0:
                each(
                    jnp.logical_and(there_is, s == 0),
                    lambda: to_side(go_right, s, w, k, None, near_rows).start(),
                )
                each(
                    jnp.logical_and(there_is, s != 0),
                    lambda: to_side(go_right, s, w, k).start(),
                )
            else:
                each(there_is, lambda: to_side(go_right, s, w, k).start())

        run_free(
            Fields(we.at[s], wh.at[s], X0, X0, 0, HALO, rows),
            Fields(fe, fh, 0, 1, 0, HALO, rows),
            lambda k, y, z: put(False, k, y, z), lambda k, y, z: put(True, k, y, z),
            lambda x: ce[X0 + x],
            lambda x, k: src[s, x] * waves[s, w * WIN + k],
        )

    H0, HM = slice(HALO, HALO + rows), slice(HALO - 1, HALO + rows - 1)
    R0, R1 = slice(0, rows), slice(1, rows + 1)

    def true(s, w, relay):
        for c in range(3):
            for p in (X0 - 2, X0 - 1, X0 + width, X0 + width + 1):
                we[s, c, p, R0, :] = plane0
                wh[s, c, p, H0, :] = plane0
        for k in range(WIN):
            reach = min(k + 1, WIN - k)
            h_lo, h_hi = -reach, width + min(k, WIN - 1 - k)
            e_out_reach = min(k + 1, WIN - 1 - k)
            if k == WIN - 2:
                relay()
            each(has_right, lambda: to_side(False, s, w, k).wait_recv())
            e_next = None
            for x in range(h_hi - 1, h_lo - 1, -1):
                p = X0 + x
                e = {c: we[s, c, p, R0, :] for c in range(3)}
                if e_next is None:
                    e_x = {c: we[s, c, p + 1, R0, :] for c in (1, 2)}
                else:
                    e_x = e_next
                e_next = e
                if x == width - 1:
                    e_x = {c: (e_x[c] + recv_e[s, w, k, c - 1]) * on_right for c in (1, 2)}
                new = h_update(
                    lambda c: wh[s, c, p, H0, :], e, lambda c: we[s, c, p, R1, :], e_x
                )
                for c in range(3):
                    wh[s, c, p, H0, :] = new[c]
            each(has_left, lambda: to_side(True, s, w, k).wait_recv())
            wave = waves[s, w * WIN + k]
            h_last = None
            for x in range(-e_out_reach, width + e_out_reach):
                p = X0 + x
                h = {c: wh[s, c, p, H0, :] for c in range(3)}
                if h_last is None:
                    h_x = {c: wh[s, c, p - 1, H0, :] for c in (1, 2)}
                else:
                    h_x = h_last
                h_last = h
                if x == 0:
                    h_x = {c: (h_x[c] + recv_h[s, w, k, c - 1]) * on_left for c in (1, 2)}
                inside = 0 <= x < width
                new = e_update(
                    lambda c: we[s, c, p, R0, :], h, lambda c: wh[s, c, p, HM, :], h_x,
                    ce[p], src[s, x] * wave if inside else None,
                )
                for c in range(3):
                    we[s, c, p, R0, :] = new[c]
                    if inside:
                        hist[s, w * WIN + k, c, x] = new[c]

    early()
    loads[2].wait()
    loads[3].wait()
    src_halo.wait()
    ce_halo.wait()
    e_halos[0].wait()
    h_halos[0].wait()

    def start_free(s, carry):
        @pl.when(s == 1)
        def _():
            e_halos[1].wait()
            h_halos[1].wait()

        free(s, 0)
        return carry

    pl.semaphore_wait(near, len(near_peers))
    signal(mid, mid_peers)
    lax.fori_loop(0, 2, start_free, 0)

    def wait_recvs(copies):
        for copy in copies:
            copy.wait_recv()

    def wait_sends(copies):
        for copy in copies:
            copy.wait_send()

    each(has_left, lambda: wait_recvs(go_right))
    each(has_right, lambda: wait_recvs(go_left))

    sum1 = [
        pltpu.make_async_remote_copy(
            part1.at[0], part1.at[1 + n], sum1_send.at[n], sum1_recv.at[n],
            device_id=peer, device_id_type=MESH,
        )
        for n, peer in enumerate(plane_peers)
    ]
    sum2 = [
        pltpu.make_async_remote_copy(
            part2.at[0], part2.at[1 + n], sum2_send.at[n], sum2_recv.at[n],
            device_id=peer, device_id_type=MESH,
        )
        for n, peer in enumerate(line_peers)
    ]
    def turn(j, carry):
        w, s = j // 2, lax.rem(j, 2)

        def add_plane():
            @pl.when(j == 3)
            def _():
                for copy in sum1:
                    copy.wait_recv()
                total = part1[0]
                for n in range(len(sum1)):
                    total = total + part1[1 + n]
                part2[0] = total
                for copy in sum2:
                    copy.start()

        true(s, w, add_plane)

        @pl.when(w == 0)
        def _():
            free(s, 1)

        @pl.when(j == 0)
        def _():
            pl.semaphore_wait(mid, len(mid_peers))
            signal(far, far_peers)

        @pl.when(j == 2)
        def _():
            pl.semaphore_wait(far, len(far_peers))
            total = jnp.zeros((own_rows, depth), jnp.float32)
            for c in range(3):
                for x in range(width):
                    e = we[0, c, X0 + x, pl.ds(own, own_rows), :]
                    total = total + e * e
            line = jnp.sum(total, axis=0, keepdims=True)
            part1[0] = jnp.where(lanes == planes[1], line, 0.0)
            for copy in sum1:
                copy.start()

        return carry

    lax.fori_loop(0, 2 * WINDOWS, turn, 0)

    for x in range(width):
        corr = jnp.zeros((own_rows, depth), jnp.float32)
        for k in range(STEPS):
            for c in range(3):
                corr = corr + (
                    hist[0, k, c, x, pl.ds(own, own_rows), :]
                    * hist[1, k, c, x, pl.ds(own, own_rows), :]
                )
        grad[x] = grad[x] * corr

    each(has_right, lambda: wait_sends(go_right))
    each(has_left, lambda: wait_sends(go_left))
    for copy in sum1 + sum2:
        copy.wait_send()

    def drain(j, carry):
        w, s = j // 2, lax.rem(j, 2)
        for k in range(WIN):
            each(has_right, lambda: to_side(True, s, w, k).wait_send())
            each(has_left, lambda: to_side(False, s, w, k).wait_send())
        return carry

    lax.fori_loop(0, 2 * WINDOWS, drain, 0)

    for copy in sum2:
        copy.wait_recv()
    total = part2[0]
    for n in range(len(sum2)):
        total = total + part2[1 + n]
    cells = count_x * width * lax.axis_size("gy") * own_rows
    power = jnp.sum(total, axis=1, keepdims=True) / cells
    scale = jnp.broadcast_to(1.0 / (power + small_eps), (own_rows, depth))
    for x in range(width):
        grad[x] = grad[x] * scale


def store(we, wh, grad, e_out, h_out, g_out, sem):
    width, own_rows = grad.shape[0], grad.shape[1]
    own = pl.multiple_of(lax.axis_index("gy") * HALO, HALO)
    block = pl.ds(LEFT, width)
    outs = [
        pltpu.make_async_copy(we.at[:, :, block, pl.ds(own, own_rows), :], e_out, sem.at[0]),
        pltpu.make_async_copy(wh.at[:, :, block, pl.ds(own + HALO, own_rows), :], h_out, sem.at[1]),
        pltpu.make_async_copy(grad, g_out, sem.at[2]),
    ]
    for out in outs:
        out.start()
    for out in outs:
        out.wait()


def vmem_array(shape):
    return pltpu.VMEM(shape, jnp.float32)


def in_vmem(x):
    return pltpu.with_memory_space_constraint(x, pltpu.VMEM)


def shards(electric, magnetic, density, design_mask, planes, profiles, waveforms):
    sets, comps, width, own_rows, depth = electric.shape
    rows = own_rows + HALO
    count_z = lax.axis_size("gx") // CHIPS_X
    f32 = jnp.float32
    vmem, dma = pltpu.VMEM, pltpu.SemaphoreType.DMA
    came = vmem((sets, WINDOWS, WIN, 2, rows, depth), f32)
    sent = vmem((sets, WINDOWS + 1, WIN, 2, rows, depth), f32)
    any_space = pl.BlockSpec(memory_space=pl.ANY)
    held = pl.BlockSpec(memory_space=pltpu.VMEM)
    smem, wait = pltpu.SMEM, pltpu.SemaphoreType.REGULAR
    frame = (sets, comps, FRAME, rows + HALO, depth)
    e_frame, h_frame, grad = pl.pallas_call(
        kernel,
        out_shape=(vmem_array(frame), vmem_array(frame), vmem_array(density.shape)),
        in_specs=[any_space] * 7,
        out_specs=(held,) * 3,
        scratch_shapes=[
            *[vmem((comps, width + 1, rows + HALO, depth), f32)] * 4,
            sent, sent, came, came,
            vmem((FRAME, rows, depth), f32),
            vmem((sets, width, rows, depth), f32),
            vmem((width, own_rows, depth), f32),
            vmem((width, own_rows, depth), jnp.int32),
            vmem((sets, STEPS, comps, width, rows, depth), f32),
            vmem((2 * CHIPS_X, 1, depth), f32),
            vmem((count_z, 1, depth), f32),
            smem(planes.shape, jnp.int32),
            smem(waveforms.shape, f32),
            vmem(profiles.shape, f32),
            dma((9,)), wait, wait, wait, dma((6,)), dma((6,)), dma((4,)), dma((4,)),
            dma((sets, WINDOWS, WIN)), dma((sets, WINDOWS, WIN)),
            dma((sets, WINDOWS, WIN)), dma((sets, WINDOWS, WIN)),
            dma((2 * CHIPS_X - 1,)), dma((2 * CHIPS_X - 1,)),
            dma((max(count_z - 1, 1),)), dma((max(count_z - 1, 1),)),
        ],
        compiler_params=pltpu.CompilerParams(
            collective_id=0, has_side_effects=True, vmem_limit_bytes=64_200_000
        ),
    )(planes, waveforms, profiles, electric, magnetic, density, design_mask)
    return pl.pallas_call(
        store,
        out_shape=(
            jax.ShapeDtypeStruct(electric.shape, f32),
            jax.ShapeDtypeStruct(magnetic.shape, f32),
            jax.ShapeDtypeStruct(density.shape, f32),
        ),
        in_specs=[held] * 3,
        out_specs=(any_space,) * 3,
        scratch_shapes=[dma((3,))],
        compiler_params=pltpu.CompilerParams(vmem_limit_bytes=4 << 20),
    )(in_vmem(e_frame), in_vmem(h_frame), in_vmem(grad))


def solution(mesh):
    return jax.shard_map(
        shards,
        mesh=mesh,
        in_specs=(
            P(None, None, CAND_GX, "gy", None),
            P(None, None, CAND_GX, "gy", None),
            P(CAND_GX, "gy", None),
            P(CAND_GX, "gy", None),
            P("cand"),
            P(None, CAND_GX, "gy"),
            P(None, "cand"),
        ),
        out_specs=(
            P(None, None, CAND_GX, "gy", None),
            P(None, None, CAND_GX, "gy", None),
            P(CAND_GX, "gy", None),
        ),
        check_vma=False,
    )
```

```python
import jax
import jax.numpy as jnp
from jax import lax
from jax.experimental import pallas as pl
from jax.experimental.pallas import tpu as pltpu
from jax.sharding import PartitionSpec as P

STEPS = 8
PMLW = 8
CAND_GX = ("cand", "gx")
CHIPS_X = 4
MESH = pl.DeviceIdType.MESH

step_dt = 0.7
contrast = 5.0
sigma_max = 2.0
small_eps = 1e-06
inv_spacing = 0.5

WIN = 4
WINDOWS = STEPS // WIN
LEFT = 3
FRAME = 9
HALO = 8


def kernel(
    planes_in, waves_in, prof_in, e_in, h_in, den_in, mask_in,
    we, wh, grad,
    fe, fh, pe, ph, send_h, send_e, recv_h, recv_e, ce, src, den, mask, hist, part1, part2,
    planes, waves, prof, load_sem, near, mid, far, halo_send, halo_recv, mat_send, mat_recv,
    right_send, right_recv, left_send, left_recv,
    sum1_send, sum1_recv, sum2_send, sum2_recv,
):
    width, own_rows = den.shape[0], den.shape[1]
    rows, depth = own_rows + HALO, den.shape[2]
    count_x = lax.axis_size("gx")
    count_z = count_x // CHIPS_X
    gx, gy = lax.axis_index("gx"), lax.axis_index("gy")
    chip_x, chip_z = gx // count_z, lax.rem(gx, count_z)
    other = 1 - gy
    right = {"gx": lax.rem(gx + 1, count_x), "gy": gy}
    left = {"gx": lax.rem(gx + count_x - 1, count_x), "gy": gy}
    across = {"gx": gx, "gy": other}
    right_across, left_across = dict(right, gy=other), dict(left, gy=other)
    has_right, has_left = gx < count_x - 1, gx > 0
    plane_peers = []
    for dx in range(CHIPS_X):
        for dc in range(2):
            if dx or dc:
                peer = lax.rem(chip_x + dx, CHIPS_X) * count_z + chip_z
                plane_peers.append({"gx": peer, "gy": other if dc else gy})

    def along_z(dz):
        return {"gx": chip_x * count_z + lax.rem(chip_z + dz, count_z), "gy": gy}

    def both_ways(d):
        return [along_z(dz) for dz in sorted({d % count_z, -d % count_z} - {0})]

    line_peers = [
        along_z(dz) for dz in sorted(range(1, count_z), key=lambda d: -min(d, count_z - d))
    ]
    next_chips = [
        {"gx": lax.rem(chip_x + dx, CHIPS_X) * count_z + chip_z, "gy": gy} for dx in (1, CHIPS_X - 1)
    ]
    own = pl.multiple_of(gy * HALO, HALO)
    top = pl.multiple_of((1 - gy) * (own_rows - HALO), HALO)
    there = pl.multiple_of(gy * own_rows, HALO)
    X0 = LEFT
    block = pl.ds(X0, width)

    early_rows = pl.ds(HALO, own_rows)
    loads = [
        pltpu.make_async_copy(den_in, den, load_sem.at[0]),
        pltpu.make_async_copy(mask_in, mask, load_sem.at[1]),
        pltpu.make_async_copy(e_in, we.at[:, :, block, pl.ds(own, own_rows), :], load_sem.at[2]),
        pltpu.make_async_copy(
            h_in, wh.at[:, :, block, pl.ds(own + HALO, own_rows), :], load_sem.at[3]
        ),
        pltpu.make_async_copy(planes_in, planes, load_sem.at[4]),
        pltpu.make_async_copy(waves_in, waves, load_sem.at[5]),
        pltpu.make_async_copy(prof_in, prof, load_sem.at[6]),
        pltpu.make_async_copy(e_in.at[0], pe.at[:, pl.ds(0, width), early_rows], load_sem.at[7]),
        pltpu.make_async_copy(h_in.at[0], ph.at[:, pl.ds(1, width), early_rows], load_sem.at[8]),
    ]
    for load in loads:
        load.start()

    def signal(semaphore, peers):
        for peer in peers:
            pl.semaphore_signal(semaphore, inc=1, device_id=peer, device_id_type=MESH)

    barrier = pltpu.get_barrier_semaphore()
    peers = [across, left, right, left_across, right_across] + next_chips + both_ways(1)
    near_peers = next_chips + both_ways(1)
    mid_peers = next_chips + both_ways(2)
    far_peers = both_ways(4)
    signal(barrier, peers)

    lanes = lax.broadcasted_iota(jnp.int32, (1, depth), 1)
    zpos = lanes.astype(jnp.float32)
    lower = (PMLW - zpos - 0.5) / PMLW
    upper = (zpos + 0.5 - (depth - PMLW)) / PMLW
    deep = jnp.maximum(jnp.maximum(lower, upper), 0.0)
    half = sigma_max * deep * deep * deep * step_dt / 2.0
    decay1 = (1.0 - half) / (1.0 + half)
    gain1 = step_dt / (1.0 + half)
    gain_half1 = gain1 * inv_spacing
    on_left = has_left.astype(jnp.float32)
    on_right = has_right.astype(jnp.float32)

    pad = jnp.zeros((HALO, depth), jnp.float32)
    plane0 = jnp.zeros((rows, depth), jnp.float32)
    for s in range(2):
        for c in range(3):
            for p in range(FRAME):
                if c != 1:
                    we[s, c, p, rows : rows + HALO, :] = pad
                    wh[s, c, p, 0:HALO, :] = pad
            wh[s, c, 0, HALO:, :] = plane0
    for c in (0, 2):
        for p in range(width + 1):
            fe[c, p, rows : rows + HALO, :] = pad
            fh[c, p, 0:HALO, :] = pad
            pe[c, p, rows : rows + HALO, :] = pad
            ph[c, p, 0:HALO, :] = pad
    for c in range(3):
        fe[c, width, 0:rows, :] = plane0
        fh[c, 0, HALO:, :] = plane0
        ph[c, 0, HALO:, :] = plane0

    @pl.when(jnp.logical_not(has_right))
    def _():
        recv_e[...] = jnp.zeros_like(recv_e)
        for p in (X0 + width, X0 + width + 1):
            ce[p] = plane0

    @pl.when(jnp.logical_not(has_left))
    def _():
        recv_h[...] = jnp.zeros_like(recv_h)
        for p in (X0 - 2, X0 - 1):
            ce[p] = plane0

    pl.semaphore_wait(barrier, len(peers))
    signal(near, near_peers)

    def halo(n, source, target):
        return pltpu.make_async_remote_copy(
            source, target, halo_send.at[n], halo_recv.at[n],
            device_id=across, device_id_type=MESH,
        )

    own_slice = pl.ds(own, own_rows)
    halo_slice = pl.ds(pl.multiple_of(own + top, HALO), HALO)
    there_slice = pl.ds(there, HALO)
    e_halos = [
        halo(s, e_in.at[s, :, :, pl.ds(top, HALO), :], we.at[s, :, block, there_slice, :])
        for s in range(2)
    ]
    h_halos = [
        halo(
            2 + s, h_in.at[s, :, :, pl.ds(top, HALO), :],
            wh.at[s, :, block, pl.ds(there + HALO, HALO), :],
        )
        for s in range(2)
    ]
    src_halo = halo(4, src.at[:, :, halo_slice, :], src.at[:, :, there_slice, :])
    ce_halo = halo(5, ce.at[block, halo_slice, :], ce.at[block, there_slice, :])
    for s in range(2):
        e_halos[s].start()
        h_halos[s].start()

    high, low = pl.ds(X0 + width - 2, 2), pl.ds(X0, 2)
    high_ghost, low_ghost = pl.ds(X0 + width, 2), pl.ds(X0 - 2, 2)

    def material(n, planes_from, planes_to, rows_from, rows_to, device):
        return pltpu.make_async_remote_copy(
            ce.at[planes_from, rows_from], ce.at[planes_to, rows_to],
            mat_send.at[n], mat_recv.at[n], device_id=device, device_id_type=MESH,
        )

    go_right = [
        material(0, high, low_ghost, own_slice, own_slice, right),
        material(1, high, low_ghost, halo_slice, there_slice, right_across),
    ]
    go_left = [
        material(2, low, high_ghost, own_slice, own_slice, left),
        material(3, low, high_ghost, halo_slice, there_slice, left_across),
    ]

    def each(condition, action):
        @pl.when(condition)
        def _():
            action()

    def start_all(copies):
        for copy in copies:
            copy.start()

    loads[0].wait()
    loads[1].wait()
    for x in range(width):
        flags = mask[x].astype(jnp.float32)
        inv_eps = 1.0 / (1.0 + contrast * den[x] * flags)
        ce[X0 + x, own_slice, :] = inv_eps * gain1
        grad[x] = flags * contrast * inv_eps * inv_eps * step_dt
    ce_halo.start()
    each(has_right, lambda: start_all(go_right))
    each(has_left, lambda: start_all(go_left))
    eye = lax.broadcasted_iota(jnp.int32, (own_rows, own_rows), 0) == lax.broadcasted_iota(
        jnp.int32, (own_rows, own_rows), 1
    )
    loads[4].wait()
    loads[6].wait()
    for s in range(2):
        spot = jnp.where(lanes == planes[s], gain1, 0.0)
        for x in range(width):
            row = jnp.broadcast_to(prof[s, x : x + 1, :], (own_rows, own_rows))
            column = jnp.sum(jnp.where(eye, row, 0.0), axis=1, keepdims=True)
            src[s, x, pl.ds(own, own_rows), :] = column * spot

    src_halo.start()
    loads[5].wait()
    loads[7].wait()
    loads[8].wait()
    def spread(row, n):
        return jnp.broadcast_to(row, (n, depth))

    def up_z(f):
        return jnp.where(spread(lanes == depth - 1, f.shape[0]), 0.0, pltpu.roll(f, depth - 1, 1))

    def down_z(f):
        return jnp.where(spread(lanes == 0, f.shape[0]), 0.0, pltpu.roll(f, 1, 1))

    def h_update(h_old, e, e_y, e_x, comps=(0, 1, 2)):
        decay, gain, gain_half = (spread(r, e[0].shape[0]) for r in (decay1, gain1, gain_half1))
        new = {}
        if 0 in comps:
            new[0] = decay * h_old(0) - gain_half * ((e_y(2) - e[2]) - (up_z(e[1]) - e[1]))
        new[1] = decay * h_old(1) - (gain_half * (up_z(e[0]) - e[0]) - gain * (e_x[2] - e[2]))
        new[2] = decay * h_old(2) - (gain * (e_x[1] - e[1]) - gain_half * (e_y(0) - e[0]))
        return new

    def e_update(e_old, h, h_y, h_x, c, drive):
        decay = spread(decay1, h[0].shape[0])
        cx = c * inv_spacing
        x = decay * e_old(0) + cx * ((h[2] - h_y(2)) - (h[1] - down_z(h[1])))
        if drive is not None:
            x = x - drive
        y = decay * e_old(1) + (cx * (h[0] - down_z(h[0])) - c * (h[2] - h_x[2]))
        z = decay * e_old(2) + (c * (h[1] - h_x[1]) - cx * (h[0] - h_y(0)))
        return {0: x, 1: y, 2: z}

    def run_free(first, rest, put_left, put_right, material_of, drive_of):
        put_left(0, first.e(1, 0, 0), first.e(2, 0, 0))
        for k in range(WIN):
            last = k == WIN - 1
            now = first if k == 0 else rest
            h_planes = [x for x in range(width) if x >= k or x < width - 1 - k]
            if last:
                h_planes = [width - 1]
            for x in h_planes:
                e = {c: now.e(c, x, 0) for c in range(3)}
                e_x = {
                    c: (now.e(c, x + 1, 0) if x < width - 1 else jnp.zeros_like(e[c]))
                    for c in (1, 2)
                }
                new = h_update(
                    lambda c: now.h(c, x, 0), e, lambda c: now.e(c, x, 1), e_x,
                    (1, 2) if last else (0, 1, 2),
                )
                if not last:
                    for c in range(3):
                        rest.set_h(c, x, new[c])
                if x == width - 1:
                    edge = new
            put_right(k, edge[1], edge[2])
            if last:
                break
            for x in [x for x in range(width) if x >= k + 1 or x < width - 1 - k]:
                h = {c: rest.h(c, x, 0) for c in range(3)}
                h_x = {c: rest.h(c, x - 1, 0) for c in (1, 2)}
                new = e_update(
                    lambda c: now.e(c, x, 0), h, lambda c: rest.h(c, x, -1), h_x,
                    material_of(x), drive_of(x, k),
                )
                for c in range(3):
                    rest.set_e(c, x, new[c])
                if x == 0:
                    edge = new
            put_left(k + 1, edge[1], edge[2])

    class Fields:
        def __init__(self, e_ref, h_ref, e_x, h_x, e_row, h_row, n):
            self.e_ref, self.h_ref, self.e_x, self.h_x = e_ref, h_ref, e_x, h_x
            self.e_row, self.h_row, self.n = e_row, h_row, n

        def e(self, c, x, dy):
            return self.e_ref[c, self.e_x + x, self.e_row + dy : self.e_row + dy + self.n, :]

        def h(self, c, x, dy):
            return self.h_ref[c, self.h_x + x, self.h_row + dy : self.h_row + dy + self.n, :]

        def set_e(self, c, x, value):
            self.e_ref[c, self.e_x + x, self.e_row : self.e_row + self.n, :] = value

        def set_h(self, c, x, value):
            self.h_ref[c, self.h_x + x, self.h_row : self.h_row + self.n, :] = value

    def to_side(go_right, s, w, k, spare=None, part=None):
        source, target = (send_h, recv_h) if go_right else (send_e, recv_e)
        source, target = source.at[s, w if spare is None else spare, k], target.at[s, w, k]
        if part is not None:
            source, target = source.at[:, part], target.at[:, part]
        send, recv = (right_send, right_recv) if go_right else (left_send, left_recv)
        return pltpu.make_async_remote_copy(
            source, target, send.at[s, w, k], recv.at[s, w, k],
            device_id=right if go_right else left, device_id_type=MESH,
        )

    def depth_of(go_right, w, k):
        return STEPS - (w * WIN + k) - (1 if go_right else 0)

    def used_rows(go_right, w, k):
        extra = depth_of(go_right, w, k)
        return pl.ds(gy * (HALO - extra), own_rows + extra)

    far_rows = pl.ds(pl.multiple_of(gy * 2 * HALO, HALO), own_rows - HALO)

    def near_rows(go_right, w, k):
        extra = depth_of(go_right, w, k)
        start = own_rows - HALO
        return pl.ds(start - gy * (start - HALO + extra), HALO + extra)

    def early():
        fields = Fields(pe, ph, 0, 1, HALO, HALO, own_rows)

        def put(go_right, k, y, z):
            buffer = send_h if go_right else send_e
            buffer[0, WINDOWS, k, 0, own_slice, :] = y
            buffer[0, WINDOWS, k, 1, own_slice, :] = z
            each(
                has_right if go_right else has_left,
                lambda: to_side(go_right, 0, 0, k, WINDOWS, far_rows).start(),
            )

        run_free(
            fields, fields,
            lambda k, y, z: put(False, k, y, z), lambda k, y, z: put(True, k, y, z),
            lambda x: ce[X0 + x, own_slice, :],
            lambda x, k: src[0, x, own_slice, :] * waves[0, k],
        )

    def free(s, w):
        def put(go_right, k, y, z):
            buffer = send_h if go_right else send_e
            buffer[s, w, k, 0] = y
            buffer[s, w, k, 1] = z
            there_is = has_right if go_right else has_left
            whole = used_rows(go_right, w, k)
            if w == 0:
                parted = (s == 0) & (gy == 0)
                each(
                    there_is & parted,
                    lambda: to_side(go_right, s, w, k, None, near_rows(go_right, w, k)).start(),
                )
                each(
                    there_is & jnp.logical_not(parted),
                    lambda: to_side(go_right, s, w, k, None, whole).start(),
                )
            else:
                each(there_is, lambda: to_side(go_right, s, w, k, None, whole).start())

        run_free(
            Fields(we.at[s], wh.at[s], X0, X0, 0, HALO, rows),
            Fields(fe, fh, 0, 1, 0, HALO, rows),
            lambda k, y, z: put(False, k, y, z), lambda k, y, z: put(True, k, y, z),
            lambda x: ce[X0 + x],
            lambda x, k: src[s, x] * waves[s, w * WIN + k],
        )

    H0, HM = slice(HALO, HALO + rows), slice(HALO - 1, HALO + rows - 1)
    R0, R1 = slice(0, rows), slice(1, rows + 1)

    def wait_series(there_is, go_right, s, w, k):
        for window in range(WINDOWS):
            rows_in = used_rows(go_right, window, k)
            each(
                there_is & (w == window),
                lambda: to_side(go_right, s, window, k, None, rows_in).wait_recv(),
            )

    def true(s, w, relay):
        for c in range(3):
            for p in (X0 - 2, X0 - 1, X0 + width, X0 + width + 1):
                we[s, c, p, R0, :] = plane0
                wh[s, c, p, H0, :] = plane0
        for k in range(WIN):
            reach = min(k + 1, WIN - k)
            h_lo, h_hi = -reach, width + min(k, WIN - 1 - k)
            e_out_reach = min(k + 1, WIN - 1 - k)
            if k == WIN - 2:
                relay()
            wait_series(has_right, False, s, w, k)
            e_next = None
            for x in range(h_hi - 1, h_lo - 1, -1):
                p = X0 + x
                e = {c: we[s, c, p, R0, :] for c in range(3)}
                if e_next is None:
                    e_x = {c: we[s, c, p + 1, R0, :] for c in (1, 2)}
                else:
                    e_x = e_next
                e_next = e
                if x == width - 1:
                    e_x = {c: (e_x[c] + recv_e[s, w, k, c - 1]) * on_right for c in (1, 2)}
                new = h_update(
                    lambda c: wh[s, c, p, H0, :], e, lambda c: we[s, c, p, R1, :], e_x
                )
                for c in range(3):
                    wh[s, c, p, H0, :] = new[c]
            wait_series(has_left, True, s, w, k)
            wave = waves[s, w * WIN + k]
            h_last = None
            for x in range(-e_out_reach, width + e_out_reach):
                p = X0 + x
                h = {c: wh[s, c, p, H0, :] for c in range(3)}
                if h_last is None:
                    h_x = {c: wh[s, c, p - 1, H0, :] for c in (1, 2)}
                else:
                    h_x = h_last
                h_last = h
                if x == 0:
                    h_x = {c: (h_x[c] + recv_h[s, w, k, c - 1]) * on_left for c in (1, 2)}
                inside = 0 <= x < width
                new = e_update(
                    lambda c: we[s, c, p, R0, :], h, lambda c: wh[s, c, p, HM, :], h_x,
                    ce[p], src[s, x] * wave if inside else None,
                )
                for c in range(3):
                    we[s, c, p, R0, :] = new[c]
                    if inside:
                        hist[s, w * WIN + k, c, x] = new[c]

    pl.when(gy == 0)(early)
    loads[2].wait()
    loads[3].wait()
    src_halo.wait()
    ce_halo.wait()
    e_halos[0].wait()
    h_halos[0].wait()

    def start_free(s, carry):
        @pl.when(s == 1)
        def _():
            e_halos[1].wait()
            h_halos[1].wait()

        free(s, 0)
        return carry

    pl.semaphore_wait(near, len(near_peers))
    signal(mid, mid_peers)
    lax.fori_loop(0, 2, start_free, 0)

    def wait_recvs(copies):
        for copy in copies:
            copy.wait_recv()

    def wait_sends(copies):
        for copy in copies:
            copy.wait_send()

    each(has_left, lambda: wait_recvs(go_right))
    each(has_right, lambda: wait_recvs(go_left))

    sum1 = [
        pltpu.make_async_remote_copy(
            part1.at[0], part1.at[1 + n], sum1_send.at[n], sum1_recv.at[n],
            device_id=peer, device_id_type=MESH,
        )
        for n, peer in enumerate(plane_peers)
    ]
    sum2 = [
        pltpu.make_async_remote_copy(
            part2.at[0], part2.at[1 + n], sum2_send.at[n], sum2_recv.at[n],
            device_id=peer, device_id_type=MESH,
        )
        for n, peer in enumerate(line_peers)
    ]
    def turn(j, carry):
        w, s = j // 2, lax.rem(j, 2)

        def add_plane():
            @pl.when(j == 3)
            def _():
                for copy in sum1:
                    copy.wait_recv()
                total = part1[0]
                for n in range(len(sum1)):
                    total = total + part1[1 + n]
                part2[0] = total
                for copy in sum2:
                    copy.start()

        true(s, w, add_plane)

        @pl.when(w == 0)
        def _():
            free(s, 1)

        @pl.when(j == 0)
        def _():
            pl.semaphore_wait(mid, len(mid_peers))
            signal(far, far_peers)

        @pl.when(j == 2)
        def _():
            pl.semaphore_wait(far, len(far_peers))
            total = jnp.zeros((own_rows, depth), jnp.float32)
            for c in range(3):
                for x in range(width):
                    e = we[0, c, X0 + x, pl.ds(own, own_rows), :]
                    total = total + e * e
            line = jnp.sum(total, axis=0, keepdims=True)
            part1[0] = jnp.where(lanes == planes[1], line, 0.0)
            for copy in sum1:
                copy.start()

        return carry

    lax.fori_loop(0, 2 * WINDOWS, turn, 0)

    for x in range(width):
        corr = jnp.zeros((own_rows, depth), jnp.float32)
        for k in range(STEPS):
            for c in range(3):
                corr = corr + (
                    hist[0, k, c, x, pl.ds(own, own_rows), :]
                    * hist[1, k, c, x, pl.ds(own, own_rows), :]
                )
        grad[x] = grad[x] * corr

    each(has_right, lambda: wait_sends(go_right))
    each(has_left, lambda: wait_sends(go_left))
    for copy in sum1 + sum2:
        copy.wait_send()

    def drain(s, carry):
        for w in range(WINDOWS):
            for k in range(WIN):
                for go_right, there_is in ((True, has_right), (False, has_left)):
                    copy = to_side(go_right, s, w, k, None, used_rows(go_right, w, k))
                    each(there_is, copy.wait_send)
        return carry

    lax.fori_loop(0, 2, drain, 0)

    for copy in sum2:
        copy.wait_recv()
    total = part2[0]
    for n in range(len(sum2)):
        total = total + part2[1 + n]
    cells = count_x * width * lax.axis_size("gy") * own_rows
    power = jnp.sum(total, axis=1, keepdims=True) / cells
    scale = jnp.broadcast_to(1.0 / (power + small_eps), (own_rows, depth))
    for x in range(width):
        grad[x] = grad[x] * scale


def store(we, wh, grad, e_out, h_out, g_out, sem):
    width, own_rows = grad.shape[0], grad.shape[1]
    own = pl.multiple_of(lax.axis_index("gy") * HALO, HALO)
    block = pl.ds(LEFT, width)
    outs = [
        pltpu.make_async_copy(we.at[:, :, block, pl.ds(own, own_rows), :], e_out, sem.at[0]),
        pltpu.make_async_copy(wh.at[:, :, block, pl.ds(own + HALO, own_rows), :], h_out, sem.at[1]),
        pltpu.make_async_copy(grad, g_out, sem.at[2]),
    ]
    for out in outs:
        out.start()
    for out in outs:
        out.wait()


def vmem_array(shape):
    return pltpu.VMEM(shape, jnp.float32)


def in_vmem(x):
    return pltpu.with_memory_space_constraint(x, pltpu.VMEM)


def shards(electric, magnetic, density, design_mask, planes, profiles, waveforms):
    sets, comps, width, own_rows, depth = electric.shape
    rows = own_rows + HALO
    count_z = lax.axis_size("gx") // CHIPS_X
    f32 = jnp.float32
    vmem, dma = pltpu.VMEM, pltpu.SemaphoreType.DMA
    came = vmem((sets, WINDOWS, WIN, 2, rows, depth), f32)
    sent = vmem((sets, WINDOWS + 1, WIN, 2, rows, depth), f32)
    any_space = pl.BlockSpec(memory_space=pl.ANY)
    held = pl.BlockSpec(memory_space=pltpu.VMEM)
    smem, wait = pltpu.SMEM, pltpu.SemaphoreType.REGULAR
    frame = (sets, comps, FRAME, rows + HALO, depth)
    e_frame, h_frame, grad = pl.pallas_call(
        kernel,
        out_shape=(vmem_array(frame), vmem_array(frame), vmem_array(density.shape)),
        in_specs=[any_space] * 7,
        out_specs=(held,) * 3,
        scratch_shapes=[
            *[vmem((comps, width + 1, rows + HALO, depth), f32)] * 4,
            sent, sent, came, came,
            vmem((FRAME, rows, depth), f32),
            vmem((sets, width, rows, depth), f32),
            vmem((width, own_rows, depth), f32),
            vmem((width, own_rows, depth), jnp.int32),
            vmem((sets, STEPS, comps, width, rows, depth), f32),
            vmem((2 * CHIPS_X, 1, depth), f32),
            vmem((count_z, 1, depth), f32),
            smem(planes.shape, jnp.int32),
            smem(waveforms.shape, f32),
            vmem(profiles.shape, f32),
            dma((9,)), wait, wait, wait, dma((6,)), dma((6,)), dma((4,)), dma((4,)),
            dma((sets, WINDOWS, WIN)), dma((sets, WINDOWS, WIN)),
            dma((sets, WINDOWS, WIN)), dma((sets, WINDOWS, WIN)),
            dma((2 * CHIPS_X - 1,)), dma((2 * CHIPS_X - 1,)),
            dma((max(count_z - 1, 1),)), dma((max(count_z - 1, 1),)),
        ],
        compiler_params=pltpu.CompilerParams(
            collective_id=0, has_side_effects=True, vmem_limit_bytes=64_200_000
        ),
    )(planes, waveforms, profiles, electric, magnetic, density, design_mask)
    return pl.pallas_call(
        store,
        out_shape=(
            jax.ShapeDtypeStruct(electric.shape, f32),
            jax.ShapeDtypeStruct(magnetic.shape, f32),
            jax.ShapeDtypeStruct(density.shape, f32),
        ),
        in_specs=[held] * 3,
        out_specs=(any_space,) * 3,
        scratch_shapes=[dma((3,))],
        compiler_params=pltpu.CompilerParams(vmem_limit_bytes=4 << 20),
    )(in_vmem(e_frame), in_vmem(h_frame), in_vmem(grad))


def solution(mesh):
    return jax.shard_map(
        shards,
        mesh=mesh,
        in_specs=(
            P(None, None, CAND_GX, "gy", None),
            P(None, None, CAND_GX, "gy", None),
            P(CAND_GX, "gy", None),
            P(CAND_GX, "gy", None),
            P("cand"),
            P(None, CAND_GX, "gy"),
            P(None, "cand"),
        ),
        out_specs=(
            P(None, None, CAND_GX, "gy", None),
            P(None, None, CAND_GX, "gy", None),
            P(CAND_GX, "gy", None),
        ),
        check_vma=False,
    )
```

```python
import jax
import jax.numpy as jnp
from jax import lax
from jax.experimental import pallas as pl
from jax.experimental.pallas import tpu as pltpu
from jax.sharding import PartitionSpec as P

STEPS = 8
PMLW = 8
CAND_GX = ("cand", "gx")
CHIPS_X = 4
MESH = pl.DeviceIdType.MESH

step_dt = 0.7
contrast = 5.0
sigma_max = 2.0
small_eps = 1e-06
inv_spacing = 0.5

WIN = 4
WINDOWS = STEPS // WIN
LEFT = 3
FRAME = 9
HALO = 8


def kernel(
    planes_in, waves_in, prof_in, e_in, h_in, den_in, mask_in,
    we, wh, grad,
    fe, fh, pe, ph, send_h, send_e, recv_h, recv_e, ce, src, den, mask, hist, part1, part2,
    planes, waves, prof, load_sem, near, mid, far, halo_send, halo_recv, mat_send, mat_recv,
    right_send, right_recv, left_send, left_recv,
    sum1_send, sum1_recv, sum2_send, sum2_recv,
):
    width, own_rows = den.shape[0], den.shape[1]
    rows, depth = own_rows + HALO, den.shape[2]
    count_x = lax.axis_size("gx")
    count_z = count_x // CHIPS_X
    gx, gy = lax.axis_index("gx"), lax.axis_index("gy")
    chip_x, chip_z = gx // count_z, lax.rem(gx, count_z)
    other = 1 - gy
    right = {"gx": lax.rem(gx + 1, count_x), "gy": gy}
    left = {"gx": lax.rem(gx + count_x - 1, count_x), "gy": gy}
    across = {"gx": gx, "gy": other}
    right_across, left_across = dict(right, gy=other), dict(left, gy=other)
    has_right, has_left = gx < count_x - 1, gx > 0
    plane_peers = []
    for dx in sorted(range(CHIPS_X), key=lambda d: -min(d, CHIPS_X - d)):
        for dc in range(2):
            if dx or dc:
                peer = lax.rem(chip_x + dx, CHIPS_X) * count_z + chip_z
                plane_peers.append({"gx": peer, "gy": other if dc else gy})

    def along_z(dz):
        return {"gx": chip_x * count_z + lax.rem(chip_z + dz, count_z), "gy": gy}

    def both_ways(d):
        return [along_z(dz) for dz in sorted({d % count_z, -d % count_z} - {0})]

    line_peers = [
        along_z(dz) for dz in sorted(range(1, count_z), key=lambda d: -min(d, count_z - d))
    ]
    next_chips = [
        {"gx": lax.rem(chip_x + dx, CHIPS_X) * count_z + chip_z, "gy": gy} for dx in (1, CHIPS_X - 1)
    ]
    own = pl.multiple_of(gy * HALO, HALO)
    top = pl.multiple_of((1 - gy) * (own_rows - HALO), HALO)
    there = pl.multiple_of(gy * own_rows, HALO)
    X0 = LEFT
    block = pl.ds(X0, width)

    early_rows = pl.ds(HALO, own_rows)
    loads = [
        pltpu.make_async_copy(den_in, den, load_sem.at[0]),
        pltpu.make_async_copy(mask_in, mask, load_sem.at[1]),
        pltpu.make_async_copy(e_in, we.at[:, :, block, pl.ds(own, own_rows), :], load_sem.at[2]),
        pltpu.make_async_copy(
            h_in, wh.at[:, :, block, pl.ds(own + HALO, own_rows), :], load_sem.at[3]
        ),
        pltpu.make_async_copy(planes_in, planes, load_sem.at[4]),
        pltpu.make_async_copy(waves_in, waves, load_sem.at[5]),
        pltpu.make_async_copy(prof_in, prof, load_sem.at[6]),
        pltpu.make_async_copy(e_in.at[0], pe.at[:, pl.ds(0, width), early_rows], load_sem.at[7]),
        pltpu.make_async_copy(h_in.at[0], ph.at[:, pl.ds(1, width), early_rows], load_sem.at[8]),
    ]
    for n in (0, 1, 4, 6, 7, 8, 5, 2, 3):
        loads[n].start()

    def signal(semaphore, peers):
        for peer in peers:
            pl.semaphore_signal(semaphore, inc=1, device_id=peer, device_id_type=MESH)

    barrier = pltpu.get_barrier_semaphore()
    peers = [across, left, right, left_across, right_across] + next_chips + both_ways(1)
    near_peers = next_chips + both_ways(1)
    mid_peers = next_chips + both_ways(2)
    far_peers = both_ways(4)
    signal(barrier, peers)

    lanes = lax.broadcasted_iota(jnp.int32, (1, depth), 1)
    zpos = lanes.astype(jnp.float32)
    lower = (PMLW - zpos - 0.5) / PMLW
    upper = (zpos + 0.5 - (depth - PMLW)) / PMLW
    deep = jnp.maximum(jnp.maximum(lower, upper), 0.0)
    half = sigma_max * deep * deep * deep * step_dt / 2.0
    decay1 = (1.0 - half) / (1.0 + half)
    gain1 = step_dt / (1.0 + half)
    gain_half1 = gain1 * inv_spacing
    on_left = has_left.astype(jnp.float32)
    on_right = has_right.astype(jnp.float32)

    pad = jnp.zeros((HALO, depth), jnp.float32)
    plane0 = jnp.zeros((rows, depth), jnp.float32)
    for s in range(2):
        for c in range(3):
            for p in range(FRAME):
                if c != 1:
                    we[s, c, p, rows : rows + HALO, :] = pad
                    wh[s, c, p, 0:HALO, :] = pad
            wh[s, c, 0, HALO:, :] = plane0
    for c in (0, 2):
        for p in range(width + 1):
            fe[c, p, rows : rows + HALO, :] = pad
            fh[c, p, 0:HALO, :] = pad
            pe[c, p, rows : rows + HALO, :] = pad
            ph[c, p, 0:HALO, :] = pad
    for c in range(3):
        fe[c, width, 0:rows, :] = plane0
        fh[c, 0, HALO:, :] = plane0
        ph[c, 0, HALO:, :] = plane0

    @pl.when(jnp.logical_not(has_right))
    def _():
        recv_e[...] = jnp.zeros_like(recv_e)
        for p in (X0 + width, X0 + width + 1):
            ce[p] = plane0

    @pl.when(jnp.logical_not(has_left))
    def _():
        recv_h[...] = jnp.zeros_like(recv_h)
        for p in (X0 - 2, X0 - 1):
            ce[p] = plane0

    pl.semaphore_wait(barrier, len(peers))

    def halo(n, source, target):
        return pltpu.make_async_remote_copy(
            source, target, halo_send.at[n], halo_recv.at[n],
            device_id=across, device_id_type=MESH,
        )

    own_slice = pl.ds(own, own_rows)
    halo_slice = pl.ds(pl.multiple_of(own + top, HALO), HALO)
    there_slice = pl.ds(there, HALO)
    e_halos = [
        halo(s, e_in.at[s, :, :, pl.ds(top, HALO), :], we.at[s, :, block, there_slice, :])
        for s in range(2)
    ]
    h_halos = [
        halo(
            2 + s, h_in.at[s, :, :, pl.ds(top, HALO), :],
            wh.at[s, :, block, pl.ds(there + HALO, HALO), :],
        )
        for s in range(2)
    ]
    src_halo = halo(4, src.at[:, :, halo_slice, :], src.at[:, :, there_slice, :])
    ce_halo = halo(5, ce.at[block, halo_slice, :], ce.at[block, there_slice, :])
    for s in range(2):
        e_halos[s].start()
        h_halos[s].start()
    signal(near, near_peers)

    high, low = pl.ds(X0 + width - 2, 2), pl.ds(X0, 2)
    high_ghost, low_ghost = pl.ds(X0 + width, 2), pl.ds(X0 - 2, 2)

    def material(n, planes_from, planes_to, rows_from, rows_to, device):
        return pltpu.make_async_remote_copy(
            ce.at[planes_from, rows_from], ce.at[planes_to, rows_to],
            mat_send.at[n], mat_recv.at[n], device_id=device, device_id_type=MESH,
        )

    go_right = [
        material(0, high, low_ghost, own_slice, own_slice, right),
        material(1, high, low_ghost, halo_slice, there_slice, right_across),
    ]
    go_left = [
        material(2, low, high_ghost, own_slice, own_slice, left),
        material(3, low, high_ghost, halo_slice, there_slice, left_across),
    ]

    def each(condition, action):
        @pl.when(condition)
        def _():
            action()

    def start_all(copies):
        for copy in copies:
            copy.start()

    loads[0].wait()
    loads[1].wait()
    for x in range(width):
        flags = mask[x].astype(jnp.float32)
        inv_eps = 1.0 / (1.0 + contrast * den[x] * flags)
        ce[X0 + x, own_slice, :] = inv_eps * gain1
        grad[x] = flags * contrast * inv_eps * inv_eps * step_dt
    ce_halo.start()
    each(has_right, lambda: start_all(go_right))
    each(has_left, lambda: start_all(go_left))
    eye = lax.broadcasted_iota(jnp.int32, (own_rows, own_rows), 0) == lax.broadcasted_iota(
        jnp.int32, (own_rows, own_rows), 1
    )
    loads[4].wait()
    loads[6].wait()
    for s in range(2):
        spot = jnp.where(lanes == planes[s], gain1, 0.0)
        for x in range(width):
            row = jnp.broadcast_to(prof[s, x : x + 1, :], (own_rows, own_rows))
            column = jnp.sum(jnp.where(eye, row, 0.0), axis=1, keepdims=True)
            src[s, x, pl.ds(own, own_rows), :] = column * spot

    src_halo.start()
    loads[5].wait()
    loads[7].wait()
    loads[8].wait()
    def spread(row, n):
        return jnp.broadcast_to(row, (n, depth))

    def up_z(f):
        return jnp.where(spread(lanes == depth - 1, f.shape[0]), 0.0, pltpu.roll(f, depth - 1, 1))

    def down_z(f):
        return jnp.where(spread(lanes == 0, f.shape[0]), 0.0, pltpu.roll(f, 1, 1))

    def h_update(h_old, e, e_y, e_x, comps=(0, 1, 2)):
        decay, gain, gain_half = (spread(r, e[0].shape[0]) for r in (decay1, gain1, gain_half1))
        new = {}
        if 0 in comps:
            new[0] = decay * h_old(0) - gain_half * ((e_y(2) - e[2]) - (up_z(e[1]) - e[1]))
        new[1] = decay * h_old(1) - (gain_half * (up_z(e[0]) - e[0]) - gain * (e_x[2] - e[2]))
        new[2] = decay * h_old(2) - (gain * (e_x[1] - e[1]) - gain_half * (e_y(0) - e[0]))
        return new

    def e_update(e_old, h, h_y, h_x, c, drive):
        decay = spread(decay1, h[0].shape[0])
        cx = c * inv_spacing
        x = decay * e_old(0) + cx * ((h[2] - h_y(2)) - (h[1] - down_z(h[1])))
        if drive is not None:
            x = x - drive
        y = decay * e_old(1) + (cx * (h[0] - down_z(h[0])) - c * (h[2] - h_x[2]))
        z = decay * e_old(2) + (c * (h[1] - h_x[1]) - cx * (h[0] - h_y(0)))
        return {0: x, 1: y, 2: z}

    def run_free(first, rest, put_left, put_right, material_of, drive_of):
        put_left(0, first.e(1, 0, 0), first.e(2, 0, 0))
        for k in range(WIN):
            last = k == WIN - 1
            now = first if k == 0 else rest
            h_planes = [x for x in range(width) if x >= k or x < width - 1 - k]
            if last:
                h_planes = [width - 1]
            for x in h_planes:
                e = {c: now.e(c, x, 0) for c in range(3)}
                e_x = {
                    c: (now.e(c, x + 1, 0) if x < width - 1 else jnp.zeros_like(e[c]))
                    for c in (1, 2)
                }
                new = h_update(
                    lambda c: now.h(c, x, 0), e, lambda c: now.e(c, x, 1), e_x,
                    (1, 2) if last else (0, 1, 2),
                )
                if not last:
                    for c in range(3):
                        rest.set_h(c, x, new[c])
                if x == width - 1:
                    edge = new
            put_right(k, edge[1], edge[2])
            if last:
                break
            for x in [x for x in range(width) if x >= k + 1 or x < width - 1 - k]:
                h = {c: rest.h(c, x, 0) for c in range(3)}
                h_x = {c: rest.h(c, x - 1, 0) for c in (1, 2)}
                new = e_update(
                    lambda c: now.e(c, x, 0), h, lambda c: rest.h(c, x, -1), h_x,
                    material_of(x), drive_of(x, k),
                )
                for c in range(3):
                    rest.set_e(c, x, new[c])
                if x == 0:
                    edge = new
            put_left(k + 1, edge[1], edge[2])

    class Fields:
        def __init__(self, e_ref, h_ref, e_x, h_x, e_row, h_row, n):
            self.e_ref, self.h_ref, self.e_x, self.h_x = e_ref, h_ref, e_x, h_x
            self.e_row, self.h_row, self.n = e_row, h_row, n

        def e(self, c, x, dy):
            return self.e_ref[c, self.e_x + x, self.e_row + dy : self.e_row + dy + self.n, :]

        def h(self, c, x, dy):
            return self.h_ref[c, self.h_x + x, self.h_row + dy : self.h_row + dy + self.n, :]

        def set_e(self, c, x, value):
            self.e_ref[c, self.e_x + x, self.e_row : self.e_row + self.n, :] = value

        def set_h(self, c, x, value):
            self.h_ref[c, self.h_x + x, self.h_row : self.h_row + self.n, :] = value

    def to_side(go_right, s, w, k, spare=None, part=None):
        source, target = (send_h, recv_h) if go_right else (send_e, recv_e)
        source, target = source.at[s, w if spare is None else spare, k], target.at[s, w, k]
        if part is not None:
            source, target = source.at[:, part], target.at[:, part]
        send, recv = (right_send, right_recv) if go_right else (left_send, left_recv)
        return pltpu.make_async_remote_copy(
            source, target, send.at[s, w, k], recv.at[s, w, k],
            device_id=right if go_right else left, device_id_type=MESH,
        )

    def depth_of(go_right, w, k):
        return STEPS - (w * WIN + k) - (1 if go_right else 0)

    def used_rows(go_right, w, k):
        extra = depth_of(go_right, w, k)
        return pl.ds(gy * (HALO - extra), own_rows + extra)

    far_rows = pl.ds(pl.multiple_of(gy * 2 * HALO, HALO), own_rows - HALO)

    def near_rows(go_right, w, k):
        extra = depth_of(go_right, w, k)
        start = own_rows - HALO
        return pl.ds(start - gy * (start - HALO + extra), HALO + extra)

    def early():
        fields = Fields(pe, ph, 0, 1, HALO, HALO, own_rows)

        def put(go_right, k, y, z):
            buffer = send_h if go_right else send_e
            buffer[0, WINDOWS, k, 0, own_slice, :] = y
            buffer[0, WINDOWS, k, 1, own_slice, :] = z
            each(
                has_right if go_right else has_left,
                lambda: to_side(go_right, 0, 0, k, WINDOWS, far_rows).start(),
            )

        run_free(
            fields, fields,
            lambda k, y, z: put(False, k, y, z), lambda k, y, z: put(True, k, y, z),
            lambda x: ce[X0 + x, own_slice, :],
            lambda x, k: src[0, x, own_slice, :] * waves[0, k],
        )

    def free(s, w):
        def put(go_right, k, y, z):
            buffer = send_h if go_right else send_e
            buffer[s, w, k, 0] = y
            buffer[s, w, k, 1] = z
            there_is = has_right if go_right else has_left
            whole = used_rows(go_right, w, k)
            if w == 0:
                parted = (s == 0) & (gy == 0)
                each(
                    there_is & parted,
                    lambda: to_side(go_right, s, w, k, None, near_rows(go_right, w, k)).start(),
                )
                each(
                    there_is & jnp.logical_not(parted),
                    lambda: to_side(go_right, s, w, k, None, whole).start(),
                )
            else:
                each(there_is, lambda: to_side(go_right, s, w, k, None, whole).start())

        run_free(
            Fields(we.at[s], wh.at[s], X0, X0, 0, HALO, rows),
            Fields(fe, fh, 0, 1, 0, HALO, rows),
            lambda k, y, z: put(False, k, y, z), lambda k, y, z: put(True, k, y, z),
            lambda x: ce[X0 + x],
            lambda x, k: src[s, x] * waves[s, w * WIN + k],
        )

    H0, HM = slice(HALO, HALO + rows), slice(HALO - 1, HALO + rows - 1)
    R0, R1 = slice(0, rows), slice(1, rows + 1)

    def wait_series(there_is, go_right, s, w, k):
        for window in range(WINDOWS):
            rows_in = used_rows(go_right, window, k)
            each(
                there_is & (w == window),
                lambda: to_side(go_right, s, window, k, None, rows_in).wait_recv(),
            )

    def true(s, w, relay):
        for c in range(3):
            for p in (X0 - 2, X0 - 1, X0 + width, X0 + width + 1):
                we[s, c, p, R0, :] = plane0
                wh[s, c, p, H0, :] = plane0
        for k in range(WIN):
            reach = min(k + 1, WIN - k)
            h_lo, h_hi = -reach, width + min(k, WIN - 1 - k)
            e_out_reach = min(k + 1, WIN - 1 - k)
            if k == WIN - 2:
                relay()
            wait_series(has_right, False, s, w, k)
            e_next = None
            for x in range(h_hi - 1, h_lo - 1, -1):
                p = X0 + x
                e = {c: we[s, c, p, R0, :] for c in range(3)}
                if e_next is None:
                    e_x = {c: we[s, c, p + 1, R0, :] for c in (1, 2)}
                else:
                    e_x = e_next
                e_next = e
                if x == width - 1:
                    e_x = {c: (e_x[c] + recv_e[s, w, k, c - 1]) * on_right for c in (1, 2)}
                new = h_update(
                    lambda c: wh[s, c, p, H0, :], e, lambda c: we[s, c, p, R1, :], e_x
                )
                for c in range(3):
                    wh[s, c, p, H0, :] = new[c]
            wait_series(has_left, True, s, w, k)
            wave = waves[s, w * WIN + k]
            h_last = None
            for x in range(-e_out_reach, width + e_out_reach):
                p = X0 + x
                h = {c: wh[s, c, p, H0, :] for c in range(3)}
                if h_last is None:
                    h_x = {c: wh[s, c, p - 1, H0, :] for c in (1, 2)}
                else:
                    h_x = h_last
                h_last = h
                if x == 0:
                    h_x = {c: (h_x[c] + recv_h[s, w, k, c - 1]) * on_left for c in (1, 2)}
                inside = 0 <= x < width
                new = e_update(
                    lambda c: we[s, c, p, R0, :], h, lambda c: wh[s, c, p, HM, :], h_x,
                    ce[p], src[s, x] * wave if inside else None,
                )
                for c in range(3):
                    we[s, c, p, R0, :] = new[c]
                    if inside:
                        hist[s, w * WIN + k, c, x] = new[c]

    pl.when(gy == 0)(early)
    loads[2].wait()
    loads[3].wait()
    src_halo.wait()
    ce_halo.wait()
    e_halos[0].wait()
    h_halos[0].wait()

    def start_free(s, carry):
        @pl.when(s == 1)
        def _():
            e_halos[1].wait()
            h_halos[1].wait()

        free(s, 0)
        return carry

    pl.semaphore_wait(near, len(near_peers))
    signal(mid, mid_peers)
    lax.fori_loop(0, 2, start_free, 0)

    def wait_recvs(copies):
        for copy in copies:
            copy.wait_recv()

    def wait_sends(copies):
        for copy in copies:
            copy.wait_send()

    each(has_left, lambda: wait_recvs(go_right))
    each(has_right, lambda: wait_recvs(go_left))

    sum1 = [
        pltpu.make_async_remote_copy(
            part1.at[0], part1.at[1 + n], sum1_send.at[n], sum1_recv.at[n],
            device_id=peer, device_id_type=MESH,
        )
        for n, peer in enumerate(plane_peers)
    ]
    sum2 = [
        pltpu.make_async_remote_copy(
            part2.at[0], part2.at[1 + n], sum2_send.at[n], sum2_recv.at[n],
            device_id=peer, device_id_type=MESH,
        )
        for n, peer in enumerate(line_peers)
    ]
    def turn(j, carry):
        w, s = j // 2, lax.rem(j, 2)

        def add_plane():
            @pl.when(j == 3)
            def _():
                for copy in sum1:
                    copy.wait_recv()
                total = part1[0]
                for n in range(len(sum1)):
                    total = total + part1[1 + n]
                part2[0] = total
                for copy in sum2:
                    copy.start()

        true(s, w, add_plane)

        @pl.when(w == 0)
        def _():
            free(s, 1)

        @pl.when(j == 0)
        def _():
            pl.semaphore_wait(mid, len(mid_peers))
            signal(far, far_peers)

        @pl.when(j == 2)
        def _():
            pl.semaphore_wait(far, len(far_peers))
            total = jnp.zeros((own_rows, depth), jnp.float32)
            for c in range(3):
                for x in range(width):
                    e = we[0, c, X0 + x, pl.ds(own, own_rows), :]
                    total = total + e * e
            line = jnp.sum(total, axis=0, keepdims=True)
            part1[0] = jnp.where(lanes == planes[1], line, 0.0)
            for copy in sum1:
                copy.start()

        return carry

    lax.fori_loop(0, 2 * WINDOWS, turn, 0)

    for x in range(width):
        corr = jnp.zeros((own_rows, depth), jnp.float32)
        for k in range(STEPS):
            for c in range(3):
                corr = corr + (
                    hist[0, k, c, x, pl.ds(own, own_rows), :]
                    * hist[1, k, c, x, pl.ds(own, own_rows), :]
                )
        grad[x] = grad[x] * corr

    each(has_right, lambda: wait_sends(go_right))
    each(has_left, lambda: wait_sends(go_left))
    for copy in sum1 + sum2:
        copy.wait_send()

    def drain(s, carry):
        for w in range(WINDOWS):
            for k in range(WIN):
                for go_right, there_is in ((True, has_right), (False, has_left)):
                    copy = to_side(go_right, s, w, k, None, used_rows(go_right, w, k))
                    each(there_is, copy.wait_send)
        return carry

    lax.fori_loop(0, 2, drain, 0)

    for copy in sum2:
        copy.wait_recv()
    total = part2[0]
    for n in range(len(sum2)):
        total = total + part2[1 + n]
    cells = count_x * width * lax.axis_size("gy") * own_rows
    power = jnp.sum(total, axis=1, keepdims=True) / cells
    scale = jnp.broadcast_to(1.0 / (power + small_eps), (own_rows, depth))
    for x in range(width):
        grad[x] = grad[x] * scale


def store(we, wh, grad, e_out, h_out, g_out, sem):
    width, own_rows = grad.shape[0], grad.shape[1]
    own = pl.multiple_of(lax.axis_index("gy") * HALO, HALO)
    block = pl.ds(LEFT, width)
    outs = [
        pltpu.make_async_copy(we.at[:, :, block, pl.ds(own, own_rows), :], e_out, sem.at[0]),
        pltpu.make_async_copy(wh.at[:, :, block, pl.ds(own + HALO, own_rows), :], h_out, sem.at[1]),
        pltpu.make_async_copy(grad, g_out, sem.at[2]),
    ]
    for out in outs:
        out.start()
    for out in outs:
        out.wait()


def vmem_array(shape):
    return pltpu.VMEM(shape, jnp.float32)


def in_vmem(x):
    return pltpu.with_memory_space_constraint(x, pltpu.VMEM)


def shards(electric, magnetic, density, design_mask, planes, profiles, waveforms):
    sets, comps, width, own_rows, depth = electric.shape
    rows = own_rows + HALO
    count_z = lax.axis_size("gx") // CHIPS_X
    f32 = jnp.float32
    vmem, dma = pltpu.VMEM, pltpu.SemaphoreType.DMA
    came = vmem((sets, WINDOWS, WIN, 2, rows, depth), f32)
    sent = vmem((sets, WINDOWS + 1, WIN, 2, rows, depth), f32)
    any_space = pl.BlockSpec(memory_space=pl.ANY)
    held = pl.BlockSpec(memory_space=pltpu.VMEM)
    smem, wait = pltpu.SMEM, pltpu.SemaphoreType.REGULAR
    frame = (sets, comps, FRAME, rows + HALO, depth)
    e_frame, h_frame, grad = pl.pallas_call(
        kernel,
        out_shape=(vmem_array(frame), vmem_array(frame), vmem_array(density.shape)),
        in_specs=[any_space] * 7,
        out_specs=(held,) * 3,
        scratch_shapes=[
            *[vmem((comps, width + 1, rows + HALO, depth), f32)] * 4,
            sent, sent, came, came,
            vmem((FRAME, rows, depth), f32),
            vmem((sets, width, rows, depth), f32),
            vmem((width, own_rows, depth), f32),
            vmem((width, own_rows, depth), jnp.int32),
            vmem((sets, STEPS, comps, width, rows, depth), f32),
            vmem((2 * CHIPS_X, 1, depth), f32),
            vmem((count_z, 1, depth), f32),
            smem(planes.shape, jnp.int32),
            smem(waveforms.shape, f32),
            vmem(profiles.shape, f32),
            dma((9,)), wait, wait, wait, dma((6,)), dma((6,)), dma((4,)), dma((4,)),
            dma((sets, WINDOWS, WIN)), dma((sets, WINDOWS, WIN)),
            dma((sets, WINDOWS, WIN)), dma((sets, WINDOWS, WIN)),
            dma((2 * CHIPS_X - 1,)), dma((2 * CHIPS_X - 1,)),
            dma((max(count_z - 1, 1),)), dma((max(count_z - 1, 1),)),
        ],
        compiler_params=pltpu.CompilerParams(
            collective_id=0, has_side_effects=True, vmem_limit_bytes=64_200_000
        ),
    )(planes, waveforms, profiles, electric, magnetic, density, design_mask)
    return pl.pallas_call(
        store,
        out_shape=(
            jax.ShapeDtypeStruct(electric.shape, f32),
            jax.ShapeDtypeStruct(magnetic.shape, f32),
            jax.ShapeDtypeStruct(density.shape, f32),
        ),
        in_specs=[held] * 3,
        out_specs=(any_space,) * 3,
        scratch_shapes=[dma((3,))],
        compiler_params=pltpu.CompilerParams(vmem_limit_bytes=4 << 20),
    )(in_vmem(e_frame), in_vmem(h_frame), in_vmem(grad))


def solution(mesh):
    return jax.shard_map(
        shards,
        mesh=mesh,
        in_specs=(
            P(None, None, CAND_GX, "gy", None),
            P(None, None, CAND_GX, "gy", None),
            P(CAND_GX, "gy", None),
            P(CAND_GX, "gy", None),
            P("cand"),
            P(None, CAND_GX, "gy"),
            P(None, "cand"),
        ),
        out_specs=(
            P(None, None, CAND_GX, "gy", None),
            P(None, None, CAND_GX, "gy", None),
            P(CAND_GX, "gy", None),
        ),
        check_vma=False,
    )
```

```python
import jax
import jax.numpy as jnp
from jax import lax
from jax.experimental import pallas as pl
from jax.experimental.pallas import tpu as pltpu
from jax.sharding import PartitionSpec as P

STEPS = 8
PMLW = 8
CAND_GX = ("cand", "gx")
CHIPS_X = 4
MESH = pl.DeviceIdType.MESH

step_dt = 0.7
contrast = 5.0
sigma_max = 2.0
small_eps = 1e-06
inv_spacing = 0.5

WIN = 4
WINDOWS = STEPS // WIN
LEFT = 3
FRAME = 9
HALO = 8


def kernel(
    planes_in, waves_in, prof_in, e_in, h_in, den_in, mask_in,
    we, wh, grad,
    fe, fh, pe, ph, send_h, send_e, recv_h, recv_e, ce, src, den, mask, hist, part1, part2,
    planes, waves, prof, load_sem, near, mid, far, halo_send, halo_recv, mat_send, mat_recv,
    right_send, right_recv, left_send, left_recv,
    sum1_send, sum1_recv, sum2_send, sum2_recv,
):
    width, own_rows = den.shape[0], den.shape[1]
    rows, depth = own_rows + HALO, den.shape[2]
    count_x = lax.axis_size("gx")
    count_z = count_x // CHIPS_X
    gx, gy = lax.axis_index("gx"), lax.axis_index("gy")
    chip_x, chip_z = gx // count_z, lax.rem(gx, count_z)
    other = 1 - gy
    right = {"gx": lax.rem(gx + 1, count_x), "gy": gy}
    left = {"gx": lax.rem(gx + count_x - 1, count_x), "gy": gy}
    across = {"gx": gx, "gy": other}
    right_across, left_across = dict(right, gy=other), dict(left, gy=other)
    has_right, has_left = gx < count_x - 1, gx > 0
    plane_peers = []
    for dx in sorted(range(CHIPS_X), key=lambda d: -min(d, CHIPS_X - d)):
        for dc in range(2):
            if dx or dc:
                peer = lax.rem(chip_x + dx, CHIPS_X) * count_z + chip_z
                plane_peers.append({"gx": peer, "gy": other if dc else gy})

    def along_z(dz):
        return {"gx": chip_x * count_z + lax.rem(chip_z + dz, count_z), "gy": gy}

    def both_ways(d):
        return [along_z(dz) for dz in sorted({d % count_z, -d % count_z} - {0})]

    line_peers = [
        along_z(dz) for dz in sorted(range(1, count_z), key=lambda d: -min(d, count_z - d))
    ]
    next_chips = [
        {"gx": lax.rem(chip_x + dx, CHIPS_X) * count_z + chip_z, "gy": gy} for dx in (1, CHIPS_X - 1)
    ]
    own = pl.multiple_of(gy * HALO, HALO)
    top = pl.multiple_of((1 - gy) * (own_rows - HALO), HALO)
    there = pl.multiple_of(gy * own_rows, HALO)
    X0 = LEFT
    block = pl.ds(X0, width)

    early_rows = pl.ds(HALO, own_rows)
    loads = [
        pltpu.make_async_copy(den_in, den, load_sem.at[0]),
        pltpu.make_async_copy(mask_in, mask, load_sem.at[1]),
        pltpu.make_async_copy(e_in, we.at[:, :, block, pl.ds(own, own_rows), :], load_sem.at[2]),
        pltpu.make_async_copy(
            h_in, wh.at[:, :, block, pl.ds(own + HALO, own_rows), :], load_sem.at[3]
        ),
        pltpu.make_async_copy(planes_in, planes, load_sem.at[4]),
        pltpu.make_async_copy(waves_in, waves, load_sem.at[5]),
        pltpu.make_async_copy(prof_in, prof, load_sem.at[6]),
        pltpu.make_async_copy(e_in.at[0], pe.at[:, pl.ds(0, width), early_rows], load_sem.at[7]),
        pltpu.make_async_copy(h_in.at[0], ph.at[:, pl.ds(1, width), early_rows], load_sem.at[8]),
    ]
    for n in (0, 1, 4, 6, 7, 8, 5, 2, 3):
        loads[n].start()

    def signal(semaphore, peers):
        for peer in peers:
            pl.semaphore_signal(semaphore, inc=1, device_id=peer, device_id_type=MESH)

    barrier = pltpu.get_barrier_semaphore()
    peers = [across, left, right, left_across, right_across] + next_chips + both_ways(1)
    near_peers = next_chips + both_ways(1)
    mid_peers = next_chips + both_ways(2)
    far_peers = both_ways(4)
    signal(barrier, peers)

    lanes = lax.broadcasted_iota(jnp.int32, (1, depth), 1)
    zpos = lanes.astype(jnp.float32)
    lower = (PMLW - zpos - 0.5) / PMLW
    upper = (zpos + 0.5 - (depth - PMLW)) / PMLW
    deep = jnp.maximum(jnp.maximum(lower, upper), 0.0)
    half = sigma_max * deep * deep * deep * step_dt / 2.0
    decay1 = (1.0 - half) / (1.0 + half)
    gain1 = step_dt / (1.0 + half)
    gain_half1 = gain1 * inv_spacing
    on_left = has_left.astype(jnp.float32)
    on_right = has_right.astype(jnp.float32)

    pad = jnp.zeros((HALO, depth), jnp.float32)
    plane0 = jnp.zeros((rows, depth), jnp.float32)
    for s in range(2):
        for c in range(3):
            for p in range(FRAME):
                if c != 1:
                    we[s, c, p, rows : rows + HALO, :] = pad
                    wh[s, c, p, 0:HALO, :] = pad
            wh[s, c, 0, HALO:, :] = plane0
    for c in (0, 2):
        for p in range(width + 1):
            fe[c, p, rows : rows + HALO, :] = pad
            fh[c, p, 0:HALO, :] = pad
            pe[c, p, rows : rows + HALO, :] = pad
            ph[c, p, 0:HALO, :] = pad
    for c in range(3):
        fe[c, width, 0:rows, :] = plane0
        fh[c, 0, HALO:, :] = plane0
        ph[c, 0, HALO:, :] = plane0

    @pl.when(jnp.logical_not(has_right))
    def _():
        recv_e[...] = jnp.zeros_like(recv_e)
        for p in (X0 + width, X0 + width + 1):
            ce[p] = plane0

    @pl.when(jnp.logical_not(has_left))
    def _():
        recv_h[...] = jnp.zeros_like(recv_h)
        for p in (X0 - 2, X0 - 1):
            ce[p] = plane0

    pl.semaphore_wait(barrier, len(peers))

    def halo(n, source, target):
        return pltpu.make_async_remote_copy(
            source, target, halo_send.at[n], halo_recv.at[n],
            device_id=across, device_id_type=MESH,
        )

    own_slice = pl.ds(own, own_rows)
    halo_slice = pl.ds(pl.multiple_of(own + top, HALO), HALO)
    there_slice = pl.ds(there, HALO)
    e_halos = [
        halo(s, e_in.at[s, :, :, pl.ds(top, HALO), :], we.at[s, :, block, there_slice, :])
        for s in range(2)
    ]
    h_halos = [
        halo(
            2 + s, h_in.at[s, :, :, pl.ds(top, HALO), :],
            wh.at[s, :, block, pl.ds(there + HALO, HALO), :],
        )
        for s in range(2)
    ]
    src_halo = halo(4, src.at[:, :, halo_slice, :], src.at[:, :, there_slice, :])
    ce_halo = halo(5, ce.at[block, halo_slice, :], ce.at[block, there_slice, :])
    for s in range(2):
        e_halos[s].start()
        h_halos[s].start()
    signal(near, near_peers)

    high, low = pl.ds(X0 + width - 2, 2), pl.ds(X0, 2)
    high_ghost, low_ghost = pl.ds(X0 + width, 2), pl.ds(X0 - 2, 2)

    def material(n, planes_from, planes_to, rows_from, rows_to, device):
        return pltpu.make_async_remote_copy(
            ce.at[planes_from, rows_from], ce.at[planes_to, rows_to],
            mat_send.at[n], mat_recv.at[n], device_id=device, device_id_type=MESH,
        )

    go_right = [
        material(0, high, low_ghost, own_slice, own_slice, right),
        material(1, high, low_ghost, halo_slice, there_slice, right_across),
    ]
    go_left = [
        material(2, low, high_ghost, own_slice, own_slice, left),
        material(3, low, high_ghost, halo_slice, there_slice, left_across),
    ]

    def each(condition, action):
        @pl.when(condition)
        def _():
            action()

    def start_all(copies):
        for copy in copies:
            copy.start()

    loads[0].wait()
    loads[1].wait()
    for x in range(width):
        flags = mask[x].astype(jnp.float32)
        inv_eps = 1.0 / (1.0 + contrast * den[x] * flags)
        ce[X0 + x, own_slice, :] = inv_eps * gain1
        grad[x] = flags * contrast * inv_eps * inv_eps * step_dt
    ce_halo.start()
    each(has_right & (gy == 0), lambda: start_all(go_right))
    each(has_left & (gy == 0), lambda: start_all(go_left))
    eye = lax.broadcasted_iota(jnp.int32, (own_rows, own_rows), 0) == lax.broadcasted_iota(
        jnp.int32, (own_rows, own_rows), 1
    )
    loads[4].wait()
    loads[6].wait()
    for s in range(2):
        spot = jnp.where(lanes == planes[s], gain1, 0.0)
        for x in range(width):
            row = jnp.broadcast_to(prof[s, x : x + 1, :], (own_rows, own_rows))
            column = jnp.sum(jnp.where(eye, row, 0.0), axis=1, keepdims=True)
            src[s, x, pl.ds(own, own_rows), :] = column * spot

    src_halo.start()
    loads[5].wait()
    loads[7].wait()
    loads[8].wait()
    def spread(row, n):
        return jnp.broadcast_to(row, (n, depth))

    def up_z(f):
        return jnp.where(spread(lanes == depth - 1, f.shape[0]), 0.0, pltpu.roll(f, depth - 1, 1))

    def down_z(f):
        return jnp.where(spread(lanes == 0, f.shape[0]), 0.0, pltpu.roll(f, 1, 1))

    def h_update(h_old, e, e_y, e_x, comps=(0, 1, 2)):
        decay, gain, gain_half = (spread(r, e[0].shape[0]) for r in (decay1, gain1, gain_half1))
        new = {}
        if 0 in comps:
            new[0] = decay * h_old(0) - gain_half * ((e_y(2) - e[2]) - (up_z(e[1]) - e[1]))
        new[1] = decay * h_old(1) - (gain_half * (up_z(e[0]) - e[0]) - gain * (e_x[2] - e[2]))
        new[2] = decay * h_old(2) - (gain * (e_x[1] - e[1]) - gain_half * (e_y(0) - e[0]))
        return new

    def e_update(e_old, h, h_y, h_x, c, drive):
        decay = spread(decay1, h[0].shape[0])
        cx = c * inv_spacing
        x = decay * e_old(0) + cx * ((h[2] - h_y(2)) - (h[1] - down_z(h[1])))
        if drive is not None:
            x = x - drive
        y = decay * e_old(1) + (cx * (h[0] - down_z(h[0])) - c * (h[2] - h_x[2]))
        z = decay * e_old(2) + (c * (h[1] - h_x[1]) - cx * (h[0] - h_y(0)))
        return {0: x, 1: y, 2: z}

    def run_free(first, rest, put_left, put_right, material_of, drive_of):
        put_left(0, first.e(1, 0, 0), first.e(2, 0, 0))
        for k in range(WIN):
            last = k == WIN - 1
            now = first if k == 0 else rest
            h_planes = [x for x in range(width) if x >= k or x < width - 1 - k]
            if last:
                h_planes = [width - 1]
            for x in h_planes:
                e = {c: now.e(c, x, 0) for c in range(3)}
                e_x = {
                    c: (now.e(c, x + 1, 0) if x < width - 1 else jnp.zeros_like(e[c]))
                    for c in (1, 2)
                }
                new = h_update(
                    lambda c: now.h(c, x, 0), e, lambda c: now.e(c, x, 1), e_x,
                    (1, 2) if last else (0, 1, 2),
                )
                if not last:
                    for c in range(3):
                        rest.set_h(c, x, new[c])
                if x == width - 1:
                    edge = new
            put_right(k, edge[1], edge[2])
            if last:
                break
            for x in [x for x in range(width) if x >= k + 1 or x < width - 1 - k]:
                h = {c: rest.h(c, x, 0) for c in range(3)}
                h_x = {c: rest.h(c, x - 1, 0) for c in (1, 2)}
                new = e_update(
                    lambda c: now.e(c, x, 0), h, lambda c: rest.h(c, x, -1), h_x,
                    material_of(x), drive_of(x, k),
                )
                for c in range(3):
                    rest.set_e(c, x, new[c])
                if x == 0:
                    edge = new
            put_left(k + 1, edge[1], edge[2])

    class Fields:
        def __init__(self, e_ref, h_ref, e_x, h_x, e_row, h_row, n):
            self.e_ref, self.h_ref, self.e_x, self.h_x = e_ref, h_ref, e_x, h_x
            self.e_row, self.h_row, self.n = e_row, h_row, n

        def e(self, c, x, dy):
            return self.e_ref[c, self.e_x + x, self.e_row + dy : self.e_row + dy + self.n, :]

        def h(self, c, x, dy):
            return self.h_ref[c, self.h_x + x, self.h_row + dy : self.h_row + dy + self.n, :]

        def set_e(self, c, x, value):
            self.e_ref[c, self.e_x + x, self.e_row : self.e_row + self.n, :] = value

        def set_h(self, c, x, value):
            self.h_ref[c, self.h_x + x, self.h_row : self.h_row + self.n, :] = value

    def to_side(go_right, s, w, k, spare=None, part=None):
        source, target = (send_h, recv_h) if go_right else (send_e, recv_e)
        source, target = source.at[s, w if spare is None else spare, k], target.at[s, w, k]
        if part is not None:
            source, target = source.at[:, part], target.at[:, part]
        send, recv = (right_send, right_recv) if go_right else (left_send, left_recv)
        return pltpu.make_async_remote_copy(
            source, target, send.at[s, w, k], recv.at[s, w, k],
            device_id=right if go_right else left, device_id_type=MESH,
        )

    def depth_of(go_right, w, k):
        return STEPS - (w * WIN + k) - (1 if go_right else 0)

    def used_rows(go_right, w, k):
        extra = depth_of(go_right, w, k)
        return pl.ds(gy * (HALO - extra), own_rows + extra)

    far_rows = pl.ds(pl.multiple_of(gy * 2 * HALO, HALO), own_rows - HALO)

    def near_rows(go_right, w, k):
        extra = depth_of(go_right, w, k)
        start = own_rows - HALO
        return pl.ds(start - gy * (start - HALO + extra), HALO + extra)

    def early():
        fields = Fields(pe, ph, 0, 1, HALO, HALO, own_rows)

        def put(go_right, k, y, z):
            buffer = send_h if go_right else send_e
            buffer[0, WINDOWS, k, 0, own_slice, :] = y
            buffer[0, WINDOWS, k, 1, own_slice, :] = z
            each(
                has_right if go_right else has_left,
                lambda: to_side(go_right, 0, 0, k, WINDOWS, far_rows).start(),
            )

        run_free(
            fields, fields,
            lambda k, y, z: put(False, k, y, z), lambda k, y, z: put(True, k, y, z),
            lambda x: ce[X0 + x, own_slice, :],
            lambda x, k: src[0, x, own_slice, :] * waves[0, k],
        )

    def free(s, w):
        def put(go_right, k, y, z):
            buffer = send_h if go_right else send_e
            buffer[s, w, k, 0] = y
            buffer[s, w, k, 1] = z
            there_is = has_right if go_right else has_left
            whole = used_rows(go_right, w, k)
            if w == 0:
                parted = (s == 0) & (gy == 0)
                each(
                    there_is & parted,
                    lambda: to_side(go_right, s, w, k, None, near_rows(go_right, w, k)).start(),
                )
                each(
                    there_is & jnp.logical_not(parted),
                    lambda: to_side(go_right, s, w, k, None, whole).start(),
                )
            else:
                each(there_is, lambda: to_side(go_right, s, w, k, None, whole).start())

        run_free(
            Fields(we.at[s], wh.at[s], X0, X0, 0, HALO, rows),
            Fields(fe, fh, 0, 1, 0, HALO, rows),
            lambda k, y, z: put(False, k, y, z), lambda k, y, z: put(True, k, y, z),
            lambda x: ce[X0 + x],
            lambda x, k: src[s, x] * waves[s, w * WIN + k],
        )

    H0, HM = slice(HALO, HALO + rows), slice(HALO - 1, HALO + rows - 1)
    R0, R1 = slice(0, rows), slice(1, rows + 1)

    def wait_series(there_is, go_right, s, w, k):
        for window in range(WINDOWS):
            rows_in = used_rows(go_right, window, k)
            each(
                there_is & (w == window),
                lambda: to_side(go_right, s, window, k, None, rows_in).wait_recv(),
            )

    def true(s, w, relay):
        for c in range(3):
            for p in (X0 - 2, X0 - 1, X0 + width, X0 + width + 1):
                we[s, c, p, R0, :] = plane0
                wh[s, c, p, H0, :] = plane0
        for k in range(WIN):
            reach = min(k + 1, WIN - k)
            h_lo, h_hi = -reach, width + min(k, WIN - 1 - k)
            e_out_reach = min(k + 1, WIN - 1 - k)
            if k == WIN - 2:
                relay()
            wait_series(has_right, False, s, w, k)
            e_next = None
            for x in range(h_hi - 1, h_lo - 1, -1):
                p = X0 + x
                e = {c: we[s, c, p, R0, :] for c in range(3)}
                if e_next is None:
                    e_x = {c: we[s, c, p + 1, R0, :] for c in (1, 2)}
                else:
                    e_x = e_next
                e_next = e
                if x == width - 1:
                    e_x = {c: (e_x[c] + recv_e[s, w, k, c - 1]) * on_right for c in (1, 2)}
                new = h_update(
                    lambda c: wh[s, c, p, H0, :], e, lambda c: we[s, c, p, R1, :], e_x
                )
                for c in range(3):
                    wh[s, c, p, H0, :] = new[c]
            wait_series(has_left, True, s, w, k)
            wave = waves[s, w * WIN + k]
            h_last = None
            for x in range(-e_out_reach, width + e_out_reach):
                p = X0 + x
                h = {c: wh[s, c, p, H0, :] for c in range(3)}
                if h_last is None:
                    h_x = {c: wh[s, c, p - 1, H0, :] for c in (1, 2)}
                else:
                    h_x = h_last
                h_last = h
                if x == 0:
                    h_x = {c: (h_x[c] + recv_h[s, w, k, c - 1]) * on_left for c in (1, 2)}
                inside = 0 <= x < width
                new = e_update(
                    lambda c: we[s, c, p, R0, :], h, lambda c: wh[s, c, p, HM, :], h_x,
                    ce[p], src[s, x] * wave if inside else None,
                )
                for c in range(3):
                    we[s, c, p, R0, :] = new[c]
                    if inside:
                        hist[s, w * WIN + k, c, x] = new[c]

    pl.when(gy == 0)(early)
    each(has_right & (gy != 0), lambda: start_all(go_right))
    each(has_left & (gy != 0), lambda: start_all(go_left))
    loads[2].wait()
    loads[3].wait()
    src_halo.wait()
    ce_halo.wait()
    e_halos[0].wait()
    h_halos[0].wait()

    def start_free(s, carry):
        @pl.when(s == 1)
        def _():
            e_halos[1].wait()
            h_halos[1].wait()

        free(s, 0)
        return carry

    pl.semaphore_wait(near, len(near_peers))
    signal(mid, mid_peers)
    lax.fori_loop(0, 2, start_free, 0)

    def wait_recvs(copies):
        for copy in copies:
            copy.wait_recv()

    def wait_sends(copies):
        for copy in copies:
            copy.wait_send()

    each(has_left, lambda: wait_recvs(go_right))
    each(has_right, lambda: wait_recvs(go_left))

    sum1 = [
        pltpu.make_async_remote_copy(
            part1.at[0], part1.at[1 + n], sum1_send.at[n], sum1_recv.at[n],
            device_id=peer, device_id_type=MESH,
        )
        for n, peer in enumerate(plane_peers)
    ]
    sum2 = [
        pltpu.make_async_remote_copy(
            part2.at[0], part2.at[1 + n], sum2_send.at[n], sum2_recv.at[n],
            device_id=peer, device_id_type=MESH,
        )
        for n, peer in enumerate(line_peers)
    ]
    def turn(j, carry):
        w, s = j // 2, lax.rem(j, 2)

        def add_plane():
            @pl.when(j == 3)
            def _():
                for copy in sum1:
                    copy.wait_recv()
                total = part1[0]
                for n in range(len(sum1)):
                    total = total + part1[1 + n]
                part2[0] = total
                for copy in sum2:
                    copy.start()

        true(s, w, add_plane)

        @pl.when(w == 0)
        def _():
            free(s, 1)

        @pl.when(j == 0)
        def _():
            pl.semaphore_wait(mid, len(mid_peers))
            signal(far, far_peers)

        @pl.when(j == 2)
        def _():
            pl.semaphore_wait(far, len(far_peers))
            total = jnp.zeros((own_rows, depth), jnp.float32)
            for c in range(3):
                for x in range(width):
                    e = we[0, c, X0 + x, pl.ds(own, own_rows), :]
                    total = total + e * e
            line = jnp.sum(total, axis=0, keepdims=True)
            part1[0] = jnp.where(lanes == planes[1], line, 0.0)
            for copy in sum1:
                copy.start()

        return carry

    lax.fori_loop(0, 2 * WINDOWS, turn, 0)

    for x in range(width):
        corr = jnp.zeros((own_rows, depth), jnp.float32)
        for k in range(STEPS):
            for c in range(3):
                corr = corr + (
                    hist[0, k, c, x, pl.ds(own, own_rows), :]
                    * hist[1, k, c, x, pl.ds(own, own_rows), :]
                )
        grad[x] = grad[x] * corr

    each(has_right, lambda: wait_sends(go_right))
    each(has_left, lambda: wait_sends(go_left))
    for copy in sum1 + sum2:
        copy.wait_send()

    def drain(s, carry):
        for w in range(WINDOWS):
            for k in range(WIN):
                for go_right, there_is in ((True, has_right), (False, has_left)):
                    copy = to_side(go_right, s, w, k, None, used_rows(go_right, w, k))
                    each(there_is, copy.wait_send)
        return carry

    lax.fori_loop(0, 2, drain, 0)

    for copy in sum2:
        copy.wait_recv()
    total = part2[0]
    for n in range(len(sum2)):
        total = total + part2[1 + n]
    cells = count_x * width * lax.axis_size("gy") * own_rows
    power = jnp.sum(total, axis=1, keepdims=True) / cells
    scale = jnp.broadcast_to(1.0 / (power + small_eps), (own_rows, depth))
    for x in range(width):
        grad[x] = grad[x] * scale


def store(we, wh, grad, e_out, h_out, g_out, sem):
    width, own_rows = grad.shape[0], grad.shape[1]
    own = pl.multiple_of(lax.axis_index("gy") * HALO, HALO)
    block = pl.ds(LEFT, width)
    outs = [pltpu.make_async_copy(grad, g_out, sem.at[0])]
    for s in range(we.shape[0]):
        outs.append(
            pltpu.make_async_copy(
                we.at[s, :, block, pl.ds(own, own_rows), :], e_out.at[s], sem.at[1 + s]
            )
        )
        outs.append(
            pltpu.make_async_copy(
                wh.at[s, :, block, pl.ds(own + HALO, own_rows), :], h_out.at[s], sem.at[3 + s]
            )
        )
    for out in outs:
        out.start()
    for out in outs:
        out.wait()


def vmem_array(shape):
    return pltpu.VMEM(shape, jnp.float32)


def in_vmem(x):
    return pltpu.with_memory_space_constraint(x, pltpu.VMEM)


def shards(electric, magnetic, density, design_mask, planes, profiles, waveforms):
    sets, comps, width, own_rows, depth = electric.shape
    rows = own_rows + HALO
    count_z = lax.axis_size("gx") // CHIPS_X
    f32 = jnp.float32
    vmem, dma = pltpu.VMEM, pltpu.SemaphoreType.DMA
    came = vmem((sets, WINDOWS, WIN, 2, rows, depth), f32)
    sent = vmem((sets, WINDOWS + 1, WIN, 2, rows, depth), f32)
    any_space = pl.BlockSpec(memory_space=pl.ANY)
    held = pl.BlockSpec(memory_space=pltpu.VMEM)
    smem, wait = pltpu.SMEM, pltpu.SemaphoreType.REGULAR
    frame = (sets, comps, FRAME, rows + HALO, depth)
    e_frame, h_frame, grad = pl.pallas_call(
        kernel,
        out_shape=(vmem_array(frame), vmem_array(frame), vmem_array(density.shape)),
        in_specs=[any_space] * 7,
        out_specs=(held,) * 3,
        scratch_shapes=[
            *[vmem((comps, width + 1, rows + HALO, depth), f32)] * 4,
            sent, sent, came, came,
            vmem((FRAME, rows, depth), f32),
            vmem((sets, width, rows, depth), f32),
            vmem((width, own_rows, depth), f32),
            vmem((width, own_rows, depth), jnp.int32),
            vmem((sets, STEPS, comps, width, rows, depth), f32),
            vmem((2 * CHIPS_X, 1, depth), f32),
            vmem((count_z, 1, depth), f32),
            smem(planes.shape, jnp.int32),
            smem(waveforms.shape, f32),
            vmem(profiles.shape, f32),
            dma((9,)), wait, wait, wait, dma((6,)), dma((6,)), dma((4,)), dma((4,)),
            dma((sets, WINDOWS, WIN)), dma((sets, WINDOWS, WIN)),
            dma((sets, WINDOWS, WIN)), dma((sets, WINDOWS, WIN)),
            dma((2 * CHIPS_X - 1,)), dma((2 * CHIPS_X - 1,)),
            dma((max(count_z - 1, 1),)), dma((max(count_z - 1, 1),)),
        ],
        compiler_params=pltpu.CompilerParams(
            collective_id=0, has_side_effects=True, vmem_limit_bytes=64_200_000
        ),
    )(planes, waveforms, profiles, electric, magnetic, density, design_mask)
    return pl.pallas_call(
        store,
        out_shape=(
            jax.ShapeDtypeStruct(electric.shape, f32),
            jax.ShapeDtypeStruct(magnetic.shape, f32),
            jax.ShapeDtypeStruct(density.shape, f32),
        ),
        in_specs=[held] * 3,
        out_specs=(any_space,) * 3,
        scratch_shapes=[dma((5,))],
        compiler_params=pltpu.CompilerParams(vmem_limit_bytes=4 << 20),
    )(in_vmem(e_frame), in_vmem(h_frame), in_vmem(grad))


def solution(mesh):
    return jax.shard_map(
        shards,
        mesh=mesh,
        in_specs=(
            P(None, None, CAND_GX, "gy", None),
            P(None, None, CAND_GX, "gy", None),
            P(CAND_GX, "gy", None),
            P(CAND_GX, "gy", None),
            P("cand"),
            P(None, CAND_GX, "gy"),
            P(None, "cand"),
        ),
        out_specs=(
            P(None, None, CAND_GX, "gy", None),
            P(None, None, CAND_GX, "gy", None),
            P(CAND_GX, "gy", None),
        ),
        check_vma=False,
    )
```

```python
import jax
import jax.numpy as jnp
from jax import lax
from jax.experimental import pallas as pl
from jax.experimental.pallas import tpu as pltpu
from jax.sharding import PartitionSpec as P

STEPS = 8
PMLW = 8
CAND_GX = ("cand", "gx")
CHIPS_X = 4
MESH = pl.DeviceIdType.MESH

step_dt = 0.7
contrast = 5.0
sigma_max = 2.0
small_eps = 1e-06
inv_spacing = 0.5

WIN = 4
WINDOWS = STEPS // WIN
LEFT = 3
FRAME = 9
HALO = 8


def kernel(
    planes_in, waves_in, prof_in, e_in, h_in, den_in, mask_in,
    we, wh, grad,
    fe, fh, pe, ph, send_h, send_e, recv_h, recv_e, ce, src, den, mask, hist, part1, part2,
    planes, waves, prof, load_sem, near, mid, far, halo_send, halo_recv, mat_send, mat_recv,
    right_send, right_recv, left_send, left_recv,
    sum1_send, sum1_recv, sum2_send, sum2_recv,
):
    width, own_rows = den.shape[0], den.shape[1]
    rows, depth = own_rows + HALO, den.shape[2]
    count_x = lax.axis_size("gx")
    count_z = count_x // CHIPS_X
    gx, gy = lax.axis_index("gx"), lax.axis_index("gy")
    chip_x, chip_z = gx // count_z, lax.rem(gx, count_z)
    other = 1 - gy
    right = {"gx": lax.rem(gx + 1, count_x), "gy": gy}
    left = {"gx": lax.rem(gx + count_x - 1, count_x), "gy": gy}
    across = {"gx": gx, "gy": other}
    right_across, left_across = dict(right, gy=other), dict(left, gy=other)
    has_right, has_left = gx < count_x - 1, gx > 0
    plane_peers = []
    for dx in range(CHIPS_X):
        for dc in range(2):
            if dx or dc:
                peer = lax.rem(chip_x + dx, CHIPS_X) * count_z + chip_z
                plane_peers.append({"gx": peer, "gy": other if dc else gy})

    def along_z(dz):
        return {"gx": chip_x * count_z + lax.rem(chip_z + dz, count_z), "gy": gy}

    def both_ways(d):
        return [along_z(dz) for dz in sorted({d % count_z, -d % count_z} - {0})]

    line_peers = [
        along_z(dz) for dz in sorted(range(1, count_z), key=lambda d: -min(d, count_z - d))
    ]
    next_chips = [
        {"gx": lax.rem(chip_x + dx, CHIPS_X) * count_z + chip_z, "gy": gy} for dx in (1, CHIPS_X - 1)
    ]
    own = pl.multiple_of(gy * HALO, HALO)
    top = pl.multiple_of((1 - gy) * (own_rows - HALO), HALO)
    there = pl.multiple_of(gy * own_rows, HALO)
    X0 = LEFT
    block = pl.ds(X0, width)

    early_rows = pl.ds(HALO, own_rows)
    loads = [
        pltpu.make_async_copy(den_in, den, load_sem.at[0]),
        pltpu.make_async_copy(mask_in, mask, load_sem.at[1]),
        pltpu.make_async_copy(e_in, we.at[:, :, block, pl.ds(own, own_rows), :], load_sem.at[2]),
        pltpu.make_async_copy(
            h_in, wh.at[:, :, block, pl.ds(own + HALO, own_rows), :], load_sem.at[3]
        ),
        pltpu.make_async_copy(planes_in, planes, load_sem.at[4]),
        pltpu.make_async_copy(waves_in, waves, load_sem.at[5]),
        pltpu.make_async_copy(prof_in, prof, load_sem.at[6]),
        pltpu.make_async_copy(e_in.at[0], pe.at[:, pl.ds(0, width), early_rows], load_sem.at[7]),
        pltpu.make_async_copy(h_in.at[0], ph.at[:, pl.ds(1, width), early_rows], load_sem.at[8]),
    ]
    for load in loads:
        load.start()

    def signal(semaphore, peers):
        for peer in peers:
            pl.semaphore_signal(semaphore, inc=1, device_id=peer, device_id_type=MESH)

    barrier = pltpu.get_barrier_semaphore()
    peers = [across, left, right, left_across, right_across] + next_chips + both_ways(1)
    near_peers = next_chips + both_ways(1)
    mid_peers = next_chips + both_ways(2)
    far_peers = both_ways(4)
    signal(barrier, peers)

    lanes = lax.broadcasted_iota(jnp.int32, (1, depth), 1)
    zpos = lanes.astype(jnp.float32)
    lower = (PMLW - zpos - 0.5) / PMLW
    upper = (zpos + 0.5 - (depth - PMLW)) / PMLW
    deep = jnp.maximum(jnp.maximum(lower, upper), 0.0)
    half = sigma_max * deep * deep * deep * step_dt / 2.0
    decay1 = (1.0 - half) / (1.0 + half)
    gain1 = step_dt / (1.0 + half)
    gain_half1 = gain1 * inv_spacing
    on_left = has_left.astype(jnp.float32)
    on_right = has_right.astype(jnp.float32)

    pad = jnp.zeros((HALO, depth), jnp.float32)
    plane0 = jnp.zeros((rows, depth), jnp.float32)
    for s in range(2):
        for c in range(3):
            for p in range(FRAME):
                if c != 1:
                    we[s, c, p, rows : rows + HALO, :] = pad
                    wh[s, c, p, 0:HALO, :] = pad
            wh[s, c, 0, HALO:, :] = plane0
    for c in (0, 2):
        for p in range(width + 1):
            fe[c, p, rows : rows + HALO, :] = pad
            fh[c, p, 0:HALO, :] = pad
            pe[c, p, rows : rows + HALO, :] = pad
            ph[c, p, 0:HALO, :] = pad
    for c in range(3):
        fe[c, width, 0:rows, :] = plane0
        fh[c, 0, HALO:, :] = plane0
        ph[c, 0, HALO:, :] = plane0

    @pl.when(jnp.logical_not(has_right))
    def _():
        recv_e[...] = jnp.zeros_like(recv_e)
        for p in (X0 + width, X0 + width + 1):
            ce[p] = plane0

    @pl.when(jnp.logical_not(has_left))
    def _():
        recv_h[...] = jnp.zeros_like(recv_h)
        for p in (X0 - 2, X0 - 1):
            ce[p] = plane0

    pl.semaphore_wait(barrier, len(peers))
    signal(near, near_peers)

    def halo(n, source, target):
        return pltpu.make_async_remote_copy(
            source, target, halo_send.at[n], halo_recv.at[n],
            device_id=across, device_id_type=MESH,
        )

    own_slice = pl.ds(own, own_rows)
    halo_slice = pl.ds(pl.multiple_of(own + top, HALO), HALO)
    there_slice = pl.ds(there, HALO)
    e_halos = [
        halo(s, e_in.at[s, :, :, pl.ds(top, HALO), :], we.at[s, :, block, there_slice, :])
        for s in range(2)
    ]
    h_halos = [
        halo(
            2 + s, h_in.at[s, :, :, pl.ds(top, HALO), :],
            wh.at[s, :, block, pl.ds(there + HALO, HALO), :],
        )
        for s in range(2)
    ]
    src_halo = halo(4, src.at[:, :, halo_slice, :], src.at[:, :, there_slice, :])
    ce_halo = halo(5, ce.at[block, halo_slice, :], ce.at[block, there_slice, :])
    for s in range(2):
        e_halos[s].start()
        h_halos[s].start()

    high, low = pl.ds(X0 + width - 2, 2), pl.ds(X0, 2)
    high_ghost, low_ghost = pl.ds(X0 + width, 2), pl.ds(X0 - 2, 2)

    def material(n, planes_from, planes_to, rows_from, rows_to, device):
        return pltpu.make_async_remote_copy(
            ce.at[planes_from, rows_from], ce.at[planes_to, rows_to],
            mat_send.at[n], mat_recv.at[n], device_id=device, device_id_type=MESH,
        )

    go_right = [
        material(0, high, low_ghost, own_slice, own_slice, right),
        material(1, high, low_ghost, halo_slice, there_slice, right_across),
    ]
    go_left = [
        material(2, low, high_ghost, own_slice, own_slice, left),
        material(3, low, high_ghost, halo_slice, there_slice, left_across),
    ]

    def each(condition, action):
        @pl.when(condition)
        def _():
            action()

    def start_all(copies):
        for copy in copies:
            copy.start()

    loads[0].wait()
    loads[1].wait()
    for x in range(width):
        flags = mask[x].astype(jnp.float32)
        inv_eps = 1.0 / (1.0 + contrast * den[x] * flags)
        ce[X0 + x, own_slice, :] = inv_eps * gain1
        grad[x] = flags * contrast * inv_eps * inv_eps * step_dt
    ce_halo.start()
    each(has_right, lambda: start_all(go_right))
    each(has_left, lambda: start_all(go_left))
    eye = lax.broadcasted_iota(jnp.int32, (own_rows, own_rows), 0) == lax.broadcasted_iota(
        jnp.int32, (own_rows, own_rows), 1
    )
    loads[4].wait()
    loads[6].wait()
    for s in range(2):
        spot = jnp.where(lanes == planes[s], gain1, 0.0)
        for x in range(width):
            row = jnp.broadcast_to(prof[s, x : x + 1, :], (own_rows, own_rows))
            column = jnp.sum(jnp.where(eye, row, 0.0), axis=1, keepdims=True)
            src[s, x, pl.ds(own, own_rows), :] = column * spot

    src_halo.start()
    loads[5].wait()
    loads[7].wait()
    loads[8].wait()
    def spread(row, n):
        return jnp.broadcast_to(row, (n, depth))

    def up_z(f):
        return jnp.where(spread(lanes == depth - 1, f.shape[0]), 0.0, pltpu.roll(f, depth - 1, 1))

    def down_z(f):
        return jnp.where(spread(lanes == 0, f.shape[0]), 0.0, pltpu.roll(f, 1, 1))

    def h_update(h_old, e, e_y, e_x, comps=(0, 1, 2)):
        decay, gain, gain_half = (spread(r, e[0].shape[0]) for r in (decay1, gain1, gain_half1))
        new = {}
        if 0 in comps:
            new[0] = decay * h_old(0) - gain_half * ((e_y(2) - e[2]) - (up_z(e[1]) - e[1]))
        new[1] = decay * h_old(1) - (gain_half * (up_z(e[0]) - e[0]) - gain * (e_x[2] - e[2]))
        new[2] = decay * h_old(2) - (gain * (e_x[1] - e[1]) - gain_half * (e_y(0) - e[0]))
        return new

    def e_update(e_old, h, h_y, h_x, c, drive):
        decay = spread(decay1, h[0].shape[0])
        cx = c * inv_spacing
        x = decay * e_old(0) + cx * ((h[2] - h_y(2)) - (h[1] - down_z(h[1])))
        if drive is not None:
            x = x - drive
        y = decay * e_old(1) + (cx * (h[0] - down_z(h[0])) - c * (h[2] - h_x[2]))
        z = decay * e_old(2) + (c * (h[1] - h_x[1]) - cx * (h[0] - h_y(0)))
        return {0: x, 1: y, 2: z}

    def run_free(first, rest, put_left, put_right, material_of, drive_of):
        put_left(0, first.e(1, 0, 0), first.e(2, 0, 0))
        for k in range(WIN):
            last = k == WIN - 1
            now = first if k == 0 else rest
            h_planes = [x for x in range(width) if x >= k or x < width - 1 - k]
            if last:
                h_planes = [width - 1]
            for x in h_planes:
                e = {c: now.e(c, x, 0) for c in range(3)}
                e_x = {
                    c: (now.e(c, x + 1, 0) if x < width - 1 else jnp.zeros_like(e[c]))
                    for c in (1, 2)
                }
                new = h_update(
                    lambda c: now.h(c, x, 0), e, lambda c: now.e(c, x, 1), e_x,
                    (1, 2) if last else (0, 1, 2),
                )
                if not last:
                    for c in range(3):
                        rest.set_h(c, x, new[c])
                if x == width - 1:
                    edge = new
            put_right(k, edge[1], edge[2])
            if last:
                break
            for x in [x for x in range(width) if x >= k + 1 or x < width - 1 - k]:
                h = {c: rest.h(c, x, 0) for c in range(3)}
                h_x = {c: rest.h(c, x - 1, 0) for c in (1, 2)}
                new = e_update(
                    lambda c: now.e(c, x, 0), h, lambda c: rest.h(c, x, -1), h_x,
                    material_of(x), drive_of(x, k),
                )
                for c in range(3):
                    rest.set_e(c, x, new[c])
                if x == 0:
                    edge = new
            put_left(k + 1, edge[1], edge[2])

    class Fields:
        def __init__(self, e_ref, h_ref, e_x, h_x, e_row, h_row, n):
            self.e_ref, self.h_ref, self.e_x, self.h_x = e_ref, h_ref, e_x, h_x
            self.e_row, self.h_row, self.n = e_row, h_row, n

        def e(self, c, x, dy):
            return self.e_ref[c, self.e_x + x, self.e_row + dy : self.e_row + dy + self.n, :]

        def h(self, c, x, dy):
            return self.h_ref[c, self.h_x + x, self.h_row + dy : self.h_row + dy + self.n, :]

        def set_e(self, c, x, value):
            self.e_ref[c, self.e_x + x, self.e_row : self.e_row + self.n, :] = value

        def set_h(self, c, x, value):
            self.h_ref[c, self.h_x + x, self.h_row : self.h_row + self.n, :] = value

    def to_side(go_right, s, w, k, spare=None, part=None):
        source, target = (send_h, recv_h) if go_right else (send_e, recv_e)
        source, target = source.at[s, w if spare is None else spare, k], target.at[s, w, k]
        if part is not None:
            source, target = source.at[:, part], target.at[:, part]
        send, recv = (right_send, right_recv) if go_right else (left_send, left_recv)
        return pltpu.make_async_remote_copy(
            source, target, send.at[s, w, k], recv.at[s, w, k],
            device_id=right if go_right else left, device_id_type=MESH,
        )

    def depth_of(go_right, w, k):
        return STEPS - (w * WIN + k) - (1 if go_right else 0)

    def used_rows(go_right, w, k):
        extra = depth_of(go_right, w, k)
        return pl.ds(gy * (HALO - extra), own_rows + extra)

    far_rows = pl.ds(pl.multiple_of(gy * 2 * HALO, HALO), own_rows - HALO)

    def near_rows(go_right, w, k):
        extra = depth_of(go_right, w, k)
        start = own_rows - HALO
        return pl.ds(start - gy * (start - HALO + extra), HALO + extra)

    def early():
        fields = Fields(pe, ph, 0, 1, HALO, HALO, own_rows)

        def put(go_right, k, y, z):
            buffer = send_h if go_right else send_e
            buffer[0, WINDOWS, k, 0, own_slice, :] = y
            buffer[0, WINDOWS, k, 1, own_slice, :] = z
            each(
                has_right if go_right else has_left,
                lambda: to_side(go_right, 0, 0, k, WINDOWS, far_rows).start(),
            )

        run_free(
            fields, fields,
            lambda k, y, z: put(False, k, y, z), lambda k, y, z: put(True, k, y, z),
            lambda x: ce[X0 + x, own_slice, :],
            lambda x, k: src[0, x, own_slice, :] * waves[0, k],
        )

    def free(s, w):
        def put(go_right, k, y, z):
            buffer = send_h if go_right else send_e
            buffer[s, w, k, 0] = y
            buffer[s, w, k, 1] = z
            there_is = has_right if go_right else has_left
            whole = used_rows(go_right, w, k)
            if w == 0:
                parted = (s == 0) & (gy == 0)
                each(
                    there_is & parted,
                    lambda: to_side(go_right, s, w, k, None, near_rows(go_right, w, k)).start(),
                )
                each(
                    there_is & jnp.logical_not(parted),
                    lambda: to_side(go_right, s, w, k, None, whole).start(),
                )
            else:
                each(there_is, lambda: to_side(go_right, s, w, k, None, whole).start())

        run_free(
            Fields(we.at[s], wh.at[s], X0, X0, 0, HALO, rows),
            Fields(fe, fh, 0, 1, 0, HALO, rows),
            lambda k, y, z: put(False, k, y, z), lambda k, y, z: put(True, k, y, z),
            lambda x: ce[X0 + x],
            lambda x, k: src[s, x] * waves[s, w * WIN + k],
        )

    H0, HM = slice(HALO, HALO + rows), slice(HALO - 1, HALO + rows - 1)
    R0, R1 = slice(0, rows), slice(1, rows + 1)

    def wait_series(there_is, go_right, s, w, k):
        for window in range(WINDOWS):
            rows_in = used_rows(go_right, window, k)
            each(
                there_is & (w == window),
                lambda: to_side(go_right, s, window, k, None, rows_in).wait_recv(),
            )

    def true(s, w, relay):
        for c in range(3):
            for p in (X0 - 2, X0 - 1, X0 + width, X0 + width + 1):
                we[s, c, p, R0, :] = plane0
                wh[s, c, p, H0, :] = plane0
        for k in range(WIN):
            reach = min(k + 1, WIN - k)
            h_lo, h_hi = -reach, width + min(k, WIN - 1 - k)
            e_out_reach = min(k + 1, WIN - 1 - k)
            if k == WIN - 2:
                relay()
            wait_series(has_right, False, s, w, k)
            e_next = None
            for x in range(h_hi - 1, h_lo - 1, -1):
                p = X0 + x
                e = {c: we[s, c, p, R0, :] for c in range(3)}
                if e_next is None:
                    e_x = {c: we[s, c, p + 1, R0, :] for c in (1, 2)}
                else:
                    e_x = e_next
                e_next = e
                if x == width - 1:
                    e_x = {c: (e_x[c] + recv_e[s, w, k, c - 1]) * on_right for c in (1, 2)}
                new = h_update(
                    lambda c: wh[s, c, p, H0, :], e, lambda c: we[s, c, p, R1, :], e_x
                )
                for c in range(3):
                    wh[s, c, p, H0, :] = new[c]
            wait_series(has_left, True, s, w, k)
            wave = waves[s, w * WIN + k]
            h_last = None
            for x in range(-e_out_reach, width + e_out_reach):
                p = X0 + x
                h = {c: wh[s, c, p, H0, :] for c in range(3)}
                if h_last is None:
                    h_x = {c: wh[s, c, p - 1, H0, :] for c in (1, 2)}
                else:
                    h_x = h_last
                h_last = h
                if x == 0:
                    h_x = {c: (h_x[c] + recv_h[s, w, k, c - 1]) * on_left for c in (1, 2)}
                inside = 0 <= x < width
                new = e_update(
                    lambda c: we[s, c, p, R0, :], h, lambda c: wh[s, c, p, HM, :], h_x,
                    ce[p], src[s, x] * wave if inside else None,
                )
                for c in range(3):
                    we[s, c, p, R0, :] = new[c]
                    if inside:
                        hist[s, w * WIN + k, c, x] = new[c]

    pl.when(gy == 0)(early)
    loads[2].wait()
    loads[3].wait()
    src_halo.wait()
    ce_halo.wait()
    e_halos[0].wait()
    h_halos[0].wait()

    def start_free(s, carry):
        @pl.when(s == 1)
        def _():
            e_halos[1].wait()
            h_halos[1].wait()

        free(s, 0)
        return carry

    pl.semaphore_wait(near, len(near_peers))
    signal(mid, mid_peers)
    lax.fori_loop(0, 2, start_free, 0)

    def wait_recvs(copies):
        for copy in copies:
            copy.wait_recv()

    def wait_sends(copies):
        for copy in copies:
            copy.wait_send()

    each(has_left, lambda: wait_recvs(go_right))
    each(has_right, lambda: wait_recvs(go_left))

    sum1 = [
        pltpu.make_async_remote_copy(
            part1.at[0], part1.at[1 + n], sum1_send.at[n], sum1_recv.at[n],
            device_id=peer, device_id_type=MESH,
        )
        for n, peer in enumerate(plane_peers)
    ]
    sum2 = [
        pltpu.make_async_remote_copy(
            part2.at[0], part2.at[1 + n], sum2_send.at[n], sum2_recv.at[n],
            device_id=peer, device_id_type=MESH,
        )
        for n, peer in enumerate(line_peers)
    ]
    def turn(j, carry):
        w, s = j // 2, lax.rem(j, 2)

        def add_plane():
            @pl.when(j == 3)
            def _():
                for copy in sum1:
                    copy.wait_recv()
                total = part1[0]
                for n in range(len(sum1)):
                    total = total + part1[1 + n]
                part2[0] = total
                for copy in sum2:
                    copy.start()

        true(s, w, add_plane)

        @pl.when(w == 0)
        def _():
            free(s, 1)

        @pl.when(j == 0)
        def _():
            pl.semaphore_wait(mid, len(mid_peers))
            signal(far, far_peers)

        @pl.when(j == 2)
        def _():
            pl.semaphore_wait(far, len(far_peers))
            total = jnp.zeros((own_rows, depth), jnp.float32)
            for c in range(3):
                for x in range(width):
                    e = we[0, c, X0 + x, pl.ds(own, own_rows), :]
                    total = total + e * e
            line = jnp.sum(total, axis=0, keepdims=True)
            part1[0] = jnp.where(lanes == planes[1], line, 0.0)
            for copy in sum1:
                copy.start()

        return carry

    lax.fori_loop(0, 2 * WINDOWS, turn, 0)

    for x in range(width):
        corr = jnp.zeros((own_rows, depth), jnp.float32)
        for k in range(STEPS):
            for c in range(3):
                corr = corr + (
                    hist[0, k, c, x, pl.ds(own, own_rows), :]
                    * hist[1, k, c, x, pl.ds(own, own_rows), :]
                )
        grad[x] = grad[x] * corr

    each(has_right, lambda: wait_sends(go_right))
    each(has_left, lambda: wait_sends(go_left))
    for copy in sum1 + sum2:
        copy.wait_send()

    def drain(s, carry):
        for w in range(WINDOWS):
            for k in range(WIN):
                for go_right, there_is in ((True, has_right), (False, has_left)):
                    copy = to_side(go_right, s, w, k, None, used_rows(go_right, w, k))
                    each(there_is, copy.wait_send)
        return carry

    lax.fori_loop(0, 2, drain, 0)

    for copy in sum2:
        copy.wait_recv()
    total = part2[0]
    for n in range(len(sum2)):
        total = total + part2[1 + n]
    cells = count_x * width * lax.axis_size("gy") * own_rows
    power = jnp.sum(total, axis=1, keepdims=True) / cells
    scale = jnp.broadcast_to(1.0 / (power + small_eps), (own_rows, depth))
    for x in range(width):
        grad[x] = grad[x] * scale


def store(we, wh, grad, e_out, h_out, g_out, sem):
    width, own_rows = grad.shape[0], grad.shape[1]
    own = pl.multiple_of(lax.axis_index("gy") * HALO, HALO)
    block = pl.ds(LEFT, width)
    outs = [pltpu.make_async_copy(grad, g_out, sem.at[0])]
    for s in range(we.shape[0]):
        outs.append(
            pltpu.make_async_copy(
                we.at[s, :, block, pl.ds(own, own_rows), :], e_out.at[s], sem.at[1 + s]
            )
        )
        outs.append(
            pltpu.make_async_copy(
                wh.at[s, :, block, pl.ds(own + HALO, own_rows), :], h_out.at[s], sem.at[3 + s]
            )
        )
    for out in outs:
        out.start()
    for out in outs:
        out.wait()


def vmem_array(shape):
    return pltpu.VMEM(shape, jnp.float32)


def in_vmem(x):
    return pltpu.with_memory_space_constraint(x, pltpu.VMEM)


def shards(electric, magnetic, density, design_mask, planes, profiles, waveforms):
    sets, comps, width, own_rows, depth = electric.shape
    rows = own_rows + HALO
    count_z = lax.axis_size("gx") // CHIPS_X
    f32 = jnp.float32
    vmem, dma = pltpu.VMEM, pltpu.SemaphoreType.DMA
    came = vmem((sets, WINDOWS, WIN, 2, rows, depth), f32)
    sent = vmem((sets, WINDOWS + 1, WIN, 2, rows, depth), f32)
    any_space = pl.BlockSpec(memory_space=pl.ANY)
    held = pl.BlockSpec(memory_space=pltpu.VMEM)
    smem, wait = pltpu.SMEM, pltpu.SemaphoreType.REGULAR
    frame = (sets, comps, FRAME, rows + HALO, depth)
    e_frame, h_frame, grad = pl.pallas_call(
        kernel,
        out_shape=(vmem_array(frame), vmem_array(frame), vmem_array(density.shape)),
        in_specs=[any_space] * 7,
        out_specs=(held,) * 3,
        scratch_shapes=[
            *[vmem((comps, width + 1, rows + HALO, depth), f32)] * 4,
            sent, sent, came, came,
            vmem((FRAME, rows, depth), f32),
            vmem((sets, width, rows, depth), f32),
            vmem((width, own_rows, depth), f32),
            vmem((width, own_rows, depth), jnp.int32),
            vmem((sets, STEPS, comps, width, rows, depth), f32),
            vmem((2 * CHIPS_X, 1, depth), f32),
            vmem((count_z, 1, depth), f32),
            smem(planes.shape, jnp.int32),
            smem(waveforms.shape, f32),
            vmem(profiles.shape, f32),
            dma((9,)), wait, wait, wait, dma((6,)), dma((6,)), dma((4,)), dma((4,)),
            dma((sets, WINDOWS, WIN)), dma((sets, WINDOWS, WIN)),
            dma((sets, WINDOWS, WIN)), dma((sets, WINDOWS, WIN)),
            dma((2 * CHIPS_X - 1,)), dma((2 * CHIPS_X - 1,)),
            dma((max(count_z - 1, 1),)), dma((max(count_z - 1, 1),)),
        ],
        compiler_params=pltpu.CompilerParams(
            collective_id=0, has_side_effects=True, vmem_limit_bytes=64_200_000
        ),
    )(planes, waveforms, profiles, electric, magnetic, density, design_mask)
    return pl.pallas_call(
        store,
        out_shape=(
            jax.ShapeDtypeStruct(electric.shape, f32),
            jax.ShapeDtypeStruct(magnetic.shape, f32),
            jax.ShapeDtypeStruct(density.shape, f32),
        ),
        in_specs=[held] * 3,
        out_specs=(any_space,) * 3,
        scratch_shapes=[dma((5,))],
        compiler_params=pltpu.CompilerParams(vmem_limit_bytes=4 << 20),
    )(in_vmem(e_frame), in_vmem(h_frame), in_vmem(grad))


def solution(mesh):
    return jax.shard_map(
        shards,
        mesh=mesh,
        in_specs=(
            P(None, None, CAND_GX, "gy", None),
            P(None, None, CAND_GX, "gy", None),
            P(CAND_GX, "gy", None),
            P(CAND_GX, "gy", None),
            P("cand"),
            P(None, CAND_GX, "gy"),
            P(None, "cand"),
        ),
        out_specs=(
            P(None, None, CAND_GX, "gy", None),
            P(None, None, CAND_GX, "gy", None),
            P(CAND_GX, "gy", None),
        ),
        check_vma=False,
    )
```
